128 devices in a mesh: seq: 4 (over x_lo, core), tensor: 32 (over z, y, x_hi).
Axes of the slice: x: 4 (x_hi: 2, x_lo: 2; x = x_hi * 2 + x_lo), y: 4, z: 4, core: 2. Of those that a mesh axis runs over, the one named last changes fastest.
Arguments:
- tokens: bfloat16 [2, 4096, 4096], P(None, 'seq', 'tensor'), may hold values from -6 to 6
- w_qkv: bfloat16 [4096, 3, 4096], P(None, None, 'tensor'), may hold values from -1 to 1
- q_gain: float32 [4096], P('tensor'), may hold values from 0.5 to 2.5
- k_gain: float32 [4096], P('tensor'), may hold values from 0.5 to 2.5
- w_out: bfloat16 [4096, 4096], P('tensor'), may hold values from -0.1875 to 0.1875
Outputs:
- mixed: bfloat16 [2, 4096, 4096], P(None, 'seq', 'tensor')
- peak: float32 [32], P('tensor')
- qk_scale: float32 [2, 2, 4096], P(None, None, 'seq')
The draws below stay inside these ranges and needn't reach their ends.
All inputs are finite; a program needn't handle non-finite values.
Results may differ from the reference program's by a relative error of at most 0.024.
Values may be sent and summed in bfloat16 or wider, within the bound.
A program may use at most 128 MiB of HBM per device.

```python
import math
import jax
import jax.numpy as jnp
from jax import lax

D = 4096
HEADS = 32
HEAD = 128
SEQS = 2
LENGTH = 4096
N_TENSOR = 32


def draw_tokens(key, part):
    base = jax.random.fold_in(key, 11)
    return jnp.clip(jax.random.normal(base, (SEQS, LENGTH, D), jnp.float32), -6.0, 6.0).astype(jnp.bfloat16)


def draw_w_qkv(key, part):
    base = jax.random.fold_in(key, 21)
    raw = jnp.clip(jax.random.normal(base, (D, 3, HEADS, HEAD), jnp.float32), -6.0, 6.0) / jnp.sqrt(jnp.float32(D))
    ramp = 0.6 * 3.0 ** (jnp.arange(HEADS, dtype=jnp.float32) / (HEADS - 1))
    scales = ramp * jnp.exp(jax.random.uniform(jax.random.fold_in(key, 22), (HEADS,), jnp.float32, jnp.log(0.8), jnp.log(1.25)))
    factors = jnp.stack([scales, scales, jnp.ones((HEADS,), jnp.float32)])
    raw = raw * factors[None, :, :, None]
    return jnp.clip(raw, -1.0, 1.0).reshape(D, 3, D).astype(jnp.bfloat16)


def with_spikes(values, own_key, source, target, shards_of, factor):
    def block_of(dim):
        return (jnp.arange(values.shape[dim]) // (values.shape[dim] // shards_of)).reshape((-1,) + (1,) * (values.ndim - 1 - dim))

    one_side = jax.random.permutation(own_key, shards_of)[block_of(target)]
    far = (block_of(target) + shards_of // 2) % shards_of
    return jnp.where((block_of(source) == one_side) | (block_of(source) == far), factor * values, values)


def block_levels(stream_key, extent, split, low, high):
    def one(axis_at, shards_of):
        steps = jax.random.uniform(jax.random.fold_in(jax.random.fold_in(stream_key, 6), axis_at), (shards_of,), jnp.float32, low / len(split), high / len(split))
        return jnp.repeat(jnp.exp(steps), extent[axis_at] // shards_of).reshape((-1,) + (1,) * (len(extent) - axis_at - 1))

    loudness = one(*split[0])
    for cut in split[1:]:
        loudness = loudness * one(*cut)
    return loudness


def gaussian_with(own_key, shape, scale, bound, cuts, heavy, kind=jnp.bfloat16):
    array = scale * jax.random.normal(own_key, shape, jnp.float32)
    if cuts:
        array = array * block_levels(own_key, shape, cuts, -0.22, 0.18)
    return jnp.clip(with_spikes(array, jax.random.fold_in(own_key, 3), *heavy), -bound, bound).astype(kind)


def setup_inputs(seed: int = 0) -> dict:
    splits = jax.random.split(jax.random.key(seed), 6)
    return {
        "tokens": draw_tokens(jax.random.fold_in(splits[5], 71), 0),
        "w_qkv": draw_w_qkv(jax.random.fold_in(splits[5], 71), 0),
        "q_gain": jnp.clip(jnp.exp(math.log(2.5) - 1.609438 * jax.random.uniform(splits[2], (D,), jnp.float32) ** block_levels(splits[2], (D,), ((0, 32),), -0.2, 0.2)), 0.5, 2.5),
        "k_gain": jnp.clip(jnp.exp(math.log(2.5) - 1.609438 * jax.random.uniform(splits[3], (D,), jnp.float32) ** block_levels(splits[3], (D,), ((0, 32),), -0.2, 0.2)), 0.5, 2.5),
        "w_out": gaussian_with(splits[4], (D, D), D ** -0.5, 0.1875, ((0, 32),), (0, 1, 32, 2.75)),
    }


EPS = 1e-06
ROPE_BASE = 500000.0
NEG = -1e+30

def rope_tables(positions):
    half = HEAD // 2
    freq = ROPE_BASE ** (-(jnp.arange(half, dtype=jnp.float32) * 2.0) / HEAD)
    angle = positions[:, None] * freq[None, :]
    return (jnp.cos(angle), jnp.sin(angle))

def rotate(values, cosine, sine):
    half = values.shape[-1] // 2
    first = values[..., :half]
    second = values[..., half:]
    cosine = cosine[:, None, :]
    sine = sine[:, None, :]
    return jnp.concatenate([first * cosine - second * sine, second * cosine + first * sine], -1)

def reference(tokens, w_qkv, q_gain, k_gain, w_out):
    flat = tokens.reshape(SEQS * LENGTH, D)
    query = jnp.dot(flat, w_qkv[:, 0, :], preferred_element_type=jnp.float32)
    keyed = jnp.dot(flat, w_qkv[:, 1, :], preferred_element_type=jnp.float32)
    value = jnp.dot(flat, w_qkv[:, 2, :], preferred_element_type=jnp.float32)
    inv_query = lax.rsqrt(lax.optimization_barrier(jnp.mean(query * query, -1)) + EPS)
    inv_key = lax.rsqrt(lax.optimization_barrier(jnp.mean(keyed * keyed, -1)) + EPS)
    positions = jnp.arange(LENGTH, dtype=jnp.float32)
    cosine, sine = rope_tables(positions)
    q_norm = (query * inv_query[:, None] * q_gain[None, :]).reshape(SEQS, LENGTH, HEADS, HEAD)
    k_norm = (keyed * inv_key[:, None] * k_gain[None, :]).reshape(SEQS, LENGTH, HEADS, HEAD)
    q_rot = lax.optimization_barrier(rotate(q_norm, cosine, sine).astype(jnp.bfloat16))
    k_rot = lax.optimization_barrier(rotate(k_norm, cosine, sine).astype(jnp.bfloat16))
    v_b = lax.optimization_barrier(value.astype(jnp.bfloat16)).reshape(SEQS, LENGTH, HEADS, HEAD)
    q_heads = q_rot.transpose(2, 0, 1, 3)
    k_heads = k_rot.transpose(2, 0, 1, 3)
    v_heads = v_b.transpose(2, 0, 1, 3)
    causal = jnp.arange(LENGTH)[None, :] <= jnp.arange(LENGTH)[:, None]
    scale = HEAD ** (-0.5)

    def attend(operands):
        qh, kh, vh = operands
        scores = jnp.einsum('sqd,skd->sqk', qh.astype(jnp.float32), kh.astype(jnp.float32)) * scale
        scores = jnp.where(causal[None], scores, NEG)
        top = lax.optimization_barrier(jnp.max(scores, -1))
        weights = jnp.where(causal[None], jnp.exp(scores - top[..., None]), 0.0)
        denom = lax.optimization_barrier(jnp.sum(weights, -1))
        rounded = lax.optimization_barrier(weights.astype(jnp.bfloat16)).astype(jnp.float32)
        mixed = jnp.einsum('sqk,skd->sqd', rounded, vh.astype(jnp.float32))
        return ((mixed / denom[..., None]).astype(jnp.bfloat16), jnp.max(top))
    outputs, peak = lax.map(attend, (q_heads, k_heads, v_heads))
    attended = lax.optimization_barrier(outputs.transpose(1, 2, 0, 3).reshape(SEQS * LENGTH, D))
    group = D // N_TENSOR

    def add_group(total, index):
        cols = lax.dynamic_slice_in_dim(attended, index * group, group, 1)
        rows = lax.dynamic_slice_in_dim(w_out, index * group, group, 0)
        term = lax.optimization_barrier(jnp.dot(cols, rows, preferred_element_type=jnp.float32).astype(jnp.bfloat16))
        return (total + term.astype(jnp.float32), None)
    total, unused = lax.scan(add_group, jnp.zeros((SEQS * LENGTH, D), jnp.float32), jnp.arange(N_TENSOR, dtype=jnp.int32))
    mixed = total.astype(jnp.bfloat16).reshape(SEQS, LENGTH, D)
    qk_scale = jnp.stack([inv_query, inv_key]).reshape(2, SEQS, LENGTH)
    return (mixed, peak, qk_scale)
```

```python
import functools

import jax
import jax.numpy as jnp
from jax import lax
from jax.experimental import pallas as pl
from jax.experimental.pallas import tpu as pltpu
from jax.sharding import Mesh
from jax.sharding import PartitionSpec as P

EPS = 1e-06
ROPE_BASE = 500000.0
NEG = -1e30
MESH = pl.DeviceIdType.MESH
HEAD = 128
TOK = 1024
HALF = TOK // 2
WIDTH = 4096
VMEM_CAP = 60 * 1024 * 1024
COPIES = 40


def here():
    xh, xl = lax.axis_index("xh"), lax.axis_index("xl")
    return xh * 2 + xl, xh, xl, lax.axis_index("co"), lax.axis_index("z"), lax.axis_index("y")


def seq_of(x):
    return 1 - ((x + 1) // 2) % 2


def half_of(x):
    return 1 - x % 2


def at_x(x, core=None):
    dev = {"xl": x % 2, "xh": x // 2}
    if core is not None:
        dev["co"] = core
    return dev


def greet(devices):
    barrier = pltpu.get_barrier_semaphore()
    for dev in devices:
        pl.semaphore_signal(barrier, inc=1, device_id=dev, device_id_type=MESH)
    pl.semaphore_wait(barrier, len(devices))


def remote(src, dst, ssem, rsem, dev):
    return pltpu.make_async_remote_copy(
        src_ref=src, dst_ref=dst, send_sem=ssem, recv_sem=rsem, device_id=dev, device_id_type=MESH
    )


def gather(buf, ssem, rsem, z, y, own_ready, use):
    sent = []
    count = [0]

    def place(h, f, s):
        return (f % 4, s % 4) if h == 0 else (s % 4, f % 4)

    first = (z, y)
    second = (y, z)
    axis = (("z", "y"), ("y", "z"))

    def send(h, f, s, part, along, dirn):
        zz, yy = place(h, f, s)
        ref = buf.at[h, zz, yy] if part is None else buf.at[h, zz, yy, part]
        name = axis[h][along]
        me = (first[h], second[h])[along]
        c = count[0]
        count[0] += 1
        cp = remote(ref, ref, ssem.at[c], rsem.at[c], {name: (me + dirn + 4) % 4})
        cp.start()
        sent.append(cp)
        return cp

    p1, p1f, p2, p2f = {}, {}, {}, {}
    part_of = {1: 0, -1: 1}
    dirs = (1, -1)
    for h in (0, 1):
        own_ready(h)
        f, s = first[h], second[h]
        for d in dirs:
            p1[h, d] = send(h, f, s, None, 0, d)
        if h == 1:
            for g in (0, 1):
                for d in dirs:
                    p2[g, 0, d] = send(g, first[g], second[g], None, 1, d)
    for h in (0, 1):
        use(h, *place(h, first[h], second[h]))
    for d in dirs:
        for h in (0, 1):
            f, s = first[h], second[h]
            p1[h, d].wait_recv()
            p1f[h, d] = send(h, f - d + 4, s, part_of[d], 0, d)
            for e in dirs:
                p2[h, -d, e] = send(h, f - d + 4, s, None, 1, e)
    for d in dirs:
        for h in (0, 1):
            use(h, *place(h, first[h] - d + 4, second[h]))
    for d in dirs:
        for h in (0, 1):
            p2[h, 0, d].wait_recv()
            p2f[h, 0, d] = send(h, first[h], second[h] - d + 4, part_of[d], 1, d)
    for h in (0, 1):
        for d in dirs:
            p1f[h, d].wait_recv()
        for d in dirs:
            p2[h, 2, d] = send(h, first[h] + 2, second[h], None, 1, d)
    for h in (0, 1):
        for d in dirs:
            use(h, *place(h, first[h], second[h] - d + 4))
        use(h, *place(h, first[h] + 2, second[h]))
    for j in (-1, 1, 2):
        for h in (0, 1):
            f, s = first[h], second[h]
            for d in dirs:
                p2[h, j, d].wait_recv()
                p2f[h, j, d] = send(h, f + j + 4, s - d + 4, part_of[d], 1, d)
        for h in (0, 1):
            for d in dirs:
                use(h, *place(h, first[h] + j + 4, second[h] - d + 4))
    for j in (0, -1, 1, 2):
        for h in (0, 1):
            for d in dirs:
                p2f[h, j, d].wait_recv()
            use(h, *place(h, first[h] + j + 4, second[h] + 2))
    return sent


def block_dot(acc, buf, w, h, zz, yy):
    base = pl.multiple_of((zz * 4 + yy) * 256, 256)
    rhs = w[pl.ds(base, 256), :]
    lhs = jnp.concatenate([buf[h, zz, yy, 0], buf[h, zz, yy, 1]], axis=-1)
    rows = pl.ds(h * HALF, HALF)
    acc[rows, :] += jnp.dot(lhs, rhs, preferred_element_type=jnp.float32)


def qkv_kernel(
    tok, w_own, gains, cosf, sinf,
    q_out, k_out, v_out, stat_out,
    buf, w_far, gains_far, acc, acc_far, qx, kx, vx, zb, yb, inv, inv_in,
    ssem, rsem, xs, xr,
):
    x, xh, xl, co, z, y = here()
    right, left, pair = (x + 1) % 4, (x + 3) % 4, 3 - x
    greet(
        [at_x(right), at_x(left), {"co": 1 - co}, at_x(pair, 1 - co)]
        + [{"z": (z + i) % 4} for i in (1, 2, 3)]
        + [{"y": (y + i) % 4} for i in (1, 2, 3)]
    )
    n = [0]
    sent = []

    def send(src, dst, dev):
        c = n[0]
        n[0] += 1
        cp = remote(src, dst, xs.at[c], xr.at[c], dev)
        cp.start()
        sent.append(cp)
        return cp

    toks = {}
    for h in (0, 1):
        rows = pl.ds(h * HALF, HALF)
        toks[h] = (
            send(tok.at[xh, rows], buf.at[h, z, y, xh], at_x(right)),
            send(tok.at[1 - xh, rows], buf.at[h, z, y, xh], at_x(left)),
        )
    far_g = send(gains, gains_far, at_x(pair))
    far_w = []
    for i in (0, 1):
        rows = pl.ds(pl.multiple_of((co * 2 + i) * 1024, 1024), 1024)
        far_w.append(send(w_own.at[rows], w_far.at[rows], at_x(pair)))
    acc[...] = jnp.zeros_like(acc)
    acc_far[...] = jnp.zeros_like(acc_far)

    def own_ready(h):
        for cp in toks[h]:
            cp.wait_recv()

    late = []
    relayed = []

    def use(h, zz, yy):
        block_dot(acc, buf, w_own, h, zz, yy)
        late.append((h, zz, yy))
        if len(late) == 20:
            for i in (0, 1):
                far_w[i].wait_recv()
                rows = pl.ds(pl.multiple_of((co * 2 + i) * 1024, 1024), 1024)
                relayed.append(send(w_far.at[rows], w_far.at[rows], {"co": 1 - co}))
        if len(late) == 24:
            for cp in relayed:
                cp.wait_recv()
            for b in late:
                block_dot(acc_far, buf, w_far, *b)
        if len(late) > 24:
            block_dot(acc_far, buf, w_far, h, zz, yy)

    sent += gather(buf, ssem, rsem, z, y, own_ready, use)

    step = 256

    def squares(i, carry):
        rows = pl.ds(pl.multiple_of(i * step, step), step)
        for j in (0, 1):
            cols = pl.ds(j * HEAD, HEAD)
            a, b = acc[rows, cols], acc_far[rows, cols]
            zb[z, pl.ds(j, 1), rows] = jnp.sum((a * a + b * b).T, axis=0, keepdims=True)
        return carry

    lax.fori_loop(0, TOK // step, squares, 0)
    got = [send(zb.at[z], zb.at[z], {"z": (z + i) % 4}) for i in (1, 2, 3)]
    for cp in got:
        cp.wait_recv()
    yb[y] = (zb[0] + zb[1]) + (zb[2] + zb[3])
    got = [send(yb.at[y], yb.at[y], {"y": (y + i) % 4}) for i in (1, 2, 3)]
    for cp in got:
        cp.wait_recv()
    inv[...] = lax.rsqrt(((yb[0] + yb[1]) + (yb[2] + yb[3])) / WIDTH + EPS)
    me_seq = seq_of(x)
    stats = [send(inv, inv_in.at[me_seq], at_x(right)), send(inv, inv_in.at[me_seq], at_x(left))]
    far_g.wait_recv()

    mine = half_of(x) * 2 + co

    def rows_of(i, carry):
        rows = pl.ds(pl.multiple_of(i * step, step), step)
        cs, sn = cosf[rows, :], sinf[rows, :]

        def turned(a, j, g):
            col = jnp.broadcast_to(inv[pl.ds(j, 1), rows], (HEAD, step)).T
            t = a[rows, pl.ds(j * HEAD, HEAD)] * col * g[pl.ds(j, 1), :]
            return (t * cs + pltpu.roll(t, HEAD // 2, 1) * sn).astype(jnp.bfloat16)

        qx[rows, :] = turned(acc_far, 0, gains_far)
        kx[rows, :] = turned(acc_far, 1, gains_far)
        vx[rows, :] = acc_far[rows, pl.ds(2 * HEAD, HEAD)].astype(jnp.bfloat16)
        q_out[0, rows, :] = turned(acc, 0, gains)
        k_out[mine, rows, :] = turned(acc, 1, gains)
        v_out[mine, rows, :] = acc[rows, pl.ds(2 * HEAD, HEAD)].astype(jnp.bfloat16)
        return carry

    lax.fori_loop(0, TOK // step, rows_of, 0)
    other = {"co": 1 - co}
    far_q = send(qx, q_out.at[1], at_x(pair, 1 - co))
    far_k = send(kx, k_out.at[mine], at_x(pair))
    far_v = send(vx, v_out.at[mine], at_x(pair))
    near = [
        send(k_out.at[mine], k_out.at[mine], other),
        send(v_out.at[mine], v_out.at[mine], other),
    ]
    theirs = (1 - half_of(x)) * 2 + co
    far_k.wait_recv()
    near.append(send(k_out.at[theirs], k_out.at[theirs], other))
    far_v.wait_recv()
    near.append(send(v_out.at[theirs], v_out.at[theirs], other))
    for cp in stats:
        cp.wait_recv()
    for s in (0, 1):
        stat_out[:, s, :] = inv_in[s]
    far_q.wait_recv()
    for cp in near:
        cp.wait_recv()
    for cp in sent:
        cp.wait_send()


def attend_kernel(q, k, v, o, top_out):
    x, xh, xl, co, z, y = here()
    own = half_of(x) * 2 + co
    factor = (HEAD ** (-0.5)) * 1.4426950408889634
    bq, bk = 256, 512
    best = jnp.full((8, 128), NEG, jnp.float32)
    for which in (0, 1):
        quarter = own if which == 0 else (1 - half_of(x)) * 2 + (1 - co)

        def tile(i, best):
            rows = pl.ds(pl.multiple_of(i * bq, bq), bq)
            qt = q[which, rows, :]
            first = quarter * TOK + i * bq

            def visit(j, state, masked):
                top, den, out = state
                at = pl.multiple_of(j * bk, bk)
                keys = pl.ds(at, bk)
                s = lax.dot_general(
                    qt, k[keys, :], (((1,), (1,)), ((), ())), preferred_element_type=jnp.float32
                )
                if masked:
                    r = lax.broadcasted_iota(jnp.int32, (bq, bk), 0) + first
                    c = lax.broadcasted_iota(jnp.int32, (bq, bk), 1) + at
                    s = jnp.where(c <= r, s, NEG)
                new = jnp.maximum(top, jnp.max(s, axis=1, keepdims=True))
                e = jnp.exp2((s - new) * factor)
                keep = jnp.exp2((top - new) * factor)
                den = den * keep + jnp.sum(e, axis=1, keepdims=True)
                out = out * keep + jnp.dot(
                    e.astype(jnp.bfloat16), v[keys, :], preferred_element_type=jnp.float32
                )
                return new, den, out

            state = (
                jnp.full((bq, 1), NEG, jnp.float32),
                jnp.zeros((bq, 1), jnp.float32),
                jnp.zeros((bq, HEAD), jnp.float32),
            )
            last = first // bk
            state = lax.fori_loop(0, last, lambda j, st: visit(j, st, False), state)
            top, den, out = visit(last, state, True)
            o[which, rows, :] = (out / den).astype(jnp.bfloat16)
            return jnp.maximum(best, jnp.max(top))

        best = lax.fori_loop(0, TOK // bq, tile, best)
    top_out[...] = best * (HEAD ** (-0.5))


def mix_kernel(
    o, top, w,
    mixed, peak,
    buf, acc, ob, tops,
    ssem, rsem, xs, xr,
):
    x, xh, xl, co, z, y = here()
    right, left, pair = (x + 1) % 4, (x + 3) % 4, 3 - x
    same = xh * 2 + (1 - xl)
    greet(
        [at_x(right), at_x(left), {"co": 1 - co}, at_x(right, 1 - co), at_x(left, 1 - co)]
        + [{"z": (z + 1) % 4}, {"z": (z + 3) % 4}, {"y": (y + 1) % 4}, {"y": (y + 3) % 4}]
    )
    n = [0]
    sent = []

    def send(src, dst, dev):
        c = n[0]
        n[0] += 1
        cp = remote(src, dst, xs.at[c], xr.at[c], dev)
        cp.start()
        sent.append(cp)
        return cp

    back = {
        h: send(o.at[1, pl.ds(h * HALF, HALF)], buf.at[h, z, y, xh], at_x(pair, 1 - co))
        for h in (0, 1)
    }
    for h in (0, 1):
        buf[h, z, y, xh] = o[0, pl.ds(h * HALF, HALF), :]
    place = xl * 2 + co
    tops[place] = top[...]
    peaks = [
        send(tops.at[place], tops.at[place], dev)
        for dev in ({"co": 1 - co}, at_x(same), at_x(same, 1 - co))
    ]
    acc[...] = jnp.zeros_like(acc)

    def use(h, zz, yy):
        block_dot(acc, buf, w, h, zz, yy)

    sent += gather(buf, ssem, rsem, z, y, lambda h: back[h].wait_recv(), use)
    ob[0] = acc[:, 0:HEAD].astype(jnp.bfloat16)
    ob[1] = acc[:, HEAD:].astype(jnp.bfloat16)
    me_seq = seq_of(x)
    fin = [
        send(ob.at[right // 2], mixed.at[me_seq], at_x(right)),
        send(ob.at[left // 2], mixed.at[me_seq], at_x(left)),
    ]
    for cp in peaks:
        cp.wait_recv()
    peak[...] = jnp.maximum(jnp.maximum(tops[0], tops[1]), jnp.maximum(tops[2], tops[3]))
    for cp in fin:
        cp.wait_recv()
    for cp in sent:
        cp.wait_send()


def vmem(count):
    return [pl.BlockSpec(memory_space=pltpu.VMEM)] * count


def shards(tokens, w_qkv, q_gain, k_gain, w_out):
    x = lax.axis_index("xh") * 2 + lax.axis_index("xl")
    quarter = half_of(x) * 2 + lax.axis_index("co")
    w_own = w_qkv.reshape(WIDTH, 3 * HEAD)
    gains = jnp.concatenate([q_gain[None], k_gain[None], jnp.zeros((6, HEAD), jnp.float32)])
    positions = (quarter * TOK + jnp.arange(TOK, dtype=jnp.int32)).astype(jnp.float32)
    freq = ROPE_BASE ** (-(jnp.arange(HEAD // 2, dtype=jnp.float32) * 2.0) / HEAD)
    angle = positions[:, None] * freq[None, :]
    cosine, sine = jnp.cos(angle), jnp.sin(angle)
    cosf = jnp.concatenate([cosine, cosine], -1)
    sinf = jnp.concatenate([-sine, sine], -1)

    half_rows = lax.all_to_all(
        w_out.reshape(HEAD, 16, 256).transpose(1, 0, 2), ("z", "y"), 0, 0, tiled=True
    )
    both = lax.all_gather(half_rows, "xh", axis=1)
    w_cols = both.reshape(WIDTH, 256)

    bf, f32 = jnp.bfloat16, jnp.float32
    dma = pltpu.SemaphoreType.DMA
    q, k, v, stat = pl.pallas_call(
        qkv_kernel,
        out_shape=(
            jax.ShapeDtypeStruct((2, TOK, HEAD), bf),
            jax.ShapeDtypeStruct((4, TOK, HEAD), bf),
            jax.ShapeDtypeStruct((4, TOK, HEAD), bf),
            jax.ShapeDtypeStruct((2, 2, TOK), f32),
        ),
        in_specs=vmem(5),
        out_specs=tuple(vmem(4)),
        scratch_shapes=[
            pltpu.VMEM((2, 4, 4, 2, HALF, HEAD), bf),
            pltpu.VMEM((WIDTH, 3 * HEAD), bf),
            pltpu.VMEM((8, HEAD), f32),
            pltpu.VMEM((TOK, 3 * HEAD), f32),
            pltpu.VMEM((TOK, 3 * HEAD), f32),
            pltpu.VMEM((TOK, HEAD), bf),
            pltpu.VMEM((TOK, HEAD), bf),
            pltpu.VMEM((TOK, HEAD), bf),
            pltpu.VMEM((4, 2, TOK), f32),
            pltpu.VMEM((4, 2, TOK), f32),
            pltpu.VMEM((2, TOK), f32),
            pltpu.VMEM((2, 2, TOK), f32),
            dma((COPIES,)),
            dma((COPIES,)),
            dma((32,)),
            dma((32,)),
        ],
        compiler_params=pltpu.CompilerParams(
            collective_id=0, has_side_effects=True, vmem_limit_bytes=VMEM_CAP
        ),
        name="qkv",
    )(tokens, w_own, gains, cosf, sinf)

    o, top = pl.pallas_call(
        attend_kernel,
        out_shape=(
            jax.ShapeDtypeStruct((2, TOK, HEAD), bf),
            jax.ShapeDtypeStruct((8, HEAD), f32),
        ),
        in_specs=vmem(3),
        out_specs=tuple(vmem(2)),
        compiler_params=pltpu.CompilerParams(vmem_limit_bytes=VMEM_CAP),
        name="attend",
    )(q, k.reshape(4 * TOK, HEAD), v.reshape(4 * TOK, HEAD))

    mixed, peak = pl.pallas_call(
        mix_kernel,
        out_shape=(
            jax.ShapeDtypeStruct((2, TOK, HEAD), bf),
            jax.ShapeDtypeStruct((8, HEAD), f32),
        ),
        in_specs=vmem(3),
        out_specs=tuple(vmem(2)),
        scratch_shapes=[
            pltpu.VMEM((2, 4, 4, 2, HALF, HEAD), bf),
            pltpu.VMEM((TOK, 256), f32),
            pltpu.VMEM((2, TOK, HEAD), bf),
            pltpu.VMEM((4, 8, HEAD), f32),
            dma((COPIES,)),
            dma((COPIES,)),
            dma((8,)),
            dma((8,)),
        ],
        compiler_params=pltpu.CompilerParams(
            collective_id=1, has_side_effects=True, vmem_limit_bytes=VMEM_CAP
        ),
        name="mix",
    )(o, top, w_cols)
    return mixed, peak[0, :1], stat


def solution(mesh):
    finer = Mesh(mesh.devices.reshape(2, 2, 4, 4, 2), ("xl", "co", "z", "y", "xh"))
    tensor = ("z", "y", "xh")
    seq = ("xl", "co")
    placed = (P(None, seq, tensor), P(None, None, tensor), P(tensor), P(tensor), P(tensor, None))
    return jax.shard_map(
        shards,
        mesh=finer,
        in_specs=placed,
        out_specs=(P(None, seq, tensor), P(tensor), P(None, None, seq)),
        check_vma=False,
    )
```

```python
import contextlib
import math

import jax
import jax.numpy as jnp
import numpy as np
from jax import lax
from jax.experimental import pallas as pl
from jax.experimental.pallas import tpu as pltpu
from jax.sharding import Mesh
from jax.sharding import PartitionSpec as P

EPS = 1e-06
ROPE_BASE = 500000.0
NEG = -1e30
MESH = pl.DeviceIdType.MESH
HEAD = 128
TOK = 1024
CHUNKS = 2
CROWS = TOK // CHUNKS
WIDTH = 4096
BK = 512
VMEM_CAP = 60 * 1024 * 1024
SCALE = HEAD ** (-0.5)
LOG2E = math.log2(math.e)
DIRS = (1, -1)
PART = {1: 0, -1: 1}


def scope(name):
    return contextlib.nullcontext()


def here():
    xh, xl = lax.axis_index("xh"), lax.axis_index("xl")
    return xh * 2 + xl, xh, xl, lax.axis_index("co"), lax.axis_index("z"), lax.axis_index("y")


def seq_of(x):
    return 1 - ((x + 1) // 2) % 2


def half_of(x):
    return 1 - x % 2


def at_x(x, core=None):
    dev = {"xl": x % 2, "xh": x // 2}
    if core is not None:
        dev["co"] = core
    return dev


class Sender:
    def __init__(self, ssem, rsem):
        self.ssem, self.rsem, self.sent = ssem, rsem, []

    def __call__(self, src, dst, dev):
        c = len(self.sent)
        cp = pltpu.make_async_remote_copy(
            src_ref=src,
            dst_ref=dst,
            send_sem=self.ssem.at[c],
            recv_sem=self.rsem.at[c],
            device_id=dev,
            device_id_type=MESH,
        )
        cp.start()
        self.sent.append(cp)
        return cp


class Gather:
    def __init__(self, buf, send, z, y, use):
        self.buf, self.send, self.use = buf, send, use
        self.first, self.second = (z, y), (y, z)
        self.p1, self.p1f, self.p2, self.p2f = {}, {}, {}, {}

    def place(self, h, f, s):
        return (f % 4, s % 4) if h == 0 else (s % 4, f % 4)

    def at(self, h, df, ds):
        return self.place(h, self.first[h] + df, self.second[h] + ds)

    def move(self, h, df, ds, part, along, d):
        zz, yy = self.at(h, df, ds)
        ref = self.buf.at[h, zz, yy] if part is None else self.buf.at[h, zz, yy, part]
        name = (("z", "y"), ("y", "z"))[h][along]
        me = (self.first[h], self.second[h])[along]
        return self.send(ref, ref, {name: (me + d + 4) % 4})

    def start(self, h):
        for d in DIRS:
            self.p1[h, d] = self.move(h, 0, 0, None, 0, d)

    def start_second(self, h):
        for d in DIRS:
            self.p2[h, 0, d] = self.move(h, 0, 0, None, 1, d)

    def own(self, h):
        self.use(h, *self.at(h, 0, 0))

    def near(self, h, d):
        self.p1[h, d].wait_recv()
        self.p1f[h, d] = self.move(h, 4 - d, 0, PART[d], 0, d)
        for e in DIRS:
            self.p2[h, -d, e] = self.move(h, 4 - d, 0, None, 1, e)

    def use_near(self, h, d):
        self.use(h, *self.at(h, 4 - d, 0))

    def pass_on(self, h, j):
        for d in DIRS:
            self.p2[h, j, d].wait_recv()
            self.p2f[h, j, d] = self.move(h, j + 4, 4 - d, PART[d], 1, d)

    def use_passed(self, h, j):
        for d in DIRS:
            self.use(h, *self.at(h, j + 4, 4 - d))

    def opposite(self, h):
        for d in DIRS:
            self.p1f[h, d].wait_recv()
        for d in DIRS:
            self.p2[h, 2, d] = self.move(h, 2, 0, None, 1, d)

    def use_opposite(self, h):
        self.use(h, *self.at(h, 2, 0))

    def last(self, h, j):
        for d in DIRS:
            self.p2f[h, j, d].wait_recv()
        self.use(h, *self.at(h, j + 4, 2))


def layer_kernel(
    tok, w_own, q_gain, k_gain, w_out, freq,
    mixed, peak, stat_out,
    buf, w_far, gains, gains_far, cosf, sinf, acc, acc_far, zb, yb, inv, inv_in,
    q_all, k_all, v_all, q_far, k_far, v_far,
    wz, w_cols, buf2, o_far, acc2, ob, tops,
    xs, xr, as_, ar, bs, br,
):
    x, xh, xl, co, z, y = here()
    right, left, pair, same = (x + 1) % 4, (x + 3) % 4, 3 - x, xh * 2 + (1 - xl)
    other = {"co": 1 - co}
    peers = (
        [at_x(right), at_x(left), other, at_x(right, 1 - co), at_x(left, 1 - co)]
        + [{"z": (z + i) % 4} for i in (1, 2, 3)]
        + [{"y": (y + i) % 4} for i in (1, 2, 3)]
    )
    with scope("greet"):
        barrier = pltpu.get_barrier_semaphore()
        for dev in peers:
            pl.semaphore_signal(barrier, inc=1, device_id=dev, device_id_type=MESH)
        pl.semaphore_wait(barrier, len(peers))
    send = Sender(xs, xr)
    mine = half_of(x) * 2 + co
    theirs = (1 - half_of(x)) * 2 + co
    me_seq = seq_of(x)
    sub = CROWS // 2

    toks = {}

    def send_tokens(ch):
        for h in (0, 1):
            rows = pl.ds(ch * CROWS + h * sub, sub)
            dst = buf.at[ch, h, z, y, xh]
            toks[ch, h] = (
                send(tok.at[xh, rows], dst, at_x(right)),
                send(tok.at[1 - xh, rows], dst, at_x(left)),
            )

    send_tokens(0)
    gains[0:1, :] = q_gain[...]
    gains[1:2, :] = k_gain[...]

    def w_rows(i):
        return pl.ds(pl.multiple_of((co * 2 + i) * 1024, 1024), 1024)

    far_w = [send(w_own.at[:, w_rows(0)], w_far.at[:, w_rows(0)], at_x(pair))]
    send_tokens(1)
    far_w.append(send(w_own.at[:, w_rows(1)], w_far.at[:, w_rows(1)], at_x(pair)))
    far_g = send(gains, gains_far, at_x(pair))
    relayed = {}

    def relay(i):
        far_w[i].wait_recv()
        relayed[i] = send(w_far.at[:, w_rows(i)], w_far.at[:, w_rows(i)], other)

    def dots(target, w, ch, h, blocks, zero=False):
        lhs, rhs = [], []
        for zz, yy in blocks:
            lhs += [buf[ch, h, zz, yy, 0], buf[ch, h, zz, yy, 1]]
            rows = pl.ds(pl.multiple_of((zz * 4 + yy) * 256, 256), 256)
            rhs.append(jnp.concatenate([w[0, rows, :], w[1, rows, :], w[2, rows, :]], axis=-1))
        lhs = jnp.concatenate(lhs, axis=-1)
        rhs = rhs[0] if len(rhs) == 1 else jnp.concatenate(rhs, axis=0)
        out = jnp.dot(lhs, rhs, preferred_element_type=jnp.float32)
        rows = pl.ds(ch * CROWS + h * sub, sub)
        target[rows, :] = out if zero else target[rows, :] + out

    def gather_of(ch):
        return Gather(
            buf.at[ch],
            Sender(as_.at[ch], ar.at[ch]),
            z,
            y,
            lambda h, zz, yy: dots(acc, w_own, ch, h, [(zz, yy)]),
        )

    def own_dot(ch, h):
        dots(acc, w_own, ch, h, [(z, y)], True)

    def far_dots(ch, zs):
        for i, zz in enumerate(zs):
            for h in (0, 1):
                dots(acc_far, w_far, ch, h, [(zz, yy) for yy in range(4)], zz == 0)

    def tables():
        def some(i, carry):
            rows = pl.ds(pl.multiple_of(i * 256, 256), 256)
            p = lax.broadcasted_iota(jnp.int32, (256, HEAD), 0) + (mine * TOK + i * 256)
            lane = lax.broadcasted_iota(jnp.int32, (256, HEAD), 1)
            angle = p.astype(jnp.float32) * freq[...]
            cosf[rows, :] = jnp.cos(angle)
            sine = jnp.sin(angle)
            sinf[rows, :] = jnp.where(lane < HEAD // 2, -sine, sine)
            return carry

        lax.fori_loop(0, TOK // 256, some, 0)

    got = {}

    def squares(ch):
        for j in (0, 1):
            cols = pl.ds(j * HEAD, HEAD)
            for i in range(2):
                rows = pl.ds(ch * CROWS + i * sub, sub)
                a, b = acc[rows, cols], acc_far[rows, cols]
                zb[ch, z, j : j + 1, i * sub : (i + 1) * sub] = jnp.sum(
                    (a * a + b * b).T, axis=0, keepdims=True
                )
        ref = zb.at[ch, z]
        got["z", ch] = [send(ref, ref, {"z": (z + i) % 4}) for i in (1, 2, 3)]

    def totals(ch):
        for cp in got["z", ch]:
            cp.wait_recv()
        yb[ch, y] = (zb[ch, 0] + zb[ch, 1]) + (zb[ch, 2] + zb[ch, 3])
        ref = yb.at[ch, y]
        got["y", ch] = [send(ref, ref, {"y": (y + i) % 4}) for i in (1, 2, 3)]

    stats = []

    def rope(ch):
        for cp in got["y", ch]:
            cp.wait_recv()
        inv[ch] = lax.rsqrt(((yb[ch, 0] + yb[ch, 1]) + (yb[ch, 2] + yb[ch, 3])) / WIDTH + EPS)
        for dev in (right, left):
            stats.append(send(inv.at[ch], inv_in.at[me_seq, ch], at_x(dev)))
        slot = mine * CHUNKS + ch
        for i in range(2):
            here_rows = slice(i * sub, (i + 1) * sub)
            rows = pl.ds(ch * CROWS + i * sub, sub)
            cs, sn = cosf[rows, :], sinf[rows, :]

            def turned(a, j, g):
                col = jnp.broadcast_to(inv[ch, j : j + 1, here_rows], (HEAD, sub)).T
                t = a[rows, j * HEAD : (j + 1) * HEAD] * col * g[j : j + 1, :]
                return (t * cs + pltpu.roll(t, HEAD // 2, 1) * sn).astype(jnp.bfloat16)

            q_far[rows, :] = turned(acc_far, 0, gains_far)
            k_far[rows, :] = turned(acc_far, 1, gains_far)
            v_far[ch, :, here_rows] = acc_far[rows, 2 * HEAD :].T.astype(jnp.bfloat16)
            q_all[0, rows, :] = turned(acc, 0, gains)
            k_all[slot, here_rows, :] = turned(acc, 1, gains)
            v_all[slot, :, here_rows] = acc[rows, 2 * HEAD :].T.astype(jnp.bfloat16)

    swaps, near = {}, []

    def swap(ch):
        rows = pl.ds(ch * CROWS, CROWS)
        slot = mine * CHUNKS + ch
        swaps[ch] = [
            send(k_far.at[rows], k_all.at[slot], at_x(pair)),
            send(v_far.at[ch], v_all.at[slot], at_x(pair)),
            send(q_far.at[rows], q_all.at[1, rows], at_x(pair, 1 - co)),
        ]
        near.append(send(k_all.at[slot], k_all.at[slot], other))
        near.append(send(v_all.at[slot], v_all.at[slot], other))

    def relay_kv(ch):
        slot = theirs * CHUNKS + ch
        for cp, ref in zip(swaps[ch], (k_all, v_all)):
            cp.wait_recv()
            near.append(send(ref.at[slot], ref.at[slot], other))

    part = pl.ds(pl.multiple_of(co * 64, 64), 64)

    def z_cols(zz):
        return pl.ds(pl.multiple_of((zz % 4) * 1024, 1024), 1024)

    def y_cols(yy):
        return pl.ds(pl.multiple_of((yy % 4) * 256, 256), 256)

    def cols_z():
        wz[z] = w_out[part, z_cols(z)]
        got["wz"] = [
            send(w_out.at[part, z_cols(z + i)], wz.at[z], {"z": (z + i) % 4}) for i in (1, 2, 3)
        ]

    def cols_y():
        for cp in got["wz"]:
            cp.wait_recv()
        w_cols[:, y, xh, part, :] = wz[:, :, y_cols(y)]
        got["wy"] = [
            send(wz.at[:, :, y_cols(y + i)], w_cols.at[:, y, xh, part], {"y": (y + i) % 4})
            for i in (1, 2, 3)
        ]

    def cols_x():
        for cp in got["wy"]:
            cp.wait_recv()
        ref = w_cols.at[:, :, xh, part]
        got["wx"] = [send(ref, ref, at_x(pair))]

    def cols_core():
        got["wx"][0].wait_recv()
        ref = w_cols.at[:, :, :, part]
        got["wc"] = [send(ref, ref, other)]

    g = [gather_of(0), gather_of(1)]

    def begin(ch):
        for h in (0, 1):
            for cp in toks[ch, h]:
                cp.wait_recv()
            g[ch].start(h)
        for h in (0, 1):
            g[ch].start_second(h)

    def middle(ch):
        for h in (0, 1):
            own_dot(ch, h)
        for d in DIRS:
            for h in (0, 1):
                g[ch].near(h, d)
        for d in DIRS:
            for h in (0, 1):
                g[ch].use_near(h, d)
        for h in (0, 1):
            g[ch].pass_on(h, 0)
        for h in (0, 1):
            g[ch].opposite(h)
        for h in (0, 1):
            g[ch].use_passed(h, 0)
            g[ch].use_opposite(h)
        for h in (0, 1):
            g[ch].pass_on(h, -1)
        for h in (0, 1):
            g[ch].use_passed(h, -1)
        for h in (0, 1):
            g[ch].pass_on(h, 1)

    def drain(ch, j):
        for h in (0, 1):
            g[ch].last(h, j)

    with scope("begin0"):
        begin(0)
    with scope("tables"):
        tables()
    with scope("middle0"):
        middle(0)
    with scope("begin1"):
        begin(1)
        for h in (0, 1):
            g[0].pass_on(h, 2)
        for h in (0, 1):
            g[0].use_passed(h, 1)
            g[0].use_passed(h, 2)
    with scope("drain0"):
        for j in (0, -1, 1, 2):
            drain(0, j)
        relay(0)
    with scope("middle1"):
        middle(1)
        for h in (0, 1):
            g[1].pass_on(h, 2)
    with scope("far0"):
        relayed[0].wait_recv()
        far_dots(0, (0, 2))
        for h in (0, 1):
            g[1].use_passed(h, 1)
    with scope("relay1"):
        relay(1)
    with scope("use2"):
        for h in (0, 1):
            g[1].use_passed(h, 2)
        relayed[1].wait_recv()
    with scope("far0b"):
        far_dots(0, (1, 3))
        squares(0)
    with scope("drain1"):
        for j in (0, -1):
            drain(1, j)
        totals(0)
        for j in (1, 2):
            drain(1, j)
        cols_z()
    with scope("far1"):
        far_dots(1, (0, 2, 1, 3))
        squares(1)
    far_g.wait_recv()
    with scope("rope0"):
        rope(0)
        swap(0)
    with scope("tot1"):
        totals(1)
        cols_y()
    with scope("rope1"):
        rope(1)
        swap(1)
    with scope("relay_kv"):
        for ch in range(CHUNKS):
            relay_kv(ch)
        cols_x()
    with scope("swap_wait"):
        for ch in range(CHUNKS):
            swaps[ch][2].wait_recv()
        for cp in near:
            cp.wait_recv()

    factor = SCALE * LOG2E
    best = [jnp.full((1, BK), NEG, jnp.float32)]

    def attend(which, ch):
        quarter = mine if which == 0 else (1 - half_of(x)) * 2 + (1 - co)
        qt = q_all[which, ch * CROWS : (ch + 1) * CROWS, :]

        def visit(j, state, masked):
            top, den, out = state
            s = lax.dot_general(
                k_all[j], qt, (((1,), (1,)), ((), ())), preferred_element_type=jnp.float32
            )
            if masked:
                r = lax.broadcasted_iota(jnp.int32, (BK, CROWS), 0)
                c = lax.broadcasted_iota(jnp.int32, (BK, CROWS), 1)
                s = jnp.where(r <= c, s, NEG)
            new = jnp.maximum(top, jnp.max(s, axis=0, keepdims=True))
            e = jnp.exp2((s - new) * factor)
            keep = jnp.exp2((top - new) * factor)
            den = den * keep + jnp.sum(e, axis=0, keepdims=True)
            out = out * keep + jnp.dot(
                v_all[j], e.astype(jnp.bfloat16), preferred_element_type=jnp.float32
            )
            return new, den, out

        state = (
            jnp.full((1, CROWS), NEG, jnp.float32),
            jnp.zeros((1, CROWS), jnp.float32),
            jnp.zeros((HEAD, CROWS), jnp.float32),
        )
        last = quarter * CHUNKS + ch
        state = lax.fori_loop(0, last, lambda j, st: visit(j, st, False), state)
        top, den, out = visit(last, state, True)
        best[0] = jnp.maximum(best[0], top)
        return (out / den).T.astype(jnp.bfloat16)

    back = {}

    def attend_half(h):
        o_far[h] = attend(1, h)
        back[h] = send(o_far.at[h], buf2.at[h, z, y, xh], at_x(pair, 1 - co))
        buf2[h, z, y, xh] = attend(0, h)

    def use2(h, zz, yy, zero=False):
        lhs = jnp.concatenate([buf2[h, zz, yy, 0], buf2[h, zz, yy, 1]], axis=-1)
        rhs = jnp.concatenate([w_cols[zz, yy, 0], w_cols[zz, yy, 1]], axis=0)
        out = jnp.dot(lhs, rhs, preferred_element_type=jnp.float32)
        rows = pl.ds(h * CROWS, CROWS)
        acc2[rows, :] = out if zero else acc2[rows, :] + out

    g2 = Gather(buf2, Sender(bs, br), z, y, use2)
    with scope("attend0"):
        attend_half(0)
    with scope("start2_0"):
        cols_core()
        back[0].wait_recv()
        g2.start(0)
        g2.start_second(0)
    with scope("attend1"):
        attend_half(1)
    with scope("start2_1"):
        place = xl * 2 + co
        tops[place] = jnp.broadcast_to(jnp.max(best[0], axis=1, keepdims=True), (8, HEAD)) * SCALE
        back[1].wait_recv()
        g2.start(1)
        g2.start_second(1)
        peaks = [
            send(tops.at[place], tops.at[place], dev)
            for dev in (other, at_x(same), at_x(same, 1 - co))
        ]
    with scope("near2"):
        for d in DIRS:
            g2.near(0, d)
        got["wc"][0].wait_recv()
        use2(0, z, y, True)
        for d in DIRS:
            g2.near(1, d)
        use2(1, z, y, True)
        for h in (0, 1):
            for d in DIRS:
                g2.use_near(h, d)
        for h in (0, 1):
            g2.pass_on(h, 0)
        for h in (0, 1):
            g2.opposite(h)
        for h in (0, 1):
            g2.use_passed(h, 0)
            g2.use_opposite(h)
    with scope("pass2"):
        for j in (-1, 1, 2):
            for h in (0, 1):
                g2.pass_on(h, j)
            for h in (0, 1):
                g2.use_passed(h, j)
    fin = []
    with scope("drain2"):
        for j in (0, -1, 1):
            for h in (0, 1):
                g2.last(h, j)
        for h in (0, 1):
            g2.last(h, 2)
            rows = pl.ds(h * CROWS, CROWS)
            for i in (0, 1):
                ob[i, rows, :] = acc2[rows, i * HEAD : (i + 1) * HEAD].astype(jnp.bfloat16)
            for dev in (right, left):
                fin.append(send(ob.at[dev // 2, rows], mixed.at[me_seq, rows], at_x(dev)))
    with scope("final"):
        for cp in peaks:
            cp.wait_recv()
        peak[...] = jnp.maximum(jnp.maximum(tops[0], tops[1]), jnp.maximum(tops[2], tops[3]))
        for cp in stats:
            cp.wait_recv()
        for s in (0, 1):
            for ch in range(CHUNKS):
                stat_out[:, s, ch * CROWS : (ch + 1) * CROWS] = inv_in[s, ch]
        for cp in fin:
            cp.wait_recv()
    with scope("wait_send"):
        for s in (send, g[0].send, g[1].send, g2.send):
            for cp in s.sent:
                cp.wait_send()


def vmem(count):
    return [pl.BlockSpec(memory_space=pltpu.VMEM)] * count


def shards(tokens, w_qkv, q_gain, k_gain, w_out):
    bf, f32 = jnp.bfloat16, jnp.float32
    dma = pltpu.SemaphoreType.DMA
    sub = CROWS // 2
    freq = ROPE_BASE ** (-(np.arange(HEAD) % (HEAD // 2) * 2.0) / HEAD)
    mixed, peak, stat = pl.pallas_call(
        layer_kernel,
        out_shape=(
            jax.ShapeDtypeStruct((2, TOK, HEAD), bf),
            jax.ShapeDtypeStruct((8, HEAD), f32),
            jax.ShapeDtypeStruct((2, 2, TOK), f32),
        ),
        in_specs=vmem(6),
        out_specs=tuple(vmem(3)),
        scratch_shapes=[
            pltpu.VMEM((CHUNKS, 2, 4, 4, 2, sub, HEAD), bf),
            pltpu.VMEM((3, WIDTH, HEAD), bf),
            pltpu.VMEM((8, HEAD), f32),
            pltpu.VMEM((8, HEAD), f32),
            pltpu.VMEM((TOK, HEAD), f32),
            pltpu.VMEM((TOK, HEAD), f32),
            pltpu.VMEM((TOK, 3 * HEAD), f32),
            pltpu.VMEM((TOK, 3 * HEAD), f32),
            pltpu.VMEM((CHUNKS, 4, 2, CROWS), f32),
            pltpu.VMEM((CHUNKS, 4, 2, CROWS), f32),
            pltpu.VMEM((CHUNKS, 2, CROWS), f32),
            pltpu.VMEM((2, CHUNKS, 2, CROWS), f32),
            pltpu.VMEM((2, TOK, HEAD), bf),
            pltpu.VMEM((4 * CHUNKS, CROWS, HEAD), bf),
            pltpu.VMEM((4 * CHUNKS, HEAD, CROWS), bf),
            pltpu.VMEM((TOK, HEAD), bf),
            pltpu.VMEM((TOK, HEAD), bf),
            pltpu.VMEM((CHUNKS, HEAD, CROWS), bf),
            pltpu.VMEM((4, 64, 1024), bf),
            pltpu.VMEM((4, 4, 2, HEAD, 256), bf),
            pltpu.VMEM((2, 4, 4, 2, CROWS, HEAD), bf),
            pltpu.VMEM((2, CROWS, HEAD), bf),
            pltpu.VMEM((TOK, 256), f32),
            pltpu.VMEM((2, TOK, HEAD), bf),
            pltpu.VMEM((4, 8, HEAD), f32),
            dma((72,)),
            dma((72,)),
            dma((CHUNKS, 40)),
            dma((CHUNKS, 40)),
            dma((40,)),
            dma((40,)),
        ],
        compiler_params=pltpu.CompilerParams(
            collective_id=0, has_side_effects=True, vmem_limit_bytes=VMEM_CAP
        ),
        name="layer",
    )(
        tokens,
        w_qkv.transpose(1, 0, 2),
        q_gain[None],
        k_gain[None],
        w_out,
        jnp.asarray(freq[None], f32),
    )
    return mixed, peak[0, :1], stat


def solution(mesh):
    finer = Mesh(mesh.devices.reshape(2, 2, 4, 4, 2), ("xl", "co", "z", "y", "xh"))
    tensor = ("z", "y", "xh")
    seq = ("xl", "co")
    placed = (P(None, seq, tensor), P(None, None, tensor), P(tensor), P(tensor), P(tensor, None))
    return jax.shard_map(
        shards,
        mesh=finer,
        in_specs=placed,
        out_specs=(P(None, seq, tensor), P(tensor), P(None, None, seq)),
        check_vma=False,
    )
```

```python
import contextlib
import math

import jax
import jax.numpy as jnp
import numpy as np
from jax import lax
from jax.experimental import pallas as pl
from jax.experimental.pallas import tpu as pltpu
from jax.sharding import Mesh
from jax.sharding import PartitionSpec as P

EPS = 1e-06
ROPE_BASE = 500000.0
NEG = -1e30
MESH = pl.DeviceIdType.MESH
HEAD = 128
TOK = 1024
CHUNKS = 2
CROWS = TOK // CHUNKS
WIDTH = 4096
BK = 512
VMEM_CAP = 60 * 1024 * 1024
SCALE = HEAD ** (-0.5)
LOG2E = math.log2(math.e)
DIRS = (1, -1)
PART = {1: 0, -1: 1}
CQ, CV, CK = 0, HEAD, 2 * HEAD


def scope(name):
    return contextlib.nullcontext()


def here():
    xh, xl = lax.axis_index("xh"), lax.axis_index("xl")
    return xh * 2 + xl, xh, xl, lax.axis_index("co"), lax.axis_index("z"), lax.axis_index("y")


def seq_of(x):
    return 1 - ((x + 1) // 2) % 2


def half_of(x):
    return 1 - x % 2


def at_x(x, core=None):
    dev = {"xl": x % 2, "xh": x // 2}
    if core is not None:
        dev["co"] = core
    return dev


class Sender:
    def __init__(self, ssem, rsem):
        self.ssem, self.rsem, self.sent = ssem, rsem, []

    def __call__(self, src, dst, dev):
        c = len(self.sent)
        cp = pltpu.make_async_remote_copy(
            src_ref=src,
            dst_ref=dst,
            send_sem=self.ssem.at[c],
            recv_sem=self.rsem.at[c],
            device_id=dev,
            device_id_type=MESH,
        )
        cp.start()
        self.sent.append(cp)
        return cp


class Gather:
    def __init__(self, buf, send, z, y, use):
        self.buf, self.send, self.use = buf, send, use
        self.first, self.second = (z, y), (y, z)
        self.p1, self.p1f, self.p2, self.p2f = {}, {}, {}, {}

    def place(self, h, f, s):
        return (f % 4, s % 4) if h == 0 else (s % 4, f % 4)

    def at(self, h, df, ds):
        return self.place(h, self.first[h] + df, self.second[h] + ds)

    def move(self, h, df, ds, part, along, d):
        zz, yy = self.at(h, df, ds)
        ref = self.buf.at[h, zz, yy] if part is None else self.buf.at[h, zz, yy, part]
        name = (("z", "y"), ("y", "z"))[h][along]
        me = (self.first[h], self.second[h])[along]
        return self.send(ref, ref, {name: (me + d + 4) % 4})

    def start(self, h, part=None):
        for d in DIRS:
            self.p1.setdefault((h, d), []).append(self.move(h, 0, 0, part, 0, d))
            self.p2.setdefault((h, 0, d), []).append(self.move(h, 0, 0, part, 1, d))

    def own(self, h):
        self.use(h, *self.at(h, 0, 0))

    def near(self, h, d):
        for cp in self.p1[h, d]:
            cp.wait_recv()
        self.p1f[h, d] = self.move(h, 4 - d, 0, PART[d], 0, d)
        for e in DIRS:
            self.p2[h, -d, e] = [self.move(h, 4 - d, 0, None, 1, e)]

    def use_near(self, h, d):
        self.use(h, *self.at(h, 4 - d, 0))

    def pass_on(self, h, j):
        for d in DIRS:
            for cp in self.p2[h, j, d]:
                cp.wait_recv()
            self.p2f[h, j, d] = self.move(h, j + 4, 4 - d, PART[d], 1, d)

    def use_passed(self, h, j):
        for d in DIRS:
            self.use(h, *self.at(h, j + 4, 4 - d))

    def opposite(self, h):
        for d in DIRS:
            self.p1f[h, d].wait_recv()
        for d in DIRS:
            self.p2[h, 2, d] = [self.move(h, 2, 0, None, 1, d)]

    def use_opposite(self, h):
        self.use(h, *self.at(h, 2, 0))

    def last(self, h, j):
        for d in DIRS:
            self.p2f[h, j, d].wait_recv()
        self.use(h, *self.at(h, j + 4, 2))


def layer_kernel(
    tok_hbm, w_hbm, q_gain, k_gain, w_out_hbm, freq,
    mixed, peak, stat_out,
    tok, w_own, w_out, buf, w_far, gains, gains_far, cosf, sinf, acc, acc_far, zb, yb, inv, inv_in,
    q_all, k_all, v_all, q_far, k_far, v_far,
    wz, w_cols, buf2, o_far, acc2, ob, tops, inv_far,
    sc0, sc1, top_r, den_r, acc_r, pace,
    xs, xr, as_, ar, bs, br, ins,
):
    loads = [
        pltpu.make_async_copy(src, dst, ins.at[i])
        for i, (src, dst) in enumerate(((tok_hbm, tok), (w_hbm, w_own), (w_out_hbm, w_out)))
    ]
    for cp in loads:
        cp.start()
    x, xh, xl, co, z, y = here()
    right, left, pair, same = (x + 1) % 4, (x + 3) % 4, 3 - x, xh * 2 + (1 - xl)
    other = {"co": 1 - co}
    peers = (
        [at_x(right), at_x(left), other, at_x(right, 1 - co), at_x(left, 1 - co)]
        + [{"z": (z + i) % 4} for i in (1, 2, 3)]
        + [{"y": (y + i) % 4} for i in (1, 2, 3)]
    )
    with scope("greet"):
        barrier = pltpu.get_barrier_semaphore()
        for dev in peers:
            pl.semaphore_signal(barrier, inc=1, device_id=dev, device_id_type=MESH)
        pl.semaphore_wait(barrier, len(peers))
    send = Sender(xs, xr)
    mine = half_of(x) * 2 + co
    theirs = (1 - half_of(x)) * 2 + co
    me_seq = seq_of(x)
    sub = CROWS // 2

    toks = {}

    def send_tokens(ch):
        for h in (0, 1):
            rows = pl.ds(ch * CROWS + h * sub, sub)
            dst = buf.at[ch, h, z, y, xh]
            toks[ch, h] = (
                send(tok.at[xh, rows], dst, at_x(right)),
                send(tok.at[1 - xh, rows], dst, at_x(left)),
            )

    loads[0].wait()
    send_tokens(0)
    gains[0:1, :] = q_gain[...]
    gains[1:2, :] = k_gain[...]
    loads[1].wait()

    w_rows = pl.ds(pl.multiple_of(co * 2048, 2048), 2048)
    far_w, relayed = {}, {}

    def send_w(j):
        far_w[j] = send(w_own.at[j, w_rows], w_far.at[j, w_rows], at_x(pair))

    def relay(j):
        far_w[j].wait_recv()
        relayed[j] = send(w_far.at[j, w_rows], w_far.at[j, w_rows], other)

    send_w(0)
    send_tokens(1)
    send_w(2)
    send_w(1)
    far_g = send(gains, gains_far, at_x(pair))

    def dots(target, w, ch, h, blocks, zero=False, kinds=(0, 2, 1), at=0):
        lhs, rhs = [], []
        for zz, yy in blocks:
            lhs += [buf[ch, h, zz, yy, 0], buf[ch, h, zz, yy, 1]]
            rows = pl.ds(pl.multiple_of((zz * 4 + yy) * 256, 256), 256)
            some = [w[j, rows, :] for j in kinds]
            rhs.append(some[0] if len(some) == 1 else jnp.concatenate(some, axis=-1))
        lhs = jnp.concatenate(lhs, axis=-1)
        rhs = rhs[0] if len(rhs) == 1 else jnp.concatenate(rhs, axis=0)
        out = jnp.dot(lhs, rhs, preferred_element_type=jnp.float32)
        place = (pl.ds(ch * CROWS + h * sub, sub), slice(at, at + HEAD * len(kinds)))
        target[place] = out if zero else target[place] + out

    def gather_of(ch):
        return Gather(
            buf.at[ch],
            Sender(as_.at[ch], ar.at[ch]),
            z,
            y,
            lambda h, zz, yy: dots(acc, w_own, ch, h, [(zz, yy)]),
        )

    def own_dot(ch, h):
        dots(acc, w_own, ch, h, [(z, y)], True)

    def far_dots(ch, kinds, at):
        for zz in range(4):
            for h in (0, 1):
                blocks = [(zz, yy) for yy in range(4)]
                dots(acc_far, w_far, ch, h, blocks, zz == 0, kinds, at)

    def tables():
        def some(i, carry):
            rows = pl.ds(pl.multiple_of(i * 256, 256), 256)
            p = lax.broadcasted_iota(jnp.int32, (256, HEAD), 0) + (mine * TOK + i * 256)
            lane = lax.broadcasted_iota(jnp.int32, (256, HEAD), 1)
            angle = p.astype(jnp.float32) * freq[...]
            cosf[rows, :] = jnp.cos(angle)
            sine = jnp.sin(angle)
            sinf[rows, :] = jnp.where(lane < HEAD // 2, -sine, sine)
            return carry

        lax.fori_loop(0, TOK // 256, some, 0)

    got = {}

    def squares(ch):
        for j, c in ((0, CQ), (1, CK)):
            cols = pl.ds(c, HEAD)
            for i in range(2):
                rows = pl.ds(ch * CROWS + i * sub, sub)
                a, b = acc[rows, cols], acc_far[rows, cols]
                zb[ch, z, j : j + 1, i * sub : (i + 1) * sub] = jnp.sum(
                    (a * a + b * b).T, axis=0, keepdims=True
                )
        ref = zb.at[ch, z]
        got["z", ch] = [send(ref, ref, {"z": (z + i) % 4}) for i in (1, 2, 3)]

    def totals(ch):
        for cp in got["z", ch]:
            cp.wait_recv()
        yb[ch, y] = (zb[ch, 0] + zb[ch, 1]) + (zb[ch, 2] + zb[ch, 3])
        ref = yb.at[ch, y]
        got["y", ch] = [send(ref, ref, {"y": (y + i) % 4}) for i in (1, 2, 3)]

    stats, invs = [], []
    swaps, near = {}, []

    def turned(a, j, g, rows, col=None):
        t = a[rows, CK : CK + HEAD] if j else a[rows, CQ : CQ + HEAD]
        if col is not None:
            t = t * col
        t = t * g[j : j + 1, :]
        return (t * cosf[rows, :] + pltpu.roll(t, HEAD // 2, 1) * sinf[rows, :]).astype(jnp.bfloat16)

    def early(ch):
        slot = mine * CHUNKS + ch
        whole = pl.ds(ch * CROWS, CROWS)
        for i in range(2):
            here_rows = slice(i * sub, (i + 1) * sub)
            rows = pl.ds(ch * CROWS + i * sub, sub)
            v_far[ch, :, here_rows] = acc_far[rows, CV : CV + HEAD].T.astype(jnp.bfloat16)
        swaps["v", ch] = send(v_far.at[ch], v_all.at[slot], at_x(pair))
        for i in range(2):
            rows = pl.ds(ch * CROWS + i * sub, sub)
            q_far[rows, :] = turned(acc_far, 0, gains_far, rows)
        swaps["q", ch] = send(q_far.at[whole], q_all.at[1, whole], at_x(pair, 1 - co))
        for i in range(2):
            here_rows = slice(i * sub, (i + 1) * sub)
            rows = pl.ds(ch * CROWS + i * sub, sub)
            q_all[0, rows, :] = turned(acc, 0, gains, rows)
            v_all[slot, :, here_rows] = acc[rows, CV : CV + HEAD].T.astype(jnp.bfloat16)
        near.append(send(v_all.at[slot], v_all.at[slot], other))

    def late(ch):
        for cp in got["y", ch]:
            cp.wait_recv()
        inv[ch] = lax.rsqrt(((yb[ch, 0] + yb[ch, 1]) + (yb[ch, 2] + yb[ch, 3])) / WIDTH + EPS)
        slot = mine * CHUNKS + ch
        whole = pl.ds(ch * CROWS, CROWS)
        cols = []
        for i in range(2):
            here_rows = slice(i * sub, (i + 1) * sub)
            rows = pl.ds(ch * CROWS + i * sub, sub)
            cols.append(jnp.broadcast_to(inv[ch, 1:2, here_rows], (HEAD, sub)).T)
            k_far[rows, :] = turned(acc_far, 1, gains_far, rows, cols[i])
        swaps["k", ch] = send(k_far.at[whole], k_all.at[slot], at_x(pair))
        invs.append(send(inv.at[ch], inv_far.at[ch], at_x(pair, 1 - co)))
        for i in range(2):
            here_rows = slice(i * sub, (i + 1) * sub)
            rows = pl.ds(ch * CROWS + i * sub, sub)
            k_all[slot, here_rows, :] = turned(acc, 1, gains, rows, cols[i])
        near.append(send(k_all.at[slot], k_all.at[slot], other))
        for dev in (right, left):
            stats.append(send(inv.at[ch], inv_in.at[me_seq, ch], at_x(dev)))

    def relay_kv(name, ch):
        slot = theirs * CHUNKS + ch
        ref = k_all if name == "k" else v_all
        swaps[name, ch].wait_recv()
        near.append(send(ref.at[slot], ref.at[slot], other))

    part = pl.ds(pl.multiple_of(co * 64, 64), 64)

    def z_cols(zz):
        return pl.ds(pl.multiple_of((zz % 4) * 1024, 1024), 1024)

    def y_cols(yy):
        return pl.ds(pl.multiple_of((yy % 4) * 256, 256), 256)

    def cols_z():
        wz[z] = w_out[part, z_cols(z)]
        got["wz"] = [
            send(w_out.at[part, z_cols(z + i)], wz.at[z], {"z": (z + i) % 4}) for i in (1, 2, 3)
        ]

    def cols_y():
        for cp in got["wz"]:
            cp.wait_recv()
        w_cols[:, y, xh, part, :] = wz[:, :, y_cols(y)]
        got["wy"] = [
            send(wz.at[:, :, y_cols(y + i)], w_cols.at[:, y, xh, part], {"y": (y + i) % 4})
            for i in (1, 2, 3)
        ]

    def cols_y_done():
        for cp in got["wy"]:
            cp.wait_recv()

    def cols_x(i):
        ref = w_cols.at[2 * i : 2 * i + 2, :, xh, part]
        got["wx", i] = send(ref, ref, at_x(pair))

    def cols_core(i):
        got["wx", i].wait_recv()
        ref = w_cols.at[2 * i : 2 * i + 2, :, :, part]
        got["wc", i] = send(ref, ref, other)

    g = [gather_of(0), gather_of(1)]

    def begin(ch):
        for h in (0, 1):
            for cp in toks[ch, h]:
                cp.wait_recv()
            g[ch].start(h)

    def middle(ch):
        for h in (0, 1):
            own_dot(ch, h)
        for d in DIRS:
            for h in (0, 1):
                g[ch].near(h, d)
        for d in DIRS:
            for h in (0, 1):
                g[ch].use_near(h, d)
        for h in (0, 1):
            g[ch].pass_on(h, 0)
        for h in (0, 1):
            g[ch].opposite(h)
        for h in (0, 1):
            g[ch].use_passed(h, 0)
            g[ch].use_opposite(h)
        for h in (0, 1):
            g[ch].pass_on(h, -1)
        for h in (0, 1):
            g[ch].use_passed(h, -1)
        for h in (0, 1):
            g[ch].pass_on(h, 1)

    def drain(ch, j):
        for h in (0, 1):
            g[ch].last(h, j)

    with scope("begin0"):
        begin(0)
    with scope("tables"):
        tables()
    with scope("middle0"):
        middle(0)
    with scope("begin1"):
        begin(1)
    with scope("pass0"):
        for h in (0, 1):
            g[0].pass_on(h, 2)
        for h in (0, 1):
            g[0].use_passed(h, 1)
        for h in (0, 1):
            own_dot(1, h)
    with scope("near1"):
        for d in DIRS:
            for h in (0, 1):
                g[1].near(h, d)
    with scope("drain0"):
        for h in (0, 1):
            g[0].use_passed(h, 2)
        for j in (0, -1, 1):
            drain(0, j)
    with scope("middle1"):
        for h in (0, 1):
            g[1].pass_on(h, 0)
        drain(0, 2)
        for d in DIRS:
            for h in (0, 1):
                g[1].use_near(h, d)
        for h in (0, 1):
            g[1].opposite(h)
        relay(0)
    with scope("mid1"):
        for h in (0, 1):
            g[1].use_passed(h, 0)
            g[1].use_opposite(h)
        for h in (0, 1):
            g[1].pass_on(h, -1)
        relay(2)
        for h in (0, 1):
            g[1].use_passed(h, -1)
    with scope("pass1"):
        for h in (0, 1):
            g[1].pass_on(h, 1)
        for h in (0, 1):
            g[1].use_passed(h, 1)
        for j in (0, 2):
            relayed[j].wait_recv()
        far_g.wait_recv()
    with scope("far_qv0"):
        far_dots(0, (0, 2), 0)
    with scope("pass1b"):
        for h in (0, 1):
            g[1].pass_on(h, 2)
    with scope("early0"):
        early(0)
        for h in (0, 1):
            g[1].use_passed(h, 2)
    with scope("drain1"):
        for j in (0, -1, 1):
            drain(1, j)
    with scope("relay_k"):
        relay(1)
    with scope("drain1b"):
        drain(1, 2)
    with scope("far_qv1"):
        far_dots(1, (0, 2), 0)
    with scope("early1"):
        early(1)
        relayed[1].wait_recv()
    with scope("far_k"):
        far_dots(0, (1,), CK)
        squares(0)
        far_dots(1, (1,), CK)
        squares(1)
    with scope("tot"):
        totals(0)
        totals(1)
        loads[2].wait()
        cols_z()
        relay_kv("v", 0)
    with scope("late"):
        late(0)
        late(1)
    with scope("relay_kv"):
        relay_kv("v", 1)
        cols_y()
        relay_kv("k", 0)
        relay_kv("k", 1)
    with scope("swap_wait"):
        for ch in range(CHUNKS):
            swaps["q", ch].wait_recv()
        for cp in invs + near:
            cp.wait_recv()

    far_quarter = (1 - half_of(x)) * 2 + (1 - co)
    back = {}

    def attend(ch):
        total = 6 + 2 * (ch + 1)
        count = far_quarter * CHUNKS + ch + 1
        rows = slice(ch * CROWS, (ch + 1) * CROWS)
        for i, r in enumerate((inv, inv_far)):
            pace[i] = r[ch, 0:1, :] * (SCALE * LOG2E)
        top_r[...] = jnp.full((2, 1, CROWS), NEG, jnp.float32)
        den_r[...] = jnp.zeros((2, 1, CROWS), jnp.float32)
        acc_r[...] = jnp.zeros((2, HEAD, CROWS), jnp.float32)

        def where(t):
            own = (t + 16 - count) // 16
            return 1 - own, (1 - own) * (count - 1 - t) + own * (t - count)

        def score(t, into):
            which, j = where(t)
            into[...] = lax.dot_general(
                k_all[j], q_all[which, rows, :], (((1,), (1,)), ((), ())),
                preferred_element_type=jnp.float32,
            )

        def weigh(t, cur, masked):
            which, j = where(t)
            s = cur[...]
            if masked:
                r = lax.broadcasted_iota(jnp.int32, (BK, CROWS), 0)
                c = lax.broadcasted_iota(jnp.int32, (BK, CROWS), 1)
                s = jnp.where(r <= c, s, NEG)
            top, p = top_r[which], pace[which]
            new = jnp.maximum(top, jnp.max(s, axis=0, keepdims=True))
            e = jnp.exp2((s - new) * p)
            keep = jnp.exp2((top - new) * p)
            den_r[which] = den_r[which] * keep + jnp.sum(e, axis=0, keepdims=True)
            acc_r[which] = acc_r[which] * keep + jnp.dot(
                v_all[j], e.astype(jnp.bfloat16), preferred_element_type=jnp.float32
            )
            top_r[which] = new

        score(0, sc0)
        score(1, sc1)
        weigh(0, sc0, True)

        def two(i, carry):
            t = 2 * i + 1
            score(t + 1, sc0)
            weigh(t, sc1, False)
            score(t + 2, sc1)
            weigh(t + 1, sc0, False)
            return carry

        lax.fori_loop(0, (total - 2) // 2, two, 0)
        weigh(total - 1, sc1, True)
        o_far[ch] = (acc_r[1] / den_r[1]).T.astype(jnp.bfloat16)
        back[ch] = send(o_far.at[ch], buf2.at[ch, z, y, xh], at_x(pair, 1 - co))
        buf2[ch, z, y, xh] = (acc_r[0] / den_r[0]).T.astype(jnp.bfloat16)
        peaks_here = [jnp.max(top_r[i] * pace[i], axis=1, keepdims=True) for i in (0, 1)]
        return jnp.maximum(*peaks_here) * (1 / LOG2E)

    def use2(h, zz, yy, zero=False):
        lhs = jnp.concatenate([buf2[h, zz, yy, 0], buf2[h, zz, yy, 1]], axis=-1)
        rhs = jnp.concatenate([w_cols[zz, yy, 0], w_cols[zz, yy, 1]], axis=0)
        out = jnp.dot(lhs, rhs, preferred_element_type=jnp.float32)
        rows = pl.ds(h * CROWS, CROWS)
        acc2[rows, :] = out if zero else acc2[rows, :] + out

    g2 = Gather(buf2, Sender(bs, br), z, y, use2)
    with scope("attend0"):
        best = [attend(0)]
        g2.start(0, xh)
    with scope("attend1"):
        best.append(attend(1))
        g2.start(1, xh)
    with scope("start2_0"):
        back[0].wait_recv()
        g2.start(0, 1 - xh)
        cols_y_done()
        cols_x(0)
        cols_x(1)
    with scope("start2_1"):
        back[1].wait_recv()
        g2.start(1, 1 - xh)
        place = xl * 2 + co
        tops[place] = jnp.broadcast_to(jnp.maximum(*best), (8, HEAD))
        peaks = [
            send(tops.at[place], tops.at[place], dev)
            for dev in (other, at_x(same), at_x(same, 1 - co))
        ]
    with scope("near2_0"):
        for d in DIRS:
            g2.near(0, d)
    with scope("near2_1"):
        for d in DIRS:
            g2.near(1, d)
        cols_core(0)
    with scope("pass2_0"):
        g2.pass_on(0, 0)
        g2.opposite(0)
        g2.pass_on(1, 0)
        g2.opposite(1)
        cols_core(1)
    with scope("pass2_1"):
        g2.pass_on(0, -1)
        for i in (0, 1):
            got["wc", i].wait_recv()
        for h in (0, 1):
            use2(h, z, y, True)
        for d in DIRS:
            g2.use_near(0, d)
        g2.pass_on(1, -1)
        for d in DIRS:
            g2.use_near(1, d)
        g2.use_passed(0, 0)
    with scope("mid2"):
        g2.pass_on(0, 1)
        g2.use_passed(1, 0)
        for h in (0, 1):
            g2.use_opposite(h)
        g2.pass_on(1, 1)
        for h in (0, 1):
            g2.use_passed(h, -1)
    with scope("pass2"):
        g2.pass_on(0, 2)
        g2.use_passed(0, 1)
        g2.pass_on(1, 2)
        g2.use_passed(1, 1)
        for h in (0, 1):
            g2.use_passed(h, 2)
    fin = []
    with scope("drain2"):
        for j in (0, -1, 1):
            for h in (0, 1):
                g2.last(h, j)
        for h in (0, 1):
            g2.last(h, 2)
            rows = pl.ds(h * CROWS, CROWS)
            for i in (0, 1):
                ob[i, rows, :] = acc2[rows, i * HEAD : (i + 1) * HEAD].astype(jnp.bfloat16)
            for dev in (right, left):
                fin.append(send(ob.at[dev // 2, rows], mixed.at[me_seq, rows], at_x(dev)))
    with scope("final"):
        for cp in peaks:
            cp.wait_recv()
        peak[...] = jnp.maximum(jnp.maximum(tops[0], tops[1]), jnp.maximum(tops[2], tops[3]))
        for cp in stats:
            cp.wait_recv()
        for s in (0, 1):
            for ch in range(CHUNKS):
                stat_out[:, s, ch * CROWS : (ch + 1) * CROWS] = inv_in[s, ch]
        for cp in fin:
            cp.wait_recv()
    with scope("wait_send"):
        for s in (send, g[0].send, g[1].send, g2.send):
            for cp in s.sent:
                cp.wait_send()


def finish_kernel(mixed, peak, stat, mixed_out, peak_out, stat_out):
    mixed_out[...] = mixed[...]
    peak_out[0] = peak[0, 0]
    stat_out[...] = stat[...]


def vmem(count):
    return [pl.BlockSpec(memory_space=pltpu.VMEM)] * count


def shards(tokens, w_qkv, q_gain, k_gain, w_out):
    bf, f32 = jnp.bfloat16, jnp.float32
    dma = pltpu.SemaphoreType.DMA
    sub = CROWS // 2
    freq = ROPE_BASE ** (-(np.arange(HEAD) % (HEAD // 2) * 2.0) / HEAD)
    mixed, peak, stat = pl.pallas_call(
        layer_kernel,
        out_shape=(
            jax.ShapeDtypeStruct((2, TOK, HEAD), bf),
            jax.ShapeDtypeStruct((8, HEAD), f32),
            jax.ShapeDtypeStruct((2, 2, TOK), f32),
        ),
        in_specs=[
            pl.BlockSpec(memory_space=pltpu.VMEM if small else pl.ANY)
            for small in (False, False, True, True, False, True)
        ],
        out_specs=tuple(vmem(3)),
        scratch_shapes=[
            pltpu.VMEM((2, TOK, HEAD), bf),
            pltpu.VMEM((3, WIDTH, HEAD), bf),
            pltpu.VMEM((HEAD, WIDTH), bf),
            pltpu.VMEM((CHUNKS, 2, 4, 4, 2, sub, HEAD), bf),
            pltpu.VMEM((3, WIDTH, HEAD), bf),
            pltpu.VMEM((8, HEAD), f32),
            pltpu.VMEM((8, HEAD), f32),
            pltpu.VMEM((TOK, HEAD), f32),
            pltpu.VMEM((TOK, HEAD), f32),
            pltpu.VMEM((TOK, 3 * HEAD), f32),
            pltpu.VMEM((TOK, 3 * HEAD), f32),
            pltpu.VMEM((CHUNKS, 4, 2, CROWS), f32),
            pltpu.VMEM((CHUNKS, 4, 2, CROWS), f32),
            pltpu.VMEM((CHUNKS, 2, CROWS), f32),
            pltpu.VMEM((2, CHUNKS, 2, CROWS), f32),
            pltpu.VMEM((2, TOK, HEAD), bf),
            pltpu.VMEM((4 * CHUNKS, CROWS, HEAD), bf),
            pltpu.VMEM((4 * CHUNKS, HEAD, CROWS), bf),
            pltpu.VMEM((TOK, HEAD), bf),
            pltpu.VMEM((TOK, HEAD), bf),
            pltpu.VMEM((CHUNKS, HEAD, CROWS), bf),
            pltpu.VMEM((4, 64, 1024), bf),
            pltpu.VMEM((4, 4, 2, HEAD, 256), bf),
            pltpu.VMEM((2, 4, 4, 2, CROWS, HEAD), bf),
            pltpu.VMEM((2, CROWS, HEAD), bf),
            pltpu.VMEM((TOK, 256), f32),
            pltpu.VMEM((2, TOK, HEAD), bf),
            pltpu.VMEM((4, 8, HEAD), f32),
            pltpu.VMEM((CHUNKS, 2, CROWS), f32),
            pltpu.VMEM((BK, CROWS), f32),
            pltpu.VMEM((BK, CROWS), f32),
            pltpu.VMEM((2, 1, CROWS), f32),
            pltpu.VMEM((2, 1, CROWS), f32),
            pltpu.VMEM((2, HEAD, CROWS), f32),
            pltpu.VMEM((2, 1, CROWS), f32),
            dma((72,)),
            dma((72,)),
            dma((CHUNKS, 40)),
            dma((CHUNKS, 40)),
            dma((48,)),
            dma((48,)),
            dma((3,)),
        ],
        compiler_params=pltpu.CompilerParams(
            collective_id=0, has_side_effects=True, vmem_limit_bytes=VMEM_CAP
        ),
        name="layer",
    )(
        tokens,
        w_qkv.transpose(1, 0, 2),
        q_gain[None],
        k_gain[None],
        w_out,
        jnp.asarray(freq[None], f32),
    )
    return pl.pallas_call(
        finish_kernel,
        out_shape=(
            jax.ShapeDtypeStruct((2, TOK, HEAD), bf),
            jax.ShapeDtypeStruct((1,), f32),
            jax.ShapeDtypeStruct((2, 2, TOK), f32),
        ),
        in_specs=vmem(3),
        out_specs=(
            pl.BlockSpec(memory_space=pltpu.VMEM),
            pl.BlockSpec(memory_space=pltpu.SMEM),
            pl.BlockSpec(memory_space=pltpu.VMEM),
        ),
        name="finish",
    )(mixed, peak, stat)


def solution(mesh):
    finer = Mesh(mesh.devices.reshape(2, 2, 4, 4, 2), ("xl", "co", "z", "y", "xh"))
    tensor = ("z", "y", "xh")
    seq = ("xl", "co")
    placed = (P(None, seq, tensor), P(None, None, tensor), P(tensor), P(tensor), P(tensor, None))
    return jax.shard_map(
        shards,
        mesh=finer,
        in_specs=placed,
        out_specs=(P(None, seq, tensor), P(tensor), P(None, None, seq)),
        check_vma=False,
    )
```

```python
import contextlib
import math

import jax
import jax.numpy as jnp
import numpy as np
from jax import lax
from jax.experimental import pallas as pl
from jax.experimental.pallas import tpu as pltpu
from jax.sharding import Mesh
from jax.sharding import PartitionSpec as P

EPS = 1e-06
ROPE_BASE = 500000.0
NEG = -1e30
MESH = pl.DeviceIdType.MESH
HEAD = 128
TOK = 1024
CHUNKS = 2
CROWS = TOK // CHUNKS
WIDTH = 4096
BK = 512
VMEM_CAP = 60 * 1024 * 1024
SCALE = HEAD ** (-0.5)
LOG2E = math.log2(math.e)
DIRS = (1, -1)
PART = {1: 0, -1: 1}
CQ, CV, CK = 0, HEAD, 2 * HEAD


def scope(name):
    return contextlib.nullcontext()


def here():
    xh, xl = lax.axis_index("xh"), lax.axis_index("xl")
    return xh * 2 + xl, xh, xl, lax.axis_index("co"), lax.axis_index("z"), lax.axis_index("y")


def seq_of(x):
    return 1 - ((x + 1) // 2) % 2


def half_of(x):
    return 1 - x % 2


def at_x(x, core=None):
    dev = {"xl": x % 2, "xh": x // 2}
    if core is not None:
        dev["co"] = core
    return dev


class Sender:
    def __init__(self, ssem, rsem, region):
        self.ssem, self.rsem, self.region = ssem, rsem, region
        self.groups, self.keys = {}, {}
        self.leaving, self.arriving = {}, {}

    def __call__(self, src, dst, dev, group, key):
        g = self.groups.setdefault(group, len(self.groups))
        k = self.keys.setdefault(key, len(self.keys))
        size = math.prod(src.shape) * jnp.dtype(src.dtype).itemsize
        self.leaving[group] = self.leaving.get(group, 0) + size
        self.arriving[key] = self.arriving.get(key, 0) + size
        pltpu.make_async_remote_copy(
            src_ref=src,
            dst_ref=dst,
            send_sem=self.ssem.at[g],
            recv_sem=self.rsem.at[k],
            device_id=dev,
            device_id_type=MESH,
        ).start()

    def wait(self, *key):
        ref = self.region(self.arriving.pop(key))
        pltpu.make_async_copy(ref, ref, self.rsem.at[self.keys[key]]).wait()

    def flush(self):
        assert not self.arriving, self.arriving
        for group, size in self.leaving.items():
            ref = self.region(size)
            pltpu.make_async_copy(ref, ref, self.ssem.at[self.groups[group]]).wait()


class Gather:
    def __init__(self, name, buf, send, z, y, use):
        self.name, self.buf, self.send, self.use = name, buf, send, use
        self.first, self.second = (z, y), (y, z)

    def place(self, h, f, s):
        return (f % 4, s % 4) if h == 0 else (s % 4, f % 4)

    def at(self, h, df, ds):
        return self.place(h, self.first[h] + df, self.second[h] + ds)

    def move(self, h, df, ds, part, along, d, *key):
        zz, yy = self.at(h, df, ds)
        ref = self.buf.at[h, zz, yy] if part is None else self.buf.at[h, zz, yy, part]
        name = (("z", "y"), ("y", "z"))[h][along]
        me = (self.first[h], self.second[h])[along]
        self.send(ref, ref, {name: (me + d + 4) % 4}, self.name, (self.name, h, *key))

    def wait(self, h, *key):
        self.send.wait(self.name, h, *key)

    def start(self, h, part=None):
        for d in DIRS:
            self.move(h, 0, 0, part, 0, d, "p1", d)
            self.move(h, 0, 0, part, 1, d, "p2", 0, d)

    def near(self, h, d):
        self.wait(h, "p1", d)
        self.move(h, 4 - d, 0, PART[d], 0, d, "p1f")
        for e in DIRS:
            self.move(h, 4 - d, 0, None, 1, e, "p2", -d, e)

    def use_near(self, h, d):
        self.use(h, *self.at(h, 4 - d, 0))

    def pass_on(self, h, j):
        for d in DIRS:
            self.wait(h, "p2", j, d)
            self.move(h, j + 4, 4 - d, PART[d], 1, d, "p2f", j)

    def use_passed(self, h, j):
        for d in DIRS:
            self.use(h, *self.at(h, j + 4, 4 - d))

    def opposite(self, h):
        self.wait(h, "p1f")
        for d in DIRS:
            self.move(h, 2, 0, None, 1, d, "p2", 2, d)

    def use_opposite(self, h):
        self.use(h, *self.at(h, 2, 0))

    def last(self, h, j):
        self.wait(h, "p2f", j)
        self.use(h, *self.at(h, j + 4, 2))


def layer_kernel(
    tok_hbm, w_hbm, q_gain, k_gain, w_out_hbm, freq,
    mixed, peak, stat_out,
    tok, w_own, w_out, buf, w_far, gains, gains_far, cosf, sinf, acc, acc_far, zb, yb, inv, inv_in,
    q_all, k_all, v_all, q_far, k_far, v_far,
    wz, w_cols, buf2, o_far, acc2, ob, tops,
    sc0, sc1, top_r, den_r, acc_r, pace, k_norm,
    ssem, rsem, ins,
):
    loads = [
        pltpu.make_async_copy(src, dst, ins.at[i])
        for i, (src, dst) in enumerate(((tok_hbm, tok), (w_hbm, w_own), (w_out_hbm, w_out)))
    ]
    for cp in loads:
        cp.start()
    x, xh, xl, co, z, y = here()
    right, left, pair, same = (x + 1) % 4, (x + 3) % 4, 3 - x, xh * 2 + (1 - xl)
    other = {"co": 1 - co}
    peers = (
        [other] + [at_x((x + i) % 4, cc) for i in (1, 2, 3) for cc in (co, 1 - co)]
        + [{"z": (z + i) % 4} for i in (1, 2, 3)]
        + [{"y": (y + i) % 4} for i in (1, 2, 3)]
    )
    with scope("greet"):
        barrier = pltpu.get_barrier_semaphore()
        for dev in peers:
            pl.semaphore_signal(barrier, inc=1, device_id=dev, device_id_type=MESH)
        pl.semaphore_wait(barrier, len(peers))

    def region(size):
        for n in (1, 2, 3):
            if size % (n * 4096) == 0 and size <= n * WIDTH * HEAD * 2:
                return w_far.at[0:n, 0 : size // (n * HEAD * 2)]
        rows, rest = divmod(size, 64 * HEAD * 2)
        assert rest == 0 and rows % 16 == 0 and rows <= CROWS // 2, size
        return buf.at[0, :, :, :, :, 0:rows]

    send = Sender(ssem, rsem, region)
    sub = CROWS // 2

    def eighth(xx, cc):
        return 4 * half_of(xx) + 2 * cc + seq_of(xx)

    mine, far_tile = eighth(x, co), eighth(pair, 1 - co)
    part_of_mine = pl.ds(pl.multiple_of(seq_of(x) * CROWS, CROWS), CROWS)

    def send_tokens(ch):
        for h in (0, 1):
            dst = buf.at[ch, h, z, y, xh]
            for part, dev in ((xh, right), (1 - xh, left)):
                src = tok.at[ch, pl.ds(pl.multiple_of(part * CROWS + h * sub, sub), sub)]
                send(src, dst, at_x(dev), "rows", ("tok", ch, h))

    loads[0].wait()
    send_tokens(0)
    gains[0:1, :] = q_gain[...]
    gains[1:2, :] = k_gain[...]
    loads[1].wait()

    def w_rows(xx):
        return pl.ds(pl.multiple_of(((xx % 2) * 2 + co) * 1024, 1024), 1024)

    def send_w(j):
        send(w_own.at[j, w_rows(x)], w_far.at[j, w_rows(x)], at_x(pair), "w", ("far_w", j))

    def relay_w(j):
        send.wait("far_w", j)
        ref = w_far.at[j, w_rows(pair)]
        send(ref, ref, at_x(same), "w", ("same_w", j))
        send(ref, ref, other, "w", ("relayed", j == 1))

    def relay_w2(j):
        send.wait("same_w", j)
        ref = w_far.at[j, w_rows(pair + 1)]
        send(ref, ref, other, "w", ("relayed", j == 1))

    send_w(0)
    send_w(2)
    send_tokens(1)
    send_w(1)
    send(gains, gains_far, at_x(pair), "small", ("gains",))

    def dots(target, w, ch, h, blocks, zero=False, kinds=(0, 2, 1), at=0):
        lhs, rhs = [], []
        for zz, yy in blocks:
            lhs += [buf[ch, h, zz, yy, 0], buf[ch, h, zz, yy, 1]]
            rows = pl.ds(pl.multiple_of((zz * 4 + yy) * 256, 256), 256)
            some = [w[j, rows, :] for j in kinds]
            rhs.append(some[0] if len(some) == 1 else jnp.concatenate(some, axis=-1))
        lhs = jnp.concatenate(lhs, axis=-1)
        rhs = rhs[0] if len(rhs) == 1 else jnp.concatenate(rhs, axis=0)
        out = jnp.dot(lhs, rhs, preferred_element_type=jnp.float32)
        place = (pl.ds(ch * CROWS + h * sub, sub), slice(at, at + HEAD * len(kinds)))
        target[place] = out if zero else target[place] + out

    def gather_of(ch):
        return Gather(
            ("tokens", ch), buf.at[ch], send, z, y, lambda h, zz, yy: dots(acc, w_own, ch, h, [(zz, yy)])
        )

    def own_dot(ch, h):
        dots(acc, w_own, ch, h, [(z, y)], True)

    def far_dots(ch, kinds, at, lines=(0, 1, 3, 2)):
        for i in lines:
            for h in (0, 1):
                blocks = [g[ch].at(h, f, i) for f in range(4)]
                dots(acc_far, w_far, ch, h, blocks, i == 0, kinds, at)

    def tables():
        def some(i, carry):
            rows = pl.ds(pl.multiple_of(i * 256, 256), 256)
            p = lax.broadcasted_iota(jnp.int32, (256, HEAD), 0) + (mine * CROWS + i * 256)
            lane = lax.broadcasted_iota(jnp.int32, (256, HEAD), 1)
            angle = p.astype(jnp.float32) * freq[...]
            cosf[rows, :] = jnp.cos(angle)
            sine = jnp.sin(angle)
            sinf[rows, :] = jnp.where(lane < HEAD // 2, -sine, sine)
            return carry

        lax.fori_loop(0, CROWS // 256, some, 0)

    def squares(ch):
        for j, c in ((0, CQ), (1, CK)):
            cols = pl.ds(c, HEAD)
            for i in range(2):
                rows = pl.ds(ch * CROWS + i * sub, sub)
                a, b = acc[rows, cols], acc_far[rows, cols]
                zb[ch, z, j : j + 1, i * sub : (i + 1) * sub] = jnp.sum(
                    (a * a + b * b).T, axis=0, keepdims=True
                )
        ref = zb.at[ch, z]
        for i in (1, 2, 3):
            send(ref, ref, {"z": (z + i) % 4}, "small", ("zsum", ch))

    def totals(ch):
        send.wait("zsum", ch)
        yb[ch, y] = (zb[ch, 0] + zb[ch, 1]) + (zb[ch, 2] + zb[ch, 3])
        ref = yb.at[ch, y]
        for i in (1, 2, 3):
            send(ref, ref, {"y": (y + i) % 4}, "small", ("ysum", ch))

    def turned(a, j, g, ch, i):
        rows = pl.ds(ch * CROWS + i * sub, sub)
        t = a[rows, CK : CK + HEAD] if j else a[rows, CQ : CQ + HEAD]
        t = t * g[j : j + 1, :]
        table = slice(i * sub, (i + 1) * sub)
        return (t * cosf[table, :] + pltpu.roll(t, HEAD // 2, 1) * sinf[table, :]).astype(
            jnp.bfloat16
        )

    def give(name, ch, far, all_):
        slot = all_.at[ch, mine]
        send(far.at[ch], slot, at_x(pair), name, ("pair", name, ch))
        send(slot, slot, at_x(same), name, ("same", name, ch))
        send(slot, slot, other, name, ("near", ch))

    def take_pair(name, ch):
        ref = (k_all if name == "k" else v_all).at[ch, eighth(pair, co)]
        send.wait("pair", name, ch)
        send(ref, ref, at_x(same), name, ("fwd", name, ch))
        send(ref, ref, other, name, ("near", ch))

    def take_same(name, ch):
        ref = (k_all if name == "k" else v_all).at[ch, eighth(same, co)]
        send.wait("same", name, ch)
        send(ref, ref, other, name, ("near", ch))

    def take_fwd(name, ch):
        ref = (k_all if name == "k" else v_all).at[ch, eighth((x + 2) % 4, co)]
        send.wait("fwd", name, ch)
        send(ref, ref, other, name, ("near", ch))

    def values(ch):
        for i in range(2):
            here_rows = slice(i * sub, (i + 1) * sub)
            rows = pl.ds(ch * CROWS + i * sub, sub)
            v_far[ch, :, here_rows] = acc_far[rows, CV : CV + HEAD].T.astype(jnp.bfloat16)
            v_all[ch, mine, :, here_rows] = acc[rows, CV : CV + HEAD].T.astype(jnp.bfloat16)
        give("v", ch, v_far, v_all)

    def keys(ch):
        for i in range(2):
            here_rows = slice(i * sub, (i + 1) * sub)
            k_far[ch, here_rows, :] = turned(acc_far, 1, gains_far, ch, i)
            k_all[ch, mine, here_rows, :] = turned(acc, 1, gains, ch, i)
        give("k", ch, k_far, k_all)

    def queries(ch):
        for i in range(2):
            q_far[ch, i * sub : (i + 1) * sub, :] = turned(acc_far, 0, gains_far, ch, i)
        send(q_far.at[ch], q_all.at[ch, 1], at_x(pair, 1 - co), "rows", ("q", ch))
        for i in range(2):
            q_all[ch, 0, i * sub : (i + 1) * sub, :] = turned(acc, 0, gains, ch, i)

    def norms(ch):
        send.wait("ysum", ch)
        inv[ch, mine] = lax.rsqrt(
            ((yb[ch, 0] + yb[ch, 1]) + (yb[ch, 2] + yb[ch, 3])) / WIDTH + EPS
        )
        ref = inv.at[ch, mine]
        opposite = (x + 2) % 4
        for dev in (
            at_x(pair), at_x(pair, 1 - co), at_x(same), at_x(same, 1 - co),
            at_x(opposite), at_x(opposite, 1 - co), other,
        ):
            send(ref, ref, dev, "small", ("scale", ch))
        for dev in (right, left):
            send(ref, inv_in.at[ch, seq_of(x)], at_x(dev), "small", ("stats",))

    part = pl.ds(pl.multiple_of(co * 64, 64), 64)
    strip = pl.ds(pl.multiple_of((co * 2 + x % 2) * 32, 32), 32)

    def z_cols(zz):
        return pl.ds(pl.multiple_of((zz % 4) * 1024, 1024), 1024)

    def y_cols(yy):
        return pl.ds(pl.multiple_of((yy % 4) * 256, 256), 256)

    def cols_z():
        wz[z] = w_out[strip, z_cols(z)]
        for i in (1, 2, 3):
            send(
                w_out.at[strip, z_cols(z + i)], wz.at[z], {"z": (z + i) % 4}, "cols", ("wz",)
            )

    def cols_y():
        send.wait("wz")
        w_cols[:, y, xh, strip, :] = wz[:, :, y_cols(y)]
        for i in (1, 2, 3):
            send(
                wz.at[:, :, y_cols(y + i)],
                w_cols.at[:, y, xh, strip],
                {"y": (y + i) % 4},
                "cols",
                ("wy",),
            )

    def cols_same():
        send.wait("wy")
        ref = w_cols.at[:, :, xh, strip]
        send(ref, ref, at_x(same), "cols", ("ws",))

    def cols_x(i):
        ref = w_cols.at[2 * i : 2 * i + 2, :, xh, part]
        send(ref, ref, at_x(pair), "cols", ("wx", i))

    def cols_core(i):
        send.wait("wx", i)
        ref = w_cols.at[2 * i : 2 * i + 2, :, :, part]
        send(ref, ref, other, "core", ("wc",))

    best = []

    def columns(ch):
        def column(e, carry):
            for i in range(CROWS // HEAD):
                lanes = slice(i * HEAD, (i + 1) * HEAD)
                k_norm[e, lanes, :] = jnp.broadcast_to(inv[ch, e, 1:2, lanes], (HEAD, HEAD)).T
            return carry

        lax.fori_loop(0, 8, column, 0)

    def attend(ch):
        count = far_tile + 1
        total = count + mine + 1
        for i, e in enumerate((mine, far_tile)):
            pace[i] = inv[ch, e, 0:1, :] * (SCALE * LOG2E)

        top_r[...] = jnp.full((2, 1, CROWS), NEG, jnp.float32)
        den_r[...] = jnp.zeros((2, 1, CROWS), jnp.float32)
        acc_r[...] = jnp.zeros((2, HEAD, CROWS), jnp.float32)

        def where(t):
            own = (t + 16 - count) // 16
            return 1 - own, (1 - own) * (count - 1 - t) + own * (t - count)

        def score(t, into):
            which, j = where(t)
            raw = lax.dot_general(
                k_all[ch, j], q_all[ch, which], (((1,), (1,)), ((), ())),
                preferred_element_type=jnp.float32,
            )
            into[...] = raw * jnp.concatenate([k_norm[j]] * (CROWS // HEAD), axis=-1)

        def weigh(t, cur, masked):
            which, j = where(t)
            s = cur[...]
            if masked:
                r = lax.broadcasted_iota(jnp.int32, (BK, CROWS), 0)
                c = lax.broadcasted_iota(jnp.int32, (BK, CROWS), 1)
                s = jnp.where(r <= c, s, NEG)
            top, p = top_r[which], pace[which]
            new = jnp.maximum(top, jnp.max(s, axis=0, keepdims=True))
            e = jnp.exp2((s - new) * p)
            keep = jnp.exp2((top - new) * p)
            den_r[which] = den_r[which] * keep + jnp.sum(e, axis=0, keepdims=True)
            acc_r[which] = acc_r[which] * keep + jnp.dot(
                v_all[ch, j], e.astype(jnp.bfloat16), preferred_element_type=jnp.float32
            )
            top_r[which] = new

        score(0, sc0)
        score(1, sc1)
        weigh(0, sc0, True)

        def two(i, carry):
            t = 2 * i + 1
            score(t + 1, sc0)
            weigh(t, sc1, False)
            score(t + 2, sc1)
            weigh(t + 1, sc0, False)
            return carry

        lax.fori_loop(0, 3 + seq_of(x), two, 0)
        weigh(total - 1, sc1, True)
        for h in (0, 1):
            o_far[ch, h] = (
                (acc_r[1, :, h * sub : (h + 1) * sub] / den_r[1, :, h * sub : (h + 1) * sub])
                .T.astype(jnp.bfloat16)
            )
            dst = buf2.at[ch, h, z, y, xh]
            send(o_far.at[ch, h], dst, at_x(pair, 1 - co), "rows", ("back", ch, h))
        for h in (0, 1):
            buf2[ch, h, z, y, xh] = (
                (acc_r[0, :, h * sub : (h + 1) * sub] / den_r[0, :, h * sub : (h + 1) * sub])
                .T.astype(jnp.bfloat16)
            )
            g2[ch].start(h, xh)
        peaks_here = [jnp.max(top_r[i] * pace[i], axis=1, keepdims=True) for i in (0, 1)]
        best.append(jnp.maximum(*peaks_here) * (1 / LOG2E))

    def start_far(ch):
        for h in (0, 1):
            send.wait("back", ch, h)
            g2[ch].start(h, 1 - xh)

    def use2(ch, h, zz, yy, zero=False):
        lhs = jnp.concatenate([buf2[ch, h, zz, yy, 0], buf2[ch, h, zz, yy, 1]], axis=-1)
        rhs = jnp.concatenate([w_cols[zz, yy, 0], w_cols[zz, yy, 1]], axis=0)
        out = jnp.dot(lhs, rhs, preferred_element_type=jnp.float32)
        rows = pl.ds(ch * CROWS + h * sub, sub)
        acc2[rows, :] = out if zero else acc2[rows, :] + out

    g = [gather_of(0), gather_of(1)]
    g2 = [
        Gather(
            ("attended", ch),
            buf2.at[ch],
            send,
            z,
            y,
            lambda h, zz, yy, ch=ch: use2(ch, h, zz, yy),
        )
        for ch in (0, 1)
    ]

    def finish(ch, h):
        rows = pl.ds(ch * CROWS + h * sub, sub)
        to = pl.ds(pl.multiple_of(seq_of(x) * CROWS + h * sub, sub), sub)
        for i in (0, 1):
            ob[i, rows, :] = acc2[rows, i * HEAD : (i + 1) * HEAD].astype(jnp.bfloat16)
        for dev in (right, left):
            send(ob.at[dev // 2, rows], mixed.at[ch, to], at_x(dev), "rows", ("fin",))

    def begin(ch):
        for h in (0, 1):
            send.wait("tok", ch, h)
            g[ch].start(h)

    def both(method, *args):
        for h in (0, 1):
            method(h, *args)

    def nears(ga):
        for d in DIRS:
            both(ga.near, d)

    def use_nears(ga):
        for d in DIRS:
            both(ga.use_near, d)

    def own_take(ch):
        send.wait("scale", ch)
        columns(ch)
        send.wait("near", ch)
        send.wait("q", ch)

    with scope("begin0"):
        loads[2].wait()
        cols_z()
        begin(0)
    with scope("tables"):
        tables()
    with scope("middle0"):
        for h in (0, 1):
            own_dot(0, h)
        nears(g[0])
        use_nears(g[0])
        both(g[0].pass_on, 0)
        both(g[0].opposite)
        relay_w(0)
        both(g[0].use_passed, 0)
        both(g[0].use_opposite)
        both(g[0].pass_on, -1)
        both(g[0].use_passed, -1)
        both(g[0].pass_on, 1)
        relay_w(2)
    with scope("begin1"):
        begin(1)
    with scope("pass0"):
        both(g[0].pass_on, 2)
        both(g[0].use_passed, 1)
        relay_w2(0)
        relay_w(1)
        both(g[0].use_passed, 2)
    with scope("drain0a"):
        both(g[0].last, 0)
    with scope("near1"):
        nears(g[1])
    with scope("relay_w2"):
        relay_w2(2)
    with scope("drain0b"):
        both(g[0].last, -1)
        both(g[0].last, 1)
    with scope("pass1_0"):
        both(g[1].pass_on, 0)
    with scope("drain0c"):
        both(g[0].last, 2)
    with scope("have_w"):
        send.wait("relayed", False)
    with scope("far_qv0"):
        far_dots(0, (0, 2), 0)
        values(0)
    with scope("opp1"):
        both(g[1].opposite)
        relay_w2(1)
    with scope("uses1"):
        for h in (0, 1):
            own_dot(1, h)
        use_nears(g[1])
    with scope("have_wk"):
        send.wait("relayed", True)
        send.wait("gains")
    with scope("far_k0"):
        far_dots(0, (1,), CK)
        keys(0)
        queries(0)
        squares(0)
    with scope("take_v"):
        take_pair("v", 0)
        take_same("v", 0)
    with scope("pass1_m"):
        both(g[1].pass_on, -1)
    with scope("take_k"):
        take_pair("k", 0)
        take_same("k", 0)
    with scope("uses1b"):
        both(g[1].use_passed, 0)
        both(g[1].use_opposite)
        both(g[1].use_passed, -1)
    with scope("tot0"):
        totals(0)
    with scope("pass1_1"):
        both(g[1].pass_on, 1)
    with scope("take_f"):
        take_fwd("v", 0)
        norms(0)
    with scope("pass1_2"):
        both(g[1].pass_on, 2)
        cols_y()
    with scope("take_fk"):
        take_fwd("k", 0)
    with scope("uses1c"):
        both(g[1].use_passed, 1)
        both(g[1].use_passed, 2)
        far_dots(1, (0, 2), 0, (0, 1, 3))
        far_dots(1, (1,), CK, (0, 1, 3))
    with scope("take0"):
        own_take(0)
    with scope("attend0"):
        attend(0)
    with scope("drain1"):
        for j in (0, -1, 1, 2):
            both(g[1].last, j)
        far_dots(1, (0, 2), 0, (2,))
        values(1)
        far_dots(1, (1,), CK, (2,))
        keys(1)
        queries(1)
        squares(1)
    with scope("start_far0"):
        start_far(0)
    with scope("take_v1"):
        take_pair("v", 1)
        take_same("v", 1)
    with scope("tot1"):
        totals(1)
    with scope("near2"):
        nears(g2[0])
    with scope("take_k1"):
        take_pair("k", 1)
        take_same("k", 1)
        cols_same()
    with scope("norms1"):
        norms(1)
    with scope("pass2_0"):
        both(g2[0].pass_on, 0)
        both(g2[0].opposite)
    with scope("take_fv1"):
        take_fwd("v", 1)
    with scope("pass2_m"):
        both(g2[0].pass_on, -1)
    with scope("take_fk1"):
        take_fwd("k", 1)
    with scope("pass2_1"):
        both(g2[0].pass_on, 1)
    with scope("take1"):
        own_take(1)
    with scope("attend1"):
        attend(1)
    with scope("pass2_2"):
        send.wait("ws")
        cols_x(0)
        cols_x(1)
        both(g2[0].pass_on, 2)
    with scope("start_far1"):
        start_far(1)
        place = xl * 2 + co
        tops[place] = jnp.broadcast_to(jnp.maximum(*best), (8, HEAD))
        for dev in (other, at_x(same), at_x(same, 1 - co)):
            send(tops.at[place], tops.at[place], dev, "small", ("peak",))
    with scope("near3"):
        nears(g2[1])
        cols_core(0)
    with scope("pass3_0"):
        both(g2[1].pass_on, 0)
        both(g2[1].opposite)
    with scope("cols_core"):
        cols_core(1)
        send.wait("wc")
    with scope("use2"):
        for ch in (0, 1):
            for h in (0, 1):
                use2(ch, h, z, y, True)
        use_nears(g2[0])
        both(g2[0].use_passed, 0)
        both(g2[0].use_opposite)
        for j in (-1, 1, 2):
            both(g2[0].use_passed, j)
    with scope("drain2_0"):
        both(g2[1].pass_on, -1)
        for j in (0, -1, 1):
            both(g2[0].last, j)
        for h in (0, 1):
            g2[0].last(h, 2)
            finish(0, h)
    with scope("pass3"):
        both(g2[1].pass_on, 1)
        use_nears(g2[1])
        both(g2[1].use_passed, 0)
        both(g2[1].use_opposite)
        both(g2[1].use_passed, -1)
        both(g2[1].use_passed, 1)
        both(g2[1].pass_on, 2)
        both(g2[1].use_passed, 2)
    with scope("drain2_1"):
        for j in (0, -1, 1):
            both(g2[1].last, j)
        for h in (0, 1):
            g2[1].last(h, 2)
            finish(1, h)
    with scope("final"):
        send.wait("peak")
        peak[...] = jnp.maximum(jnp.maximum(tops[0], tops[1]), jnp.maximum(tops[2], tops[3]))
        send.wait("stats")
        for s in (0, 1):
            for i in (0, 1):
                stat_out[:, s, i * CROWS : (i + 1) * CROWS] = inv_in[s, i]
        send.wait("fin")
    with scope("wait_send"):
        send.flush()


def finish_kernel(mixed, peak, stat, mixed_out, peak_out, stat_out):
    mixed_out[...] = mixed[...]
    peak_out[0] = peak[0, 0]
    stat_out[...] = stat[...]


def vmem(count):
    return [pl.BlockSpec(memory_space=pltpu.VMEM)] * count


def shards(tokens, w_qkv, q_gain, k_gain, w_out):
    bf, f32 = jnp.bfloat16, jnp.float32
    dma = pltpu.SemaphoreType.DMA
    sub = CROWS // 2
    freq = ROPE_BASE ** (-(np.arange(HEAD) % (HEAD // 2) * 2.0) / HEAD)
    mixed, peak, stat = pl.pallas_call(
        layer_kernel,
        out_shape=(
            jax.ShapeDtypeStruct((2, TOK, HEAD), bf),
            jax.ShapeDtypeStruct((8, HEAD), f32),
            jax.ShapeDtypeStruct((2, 2, TOK), f32),
        ),
        in_specs=[
            pl.BlockSpec(memory_space=pltpu.VMEM if small else pl.ANY)
            for small in (False, False, True, True, False, True)
        ],
        out_specs=tuple(vmem(3)),
        scratch_shapes=[
            pltpu.VMEM((2, TOK, HEAD), bf),
            pltpu.VMEM((3, WIDTH, HEAD), bf),
            pltpu.VMEM((HEAD, WIDTH), bf),
            pltpu.VMEM((CHUNKS, 2, 4, 4, 2, sub, HEAD), bf),
            pltpu.VMEM((3, WIDTH, HEAD), bf),
            pltpu.VMEM((8, HEAD), f32),
            pltpu.VMEM((8, HEAD), f32),
            pltpu.VMEM((CROWS, HEAD), f32),
            pltpu.VMEM((CROWS, HEAD), f32),
            pltpu.VMEM((TOK, 3 * HEAD), f32),
            pltpu.VMEM((TOK, 3 * HEAD), f32),
            pltpu.VMEM((CHUNKS, 4, 2, CROWS), f32),
            pltpu.VMEM((CHUNKS, 4, 2, CROWS), f32),
            pltpu.VMEM((CHUNKS, 8, 2, CROWS), f32),
            pltpu.VMEM((CHUNKS, 2, 2, CROWS), f32),
            pltpu.VMEM((CHUNKS, 2, CROWS, HEAD), bf),
            pltpu.VMEM((CHUNKS, 8, CROWS, HEAD), bf),
            pltpu.VMEM((CHUNKS, 8, HEAD, CROWS), bf),
            pltpu.VMEM((CHUNKS, CROWS, HEAD), bf),
            pltpu.VMEM((CHUNKS, CROWS, HEAD), bf),
            pltpu.VMEM((CHUNKS, HEAD, CROWS), bf),
            pltpu.VMEM((4, 32, 1024), bf),
            pltpu.VMEM((4, 4, 2, HEAD, 256), bf),
            pltpu.VMEM((CHUNKS, 2, 4, 4, 2, sub, HEAD), bf),
            pltpu.VMEM((CHUNKS, 2, sub, HEAD), bf),
            pltpu.VMEM((TOK, 256), f32),
            pltpu.VMEM((2, TOK, HEAD), bf),
            pltpu.VMEM((4, 8, HEAD), f32),
            pltpu.VMEM((BK, CROWS), f32),
            pltpu.VMEM((BK, CROWS), f32),
            pltpu.VMEM((2, 1, CROWS), f32),
            pltpu.VMEM((2, 1, CROWS), f32),
            pltpu.VMEM((2, HEAD, CROWS), f32),
            pltpu.VMEM((2, 1, CROWS), f32),
            pltpu.VMEM((8, CROWS, HEAD), f32),
            dma((11,)),
            dma((169,)),
            dma((3,)),
        ],
        compiler_params=pltpu.CompilerParams(
            collective_id=0, has_side_effects=True, vmem_limit_bytes=VMEM_CAP
        ),
        name="layer",
    )(
        tokens,
        w_qkv.transpose(1, 0, 2),
        q_gain[None],
        k_gain[None],
        w_out,
        jnp.asarray(freq[None], f32),
    )
    return pl.pallas_call(
        finish_kernel,
        out_shape=(
            jax.ShapeDtypeStruct((2, TOK, HEAD), bf),
            jax.ShapeDtypeStruct((1,), f32),
            jax.ShapeDtypeStruct((2, 2, TOK), f32),
        ),
        in_specs=vmem(3),
        out_specs=(
            pl.BlockSpec(memory_space=pltpu.VMEM),
            pl.BlockSpec(memory_space=pltpu.SMEM),
            pl.BlockSpec(memory_space=pltpu.VMEM),
        ),
        name="finish",
    )(mixed, peak, stat)


def solution(mesh):
    finer = Mesh(mesh.devices.reshape(2, 2, 4, 4, 2), ("xl", "co", "z", "y", "xh"))
    tensor = ("z", "y", "xh")
    seq = ("xl", "co")
    placed = (P(None, seq, tensor), P(None, None, tensor), P(tensor), P(tensor), P(tensor, None))
    return jax.shard_map(
        shards,
        mesh=finer,
        in_specs=placed,
        out_specs=(P(None, seq, tensor), P(tensor), P(None, None, seq)),
        check_vma=False,
    )
```

```python
import contextlib
import math

import jax
import jax.numpy as jnp
import numpy as np
from jax import lax
from jax.experimental import pallas as pl
from jax.experimental.pallas import tpu as pltpu
from jax.sharding import Mesh
from jax.sharding import PartitionSpec as P

EPS = 1e-06
ROPE_BASE = 500000.0
NEG = -1e30
MESH = pl.DeviceIdType.MESH
HEAD = 128
TOK = 1024
CHUNKS = 2
CROWS = TOK // CHUNKS
WIDTH = 4096
BK = 512
VMEM_CAP = 60 * 1024 * 1024
SCALE = HEAD ** (-0.5)
LOG2E = math.log2(math.e)
DIRS = (1, -1)
PART = {1: 0, -1: 1}
CQ, CK, CV = 0, HEAD, 2 * HEAD


def scope(name):
    return contextlib.nullcontext()


def here():
    xh, xl = lax.axis_index("xh"), lax.axis_index("xl")
    return xh * 2 + xl, xh, xl, lax.axis_index("co"), lax.axis_index("z"), lax.axis_index("y")


def seq_of(x):
    return 1 - ((x + 1) // 2) % 2


def half_of(x):
    return 1 - x % 2


def at_x(x, core=None):
    dev = {"xl": x % 2, "xh": x // 2}
    if core is not None:
        dev["co"] = core
    return dev


class Sender:
    def __init__(self, ssem, rsem, region):
        self.ssem, self.rsem, self.region = ssem, rsem, region
        self.groups, self.keys = {}, {}
        self.leaving, self.arriving = {}, {}

    def __call__(self, src, dst, dev, group, key):
        g = self.groups.setdefault(group, len(self.groups))
        k = self.keys.setdefault(key, len(self.keys))
        size = math.prod(src.shape) * jnp.dtype(src.dtype).itemsize
        self.leaving[group] = self.leaving.get(group, 0) + size
        self.arriving[key] = self.arriving.get(key, 0) + size
        pltpu.make_async_remote_copy(
            src_ref=src,
            dst_ref=dst,
            send_sem=self.ssem.at[g],
            recv_sem=self.rsem.at[k],
            device_id=dev,
            device_id_type=MESH,
        ).start()

    def wait(self, *key):
        ref = self.region(self.arriving.pop(key))
        pltpu.make_async_copy(ref, ref, self.rsem.at[self.keys[key]]).wait()

    def flush(self):
        assert not self.arriving, self.arriving
        for group, size in self.leaving.items():
            ref = self.region(size)
            pltpu.make_async_copy(ref, ref, self.ssem.at[self.groups[group]]).wait()


class Gather:
    def __init__(self, name, buf, send, z, y, use):
        self.name, self.buf, self.send, self.use = name, buf, send, use
        self.first, self.second = (z, y), (y, z)

    def place(self, h, f, s):
        return (f % 4, s % 4) if h == 0 else (s % 4, f % 4)

    def at(self, h, df, ds):
        return self.place(h, self.first[h] + df, self.second[h] + ds)

    def move(self, h, df, ds, part, along, d, *key):
        zz, yy = self.at(h, df, ds)
        ref = self.buf.at[h, zz, yy] if part is None else self.buf.at[h, zz, yy, part]
        name = (("z", "y"), ("y", "z"))[h][along]
        me = (self.first[h], self.second[h])[along]
        self.send(ref, ref, {name: (me + d + 4) % 4}, self.name, (self.name, h, *key))

    def wait(self, h, *key):
        self.send.wait(self.name, h, *key)

    def start(self, h, part=None):
        for d in DIRS:
            self.move(h, 0, 0, part, 0, d, "p1", d)
            self.move(h, 0, 0, part, 1, d, "p2", 0, d)

    def near(self, h, d):
        self.wait(h, "p1", d)
        self.move(h, 4 - d, 0, PART[d], 0, d, "p1f")
        for e in DIRS:
            self.move(h, 4 - d, 0, None, 1, e, "p2", -d, e)

    def use_near(self, h, d):
        self.use(h, *self.at(h, 4 - d, 0))

    def pass_on(self, h, j):
        for d in DIRS:
            self.wait(h, "p2", j, d)
            self.move(h, j + 4, 4 - d, PART[d], 1, d, "p2f", j)

    def use_passed(self, h, j):
        for d in DIRS:
            self.use(h, *self.at(h, j + 4, 4 - d))

    def opposite(self, h):
        self.wait(h, "p1f")
        for d in DIRS:
            self.move(h, 2, 0, None, 1, d, "p2", 2, d)

    def use_opposite(self, h):
        self.use(h, *self.at(h, 2, 0))

    def last(self, h, j):
        self.wait(h, "p2f", j)
        self.use(h, *self.at(h, j + 4, 2))


def layer_kernel(
    tok_hbm, w_hbm, q_gain, k_gain, w_out_hbm, freq,
    mixed, peak, stat_out,
    tok, w_own, w_out, buf, w_far, gains, gains_far, cosf, sinf, acc, acc_far, zb, yb, inv, inv_in,
    q_all, k_all, v_all, q_far, k_far, v_far,
    wz, w_cols, buf2, o_far, acc2, ob, tops,
    sc0, sc1, top_r, den_r, acc_r,
    ssem, rsem, ins,
):
    loads = [
        pltpu.make_async_copy(src, dst, ins.at[i])
        for i, (src, dst) in enumerate(((tok_hbm, tok), (w_hbm, w_own), (w_out_hbm, w_out)))
    ]
    for cp in loads:
        cp.start()
    x, xh, xl, co, z, y = here()
    right, left, pair, same = (x + 1) % 4, (x + 3) % 4, 3 - x, xh * 2 + (1 - xl)
    other = {"co": 1 - co}
    peers = (
        [other] + [at_x((x + i) % 4, cc) for i in (1, 2, 3) for cc in (co, 1 - co)]
        + [{"z": (z + i) % 4} for i in (1, 2, 3)]
        + [{"y": (y + i) % 4} for i in (1, 2, 3)]
    )
    with scope("greet"):
        barrier = pltpu.get_barrier_semaphore()
        for dev in peers:
            pl.semaphore_signal(barrier, inc=1, device_id=dev, device_id_type=MESH)
        pl.semaphore_wait(barrier, len(peers))

    def region(size):
        for n in (1, 2, 3):
            if size % (n * 4096) == 0 and size <= n * WIDTH * HEAD * 2:
                return w_far.at[0:n, 0 : size // (n * HEAD * 2)]
        rows, rest = divmod(size, 64 * HEAD * 2)
        assert rest == 0 and rows % 16 == 0 and rows <= CROWS // 2, size
        return buf.at[0, :, :, :, :, 0:rows]

    send = Sender(ssem, rsem, region)
    sub = CROWS // 2

    def eighth(xx, cc):
        return 4 * half_of(xx) + 2 * cc + seq_of(xx)

    mine, far_tile = eighth(x, co), eighth(pair, 1 - co)
    part_of_mine = pl.ds(pl.multiple_of(seq_of(x) * CROWS, CROWS), CROWS)

    def send_tokens(ch):
        for h in (0, 1):
            dst = buf.at[ch, h, z, y, xh]
            for part, dev in ((xh, right), (1 - xh, left)):
                src = tok.at[ch, pl.ds(pl.multiple_of(part * CROWS + h * sub, sub), sub)]
                send(src, dst, at_x(dev), "rows", ("tok", ch, h))

    loads[0].wait()
    send_tokens(0)
    gains[0:1, :] = q_gain[...]
    gains[1:2, :] = k_gain[...]
    loads[1].wait()

    def w_rows(xx):
        return pl.ds(pl.multiple_of(((xx % 2) * 2 + co) * 1024, 1024), 1024)

    def send_w(j):
        send(w_own.at[j, w_rows(x)], w_far.at[j, w_rows(x)], at_x(pair), "w", ("far_w", j))

    def relay_w(j):
        send.wait("far_w", j)
        ref = w_far.at[j, w_rows(pair)]
        send(ref, ref, at_x(same), "w", ("same_w", j))
        send(ref, ref, other, "w", ("relayed", j == 2))

    def relay_w2(j):
        send.wait("same_w", j)
        ref = w_far.at[j, w_rows(pair + 1)]
        send(ref, ref, other, "w", ("relayed", j == 2))

    send_w(0)
    send_w(1)
    send_tokens(1)
    send_w(2)
    send(gains, gains_far, at_x(pair), "small", ("gains",))

    def dots(target, w, ch, h, blocks, zero=False, kinds=(0, 1, 2), at=0):
        lhs, rhs = [], []
        for zz, yy in blocks:
            lhs += [buf[ch, h, zz, yy, 0], buf[ch, h, zz, yy, 1]]
            rows = pl.ds(pl.multiple_of((zz * 4 + yy) * 256, 256), 256)
            some = [w[j, rows, :] for j in kinds]
            rhs.append(some[0] if len(some) == 1 else jnp.concatenate(some, axis=-1))
        lhs = jnp.concatenate(lhs, axis=-1)
        rhs = rhs[0] if len(rhs) == 1 else jnp.concatenate(rhs, axis=0)
        out = jnp.dot(lhs, rhs, preferred_element_type=jnp.float32)
        place = (pl.ds(ch * CROWS + h * sub, sub), slice(at, at + HEAD * len(kinds)))
        target[place] = out if zero else target[place] + out

    def gather_of(ch):
        return Gather(
            ("tokens", ch), buf.at[ch], send, z, y, lambda h, zz, yy: dots(acc, w_own, ch, h, [(zz, yy)])
        )

    def own_dot(ch, h):
        dots(acc, w_own, ch, h, [(z, y)], True)

    def far_dots(ch, kinds, at, lines=(0, 1, 3, 2)):
        for i in lines:
            for h in (0, 1):
                blocks = [g[ch].at(h, f, i) for f in range(4)]
                dots(acc_far, w_far, ch, h, blocks, i == 0, kinds, at)

    def tables():
        def some(i, carry):
            rows = pl.ds(pl.multiple_of(i * 256, 256), 256)
            p = lax.broadcasted_iota(jnp.int32, (256, HEAD), 0) + (mine * CROWS + i * 256)
            lane = lax.broadcasted_iota(jnp.int32, (256, HEAD), 1)
            angle = p.astype(jnp.float32) * freq[...]
            cosf[rows, :] = jnp.cos(angle)
            sine = jnp.sin(angle)
            sinf[rows, :] = jnp.where(lane < HEAD // 2, -sine, sine)
            return carry

        lax.fori_loop(0, CROWS // 256, some, 0)

    def squares(ch):
        for j, c in ((0, CQ), (1, CK)):
            cols = pl.ds(c, HEAD)
            for i in range(2):
                rows = pl.ds(ch * CROWS + i * sub, sub)
                a, b = acc[rows, cols], acc_far[rows, cols]
                zb[ch, z, j : j + 1, i * sub : (i + 1) * sub] = jnp.sum(
                    (a * a + b * b).T, axis=0, keepdims=True
                )
        ref = zb.at[ch, z]
        for i in (1, 2, 3):
            send(ref, ref, {"z": (z + i) % 4}, "small", ("zsum", ch))

    def totals(ch):
        send.wait("zsum", ch)
        yb[ch, y] = (zb[ch, 0] + zb[ch, 1]) + (zb[ch, 2] + zb[ch, 3])
        ref = yb.at[ch, y]
        for i in (1, 2, 3):
            send(ref, ref, {"y": (y + i) % 4}, "small", ("ysum", ch))

    def turned(a, j, g, ch, i):
        rows = pl.ds(ch * CROWS + i * sub, sub)
        table = slice(i * sub, (i + 1) * sub)
        col = jnp.broadcast_to(inv[ch, j : j + 1, table], (HEAD, sub)).T
        t = a[rows, j * HEAD : (j + 1) * HEAD] * col * g[j : j + 1, :]
        return (t * cosf[table, :] + pltpu.roll(t, HEAD // 2, 1) * sinf[table, :]).astype(
            jnp.bfloat16
        )

    def give(name, ch, far, all_):
        slot = all_.at[ch, mine]
        send(far.at[ch], slot, at_x(pair), name, ("pair", name, ch))
        send(slot, slot, at_x(same), name, ("same", name, ch))
        send(slot, slot, other, name, ("near", ch))

    def take_pair(name, ch):
        ref = (k_all if name == "k" else v_all).at[ch, eighth(pair, co)]
        send.wait("pair", name, ch)
        send(ref, ref, at_x(same), name, ("fwd", name, ch))
        send(ref, ref, other, name, ("near", ch))

    def take_same(name, ch):
        ref = (k_all if name == "k" else v_all).at[ch, eighth(same, co)]
        send.wait("same", name, ch)
        send(ref, ref, other, name, ("near", ch))

    def take_fwd(name, ch):
        ref = (k_all if name == "k" else v_all).at[ch, eighth((x + 2) % 4, co)]
        send.wait("fwd", name, ch)
        send(ref, ref, other, name, ("near", ch))

    def values(ch):
        for i in range(2):
            here_rows = slice(i * sub, (i + 1) * sub)
            rows = pl.ds(ch * CROWS + i * sub, sub)
            v_far[ch, :, here_rows] = acc_far[rows, CV : CV + HEAD].T.astype(jnp.bfloat16)
            v_all[ch, mine, :, here_rows] = acc[rows, CV : CV + HEAD].T.astype(jnp.bfloat16)
        give("v", ch, v_far, v_all)

    def keys(ch):
        for i in range(2):
            here_rows = slice(i * sub, (i + 1) * sub)
            k_far[ch, here_rows, :] = turned(acc_far, 1, gains_far, ch, i)
            k_all[ch, mine, here_rows, :] = turned(acc, 1, gains, ch, i)
        give("k", ch, k_far, k_all)

    def queries(ch):
        for i in range(2):
            q_far[ch, i * sub : (i + 1) * sub, :] = turned(acc_far, 0, gains_far, ch, i)
        send(q_far.at[ch], q_all.at[ch, 1], at_x(pair, 1 - co), "rows", ("q", ch))
        for i in range(2):
            q_all[ch, 0, i * sub : (i + 1) * sub, :] = turned(acc, 0, gains, ch, i)

    def norms(ch):
        send.wait("ysum", ch)
        inv[ch] = lax.rsqrt(((yb[ch, 0] + yb[ch, 1]) + (yb[ch, 2] + yb[ch, 3])) / WIDTH + EPS)
        for dev in (right, left):
            send(inv.at[ch], inv_in.at[ch, seq_of(x)], at_x(dev), "small", ("stats",))

    part = pl.ds(pl.multiple_of(co * 64, 64), 64)
    strip = pl.ds(pl.multiple_of((co * 2 + x % 2) * 32, 32), 32)

    def z_cols(zz):
        return pl.ds(pl.multiple_of((zz % 4) * 1024, 1024), 1024)

    def y_cols(yy):
        return pl.ds(pl.multiple_of((yy % 4) * 256, 256), 256)

    def cols_z():
        wz[z] = w_out[strip, z_cols(z)]
        for i in (1, 2, 3):
            send(
                w_out.at[strip, z_cols(z + i)], wz.at[z], {"z": (z + i) % 4}, "cols", ("wz",)
            )

    def cols_y():
        send.wait("wz")
        w_cols[:, y, xh, strip, :] = wz[:, :, y_cols(y)]
        for i in (1, 2, 3):
            send(
                wz.at[:, :, y_cols(y + i)],
                w_cols.at[:, y, xh, strip],
                {"y": (y + i) % 4},
                "cols",
                ("wy",),
            )

    def cols_same():
        send.wait("wy")
        ref = w_cols.at[:, :, xh, strip]
        send(ref, ref, at_x(same), "cols", ("ws",))

    def cols_x(i):
        ref = w_cols.at[2 * i : 2 * i + 2, :, xh, part]
        send(ref, ref, at_x(pair), "cols", ("wx", i))

    def cols_core(i):
        send.wait("wx", i)
        ref = w_cols.at[2 * i : 2 * i + 2, :, :, part]
        send(ref, ref, other, "core", ("wc",))

    best = []

    def attend(ch):
        count = far_tile + 1
        total = count + mine + 1

        top_r[...] = jnp.full((2, 1, CROWS), NEG, jnp.float32)
        den_r[...] = jnp.zeros((2, 1, CROWS), jnp.float32)
        acc_r[...] = jnp.zeros((2, HEAD, CROWS), jnp.float32)

        def where(t):
            own = (t + 16 - count) // 16
            return 1 - own, (1 - own) * (count - 1 - t) + own * (t - count)

        def score(t, into):
            which, j = where(t)
            raw = lax.dot_general(
                k_all[ch, j], q_all[ch, which], (((1,), (1,)), ((), ())),
                preferred_element_type=jnp.float32,
            )
            into[...] = raw

        def weigh(t, cur, masked):
            which, j = where(t)
            s = cur[...]
            if masked:
                r = lax.broadcasted_iota(jnp.int32, (BK, CROWS), 0)
                c = lax.broadcasted_iota(jnp.int32, (BK, CROWS), 1)
                s = jnp.where(r <= c, s, NEG)
            top, p = top_r[which], SCALE * LOG2E
            new = jnp.maximum(top, jnp.max(s, axis=0, keepdims=True))
            e = jnp.exp2((s - new) * p)
            keep = jnp.exp2((top - new) * p)
            den_r[which] = den_r[which] * keep + jnp.sum(e, axis=0, keepdims=True)
            acc_r[which] = acc_r[which] * keep + jnp.dot(
                v_all[ch, j], e.astype(jnp.bfloat16), preferred_element_type=jnp.float32
            )
            top_r[which] = new

        score(0, sc0)
        score(1, sc1)
        weigh(0, sc0, True)

        def two(i, carry):
            t = 2 * i + 1
            score(t + 1, sc0)
            weigh(t, sc1, False)
            score(t + 2, sc1)
            weigh(t + 1, sc0, False)
            return carry

        lax.fori_loop(0, 3 + seq_of(x), two, 0)
        weigh(total - 1, sc1, True)
        for h in (0, 1):
            o_far[ch, h] = (
                (acc_r[1, :, h * sub : (h + 1) * sub] / den_r[1, :, h * sub : (h + 1) * sub])
                .T.astype(jnp.bfloat16)
            )
            dst = buf2.at[ch, h, z, y, xh]
            send(o_far.at[ch, h], dst, at_x(pair, 1 - co), "rows", ("back", ch, h))
        for h in (0, 1):
            buf2[ch, h, z, y, xh] = (
                (acc_r[0, :, h * sub : (h + 1) * sub] / den_r[0, :, h * sub : (h + 1) * sub])
                .T.astype(jnp.bfloat16)
            )
            g2[ch].start(h, xh)
        peaks_here = [jnp.max(top_r[i], axis=1, keepdims=True) for i in (0, 1)]
        best.append(jnp.maximum(*peaks_here) * SCALE)

    def start_far(ch):
        for h in (0, 1):
            send.wait("back", ch, h)
            g2[ch].start(h, 1 - xh)

    def use2(ch, h, zz, yy, zero=False):
        lhs = jnp.concatenate([buf2[ch, h, zz, yy, 0], buf2[ch, h, zz, yy, 1]], axis=-1)
        rhs = jnp.concatenate([w_cols[zz, yy, 0], w_cols[zz, yy, 1]], axis=0)
        out = jnp.dot(lhs, rhs, preferred_element_type=jnp.float32)
        rows = pl.ds(ch * CROWS + h * sub, sub)
        acc2[rows, :] = out if zero else acc2[rows, :] + out

    g = [gather_of(0), gather_of(1)]
    g2 = [
        Gather(
            ("attended", ch),
            buf2.at[ch],
            send,
            z,
            y,
            lambda h, zz, yy, ch=ch: use2(ch, h, zz, yy),
        )
        for ch in (0, 1)
    ]

    def finish(ch, h):
        rows = pl.ds(ch * CROWS + h * sub, sub)
        to = pl.ds(pl.multiple_of(seq_of(x) * CROWS + h * sub, sub), sub)
        for i in (0, 1):
            ob[i, rows, :] = acc2[rows, i * HEAD : (i + 1) * HEAD].astype(jnp.bfloat16)
        for dev in (right, left):
            send(ob.at[dev // 2, rows], mixed.at[ch, to], at_x(dev), "rows", ("fin",))

    def begin(ch):
        for h in (0, 1):
            send.wait("tok", ch, h)
            g[ch].start(h)

    def both(method, *args):
        for h in (0, 1):
            method(h, *args)

    def nears(ga):
        for d in DIRS:
            both(ga.near, d)

    def use_nears(ga):
        for d in DIRS:
            both(ga.use_near, d)

    def own_take(ch):
        send.wait("near", ch)
        send.wait("q", ch)

    with scope("begin0"):
        loads[2].wait()
        cols_z()
        begin(0)
    with scope("tables"):
        tables()
    with scope("middle0"):
        for h in (0, 1):
            own_dot(0, h)
        nears(g[0])
        use_nears(g[0])
        both(g[0].pass_on, 0)
        both(g[0].opposite)
        relay_w(0)
        both(g[0].use_passed, 0)
        both(g[0].use_opposite)
        both(g[0].pass_on, -1)
        both(g[0].use_passed, -1)
        both(g[0].pass_on, 1)
        relay_w(1)
    with scope("begin1"):
        begin(1)
    with scope("pass0"):
        both(g[0].pass_on, 2)
        both(g[0].use_passed, 1)
        relay_w2(0)
        relay_w(2)
        both(g[0].use_passed, 2)
    with scope("drain0a"):
        both(g[0].last, 0)
    with scope("near1"):
        nears(g[1])
    with scope("relay_w2"):
        relay_w2(1)
    with scope("drain0b"):
        both(g[0].last, -1)
        both(g[0].last, 1)
    with scope("pass1_0"):
        both(g[1].pass_on, 0)
    with scope("drain0c"):
        both(g[0].last, 2)
    with scope("have_w"):
        send.wait("relayed", False)
    with scope("far_qk0"):
        far_dots(0, (0, 1), CQ)
        squares(0)
    with scope("opp1"):
        both(g[1].opposite)
        relay_w2(2)
    with scope("uses1"):
        for h in (0, 1):
            own_dot(1, h)
        use_nears(g[1])
        send.wait("gains")
    with scope("tot0"):
        totals(0)
    with scope("have_wv"):
        send.wait("relayed", True)
    with scope("far_v0"):
        far_dots(0, (2,), CV)
        values(0)
    with scope("norms0"):
        norms(0)
        keys(0)
        queries(0)
    with scope("pass1_m"):
        both(g[1].pass_on, -1)
        both(g[1].use_passed, 0)
        both(g[1].use_opposite)
        both(g[1].use_passed, -1)
    with scope("take_v"):
        take_pair("v", 0)
        take_same("v", 0)
    with scope("pass1_1"):
        both(g[1].pass_on, 1)
    with scope("take_k"):
        take_pair("k", 0)
        take_same("k", 0)
    with scope("pass1_2"):
        both(g[1].pass_on, 2)
        cols_y()
    with scope("uses1c"):
        both(g[1].use_passed, 1)
        both(g[1].use_passed, 2)
        far_dots(1, (0, 1), CQ, (0, 1, 3))
    with scope("take_f"):
        take_fwd("v", 0)
        take_fwd("k", 0)
    with scope("far_v1"):
        far_dots(1, (2,), CV, (0, 1, 3))
    with scope("drain1"):
        for j in (0, -1, 1, 2):
            both(g[1].last, j)
    with scope("far1"):
        far_dots(1, (0, 1), CQ, (2,))
        squares(1)
        far_dots(1, (2,), CV, (2,))
        values(1)
    with scope("take0"):
        own_take(0)
    with scope("attend0"):
        attend(0)
    with scope("tot1"):
        totals(1)
        take_pair("v", 1)
        take_same("v", 1)
    with scope("start_far0"):
        start_far(0)
    with scope("norms1"):
        norms(1)
        keys(1)
        queries(1)
        take_fwd("v", 1)
    with scope("near2"):
        nears(g2[0])
    with scope("take_k1"):
        take_pair("k", 1)
        take_same("k", 1)
        cols_same()
    with scope("pass2_0"):
        both(g2[0].pass_on, 0)
        both(g2[0].opposite)
    with scope("pass2_m"):
        both(g2[0].pass_on, -1)
    with scope("take_fk1"):
        take_fwd("k", 1)
    with scope("pass2_1"):
        both(g2[0].pass_on, 1)
    with scope("take1"):
        own_take(1)
    with scope("attend1"):
        attend(1)
    with scope("pass2_2"):
        send.wait("ws")
        cols_x(0)
        cols_x(1)
        both(g2[0].pass_on, 2)
    with scope("start_far1"):
        start_far(1)
        place = xl * 2 + co
        tops[place] = jnp.broadcast_to(jnp.maximum(*best), (8, HEAD))
        for dev in (other, at_x(same), at_x(same, 1 - co)):
            send(tops.at[place], tops.at[place], dev, "small", ("peak",))
    with scope("near3"):
        nears(g2[1])
        cols_core(0)
    with scope("pass3_0"):
        both(g2[1].pass_on, 0)
        both(g2[1].opposite)
    with scope("cols_core"):
        cols_core(1)
        send.wait("wc")
    with scope("use2"):
        for ch in (0, 1):
            for h in (0, 1):
                use2(ch, h, z, y, True)
        use_nears(g2[0])
        both(g2[0].use_passed, 0)
        both(g2[0].use_opposite)
        for j in (-1, 1, 2):
            both(g2[0].use_passed, j)
    with scope("drain2_0"):
        both(g2[1].pass_on, -1)
        for j in (0, -1, 1):
            both(g2[0].last, j)
        for h in (0, 1):
            g2[0].last(h, 2)
            finish(0, h)
    with scope("pass3"):
        both(g2[1].pass_on, 1)
        use_nears(g2[1])
        both(g2[1].use_passed, 0)
        both(g2[1].use_opposite)
        both(g2[1].use_passed, -1)
        both(g2[1].use_passed, 1)
        both(g2[1].pass_on, 2)
        both(g2[1].use_passed, 2)
    with scope("drain2_1"):
        for j in (0, -1, 1):
            both(g2[1].last, j)
        for h in (0, 1):
            g2[1].last(h, 2)
            finish(1, h)
    with scope("final"):
        send.wait("peak")
        peak[...] = jnp.maximum(jnp.maximum(tops[0], tops[1]), jnp.maximum(tops[2], tops[3]))
        send.wait("stats")
        for s in (0, 1):
            for i in (0, 1):
                stat_out[:, s, i * CROWS : (i + 1) * CROWS] = inv_in[s, i]
        send.wait("fin")
    with scope("wait_send"):
        send.flush()


def finish_kernel(mixed, peak, stat, mixed_out, peak_out, stat_out):
    mixed_out[...] = mixed[...]
    peak_out[0] = peak[0, 0]
    stat_out[...] = stat[...]


def vmem(count):
    return [pl.BlockSpec(memory_space=pltpu.VMEM)] * count


def shards(tokens, w_qkv, q_gain, k_gain, w_out):
    bf, f32 = jnp.bfloat16, jnp.float32
    dma = pltpu.SemaphoreType.DMA
    sub = CROWS // 2
    freq = ROPE_BASE ** (-(np.arange(HEAD) % (HEAD // 2) * 2.0) / HEAD)
    mixed, peak, stat = pl.pallas_call(
        layer_kernel,
        out_shape=(
            jax.ShapeDtypeStruct((2, TOK, HEAD), bf),
            jax.ShapeDtypeStruct((8, HEAD), f32),
            jax.ShapeDtypeStruct((2, 2, TOK), f32),
        ),
        in_specs=[
            pl.BlockSpec(memory_space=pltpu.VMEM if small else pl.ANY)
            for small in (False, False, True, True, False, True)
        ],
        out_specs=tuple(vmem(3)),
        scratch_shapes=[
            pltpu.VMEM((2, TOK, HEAD), bf),
            pltpu.VMEM((3, WIDTH, HEAD), bf),
            pltpu.VMEM((HEAD, WIDTH), bf),
            pltpu.VMEM((CHUNKS, 2, 4, 4, 2, sub, HEAD), bf),
            pltpu.VMEM((3, WIDTH, HEAD), bf),
            pltpu.VMEM((8, HEAD), f32),
            pltpu.VMEM((8, HEAD), f32),
            pltpu.VMEM((CROWS, HEAD), f32),
            pltpu.VMEM((CROWS, HEAD), f32),
            pltpu.VMEM((TOK, 3 * HEAD), f32),
            pltpu.VMEM((TOK, 3 * HEAD), f32),
            pltpu.VMEM((CHUNKS, 4, 2, CROWS), f32),
            pltpu.VMEM((CHUNKS, 4, 2, CROWS), f32),
            pltpu.VMEM((CHUNKS, 2, CROWS), f32),
            pltpu.VMEM((CHUNKS, 2, 2, CROWS), f32),
            pltpu.VMEM((CHUNKS, 2, CROWS, HEAD), bf),
            pltpu.VMEM((CHUNKS, 8, CROWS, HEAD), bf),
            pltpu.VMEM((CHUNKS, 8, HEAD, CROWS), bf),
            pltpu.VMEM((CHUNKS, CROWS, HEAD), bf),
            pltpu.VMEM((CHUNKS, CROWS, HEAD), bf),
            pltpu.VMEM((CHUNKS, HEAD, CROWS), bf),
            pltpu.VMEM((4, 32, 1024), bf),
            pltpu.VMEM((4, 4, 2, HEAD, 256), bf),
            pltpu.VMEM((CHUNKS, 2, 4, 4, 2, sub, HEAD), bf),
            pltpu.VMEM((CHUNKS, 2, sub, HEAD), bf),
            pltpu.VMEM((TOK, 256), f32),
            pltpu.VMEM((2, TOK, HEAD), bf),
            pltpu.VMEM((4, 8, HEAD), f32),
            pltpu.VMEM((BK, CROWS), f32),
            pltpu.VMEM((BK, CROWS), f32),
            pltpu.VMEM((2, 1, CROWS), f32),
            pltpu.VMEM((2, 1, CROWS), f32),
            pltpu.VMEM((2, HEAD, CROWS), f32),
            dma((11,)),
            dma((169,)),
            dma((3,)),
        ],
        compiler_params=pltpu.CompilerParams(
            collective_id=0, has_side_effects=True, vmem_limit_bytes=VMEM_CAP
        ),
        name="layer",
    )(
        tokens,
        w_qkv.transpose(1, 0, 2),
        q_gain[None],
        k_gain[None],
        w_out,
        jnp.asarray(freq[None], f32),
    )
    return pl.pallas_call(
        finish_kernel,
        out_shape=(
            jax.ShapeDtypeStruct((2, TOK, HEAD), bf),
            jax.ShapeDtypeStruct((1,), f32),
            jax.ShapeDtypeStruct((2, 2, TOK), f32),
        ),
        in_specs=vmem(3),
        out_specs=(
            pl.BlockSpec(memory_space=pltpu.VMEM),
            pl.BlockSpec(memory_space=pltpu.SMEM),
            pl.BlockSpec(memory_space=pltpu.VMEM),
        ),
        name="finish",
    )(mixed, peak, stat)


def solution(mesh):
    finer = Mesh(mesh.devices.reshape(2, 2, 4, 4, 2), ("xl", "co", "z", "y", "xh"))
    tensor = ("z", "y", "xh")
    seq = ("xl", "co")
    placed = (P(None, seq, tensor), P(None, None, tensor), P(tensor), P(tensor), P(tensor, None))
    return jax.shard_map(
        shards,
        mesh=finer,
        in_specs=placed,
        out_specs=(P(None, seq, tensor), P(tensor), P(None, None, seq)),
        check_vma=False,
    )
```

```python
import contextlib
import math

import jax
import jax.numpy as jnp
import numpy as np
from jax import lax
from jax.experimental import pallas as pl
from jax.experimental.pallas import tpu as pltpu
from jax.sharding import Mesh
from jax.sharding import PartitionSpec as P

EPS = 1e-06
ROPE_BASE = 500000.0
NEG = -1e30
MESH = pl.DeviceIdType.MESH
HEAD = 128
TOK = 1024
CHUNKS = 2
CROWS = TOK // CHUNKS
WIDTH = 4096
BK = 512
VMEM_CAP = 60 * 1024 * 1024
SCALE = HEAD ** (-0.5)
LOG2E = math.log2(math.e)
DIRS = (1, -1)
PART = {1: 0, -1: 1}
CQ, CK, CV = 0, HEAD, 2 * HEAD


def scope(name):
    return contextlib.nullcontext()


def here():
    xh, xl = lax.axis_index("xh"), lax.axis_index("xl")
    return xh * 2 + xl, xh, xl, lax.axis_index("co"), lax.axis_index("z"), lax.axis_index("y")


def seq_of(x):
    return 1 - ((x + 1) // 2) % 2


def half_of(x):
    return 1 - x % 2


def at_x(x, core=None):
    dev = {"xl": x % 2, "xh": x // 2}
    if core is not None:
        dev["co"] = core
    return dev


class Sender:
    def __init__(self, ssem, rsem, region):
        self.ssem, self.rsem, self.region = ssem, rsem, region
        self.groups, self.keys = {}, {}
        self.leaving, self.arriving = {}, {}

    def __call__(self, src, dst, dev, group, key):
        g = self.groups.setdefault(group, len(self.groups))
        k = self.keys.setdefault(key, len(self.keys))
        size = math.prod(src.shape) * jnp.dtype(src.dtype).itemsize
        self.leaving[group] = self.leaving.get(group, 0) + size
        self.arriving[key] = self.arriving.get(key, 0) + size
        pltpu.make_async_remote_copy(
            src_ref=src,
            dst_ref=dst,
            send_sem=self.ssem.at[g],
            recv_sem=self.rsem.at[k],
            device_id=dev,
            device_id_type=MESH,
        ).start()

    def wait(self, *key):
        ref = self.region(self.arriving.pop(key))
        pltpu.make_async_copy(ref, ref, self.rsem.at[self.keys[key]]).wait()

    def flush(self):
        assert not self.arriving, self.arriving
        for group, size in self.leaving.items():
            ref = self.region(size)
            pltpu.make_async_copy(ref, ref, self.ssem.at[self.groups[group]]).wait()


class Gather:
    def __init__(self, name, buf, send, z, y, use):
        self.name, self.buf, self.send, self.use = name, buf, send, use
        self.first, self.second = (z, y), (y, z)

    def place(self, h, f, s):
        return (f % 4, s % 4) if h == 0 else (s % 4, f % 4)

    def at(self, h, df, ds):
        return self.place(h, self.first[h] + df, self.second[h] + ds)

    def move(self, h, df, ds, part, along, d, *key):
        zz, yy = self.at(h, df, ds)
        ref = self.buf.at[h, zz, yy] if part is None else self.buf.at[h, zz, yy, part]
        name = (("z", "y"), ("y", "z"))[h][along]
        me = (self.first[h], self.second[h])[along]
        self.send(ref, ref, {name: (me + d + 4) % 4}, self.name, (self.name, h, *key))

    def wait(self, h, *key):
        self.send.wait(self.name, h, *key)

    def start(self, h, part=None):
        for d in DIRS:
            self.move(h, 0, 0, part, 0, d, "p1")
            self.move(h, 0, 0, part, 1, d, "p2", 0)

    def near(self, h):
        self.wait(h, "p1")
        for d in DIRS:
            self.move(h, 4 - d, 0, PART[d], 0, d, "p1f")

    def spread(self, h):
        for d in DIRS:
            for e in DIRS:
                self.move(h, 4 - d, 0, None, 1, e, "p2", -d)

    def use_near(self, h, d):
        self.use(h, *self.at(h, 4 - d, 0))

    def pass_on(self, h, j):
        self.wait(h, "p2", j)
        for d in DIRS:
            self.move(h, j + 4, 4 - d, PART[d], 1, d, "p2f", j)

    def use_passed(self, h, j):
        for d in DIRS:
            self.use(h, *self.at(h, j + 4, 4 - d))

    def opposite(self, h):
        self.wait(h, "p1f")
        for d in DIRS:
            self.move(h, 2, 0, None, 1, d, "p2", 2)

    def use_opposite(self, h):
        self.use(h, *self.at(h, 2, 0))

    def last(self, h, j):
        self.wait(h, "p2f", j)
        self.use(h, *self.at(h, j + 4, 2))


def layer_kernel(
    tok_hbm, w_hbm, q_gain, k_gain, w_out_hbm, freq_hbm,
    mixed, peak, stat_out,
    tok, w_own, w_out, freq, buf, w_far, gains, gains_far, cosf, sinf, acc, acc_far, zb, yb, inv, inv_in,
    q_all, k_all, v_all, q_far, k_far, v_far,
    wz, w_cols, buf2, o_far, acc2, ob, tops,
    sc0, sc1, top_r, den_r, acc_r,
    ssem, rsem, ins,
):
    loads = [
        pltpu.make_async_copy(src, dst, ins.at[i])
        for i, (src, dst) in enumerate(
            (
                (tok_hbm, tok), (w_hbm, w_own), (w_out_hbm, w_out), (freq_hbm, freq),
                (q_gain, gains.at[0:1]), (k_gain, gains.at[1:2]),
            )
        )
    ]
    for cp in loads:
        cp.start()
    x, xh, xl, co, z, y = here()
    right, left, pair, same = (x + 1) % 4, (x + 3) % 4, 3 - x, xh * 2 + (1 - xl)
    other = {"co": 1 - co}
    peers = (
        [other] + [at_x((x + i) % 4, cc) for i in (1, 2, 3) for cc in (co, 1 - co)]
        + [{"z": (z + i) % 4} for i in (1, 2, 3)]
        + [{"y": (y + i) % 4} for i in (1, 2, 3)]
    )
    with scope("greet"):
        barrier = pltpu.get_barrier_semaphore()
        for dev in peers:
            pl.semaphore_signal(barrier, inc=1, device_id=dev, device_id_type=MESH)
        pl.semaphore_wait(barrier, len(peers))

    def region(size):
        for n in (1, 2, 3):
            if size % (n * 4096) == 0 and size <= n * WIDTH * HEAD * 2:
                return w_far.at[0:n, 0 : size // (n * HEAD * 2)]
        rows, rest = divmod(size, 64 * HEAD * 2)
        assert rest == 0 and rows % 16 == 0 and rows <= CROWS // 2, size
        return buf.at[0, :, :, :, :, 0:rows]

    send = Sender(ssem, rsem, region)
    sub = CROWS // 2

    def eighth(xx, cc):
        return 4 * half_of(xx) + 2 * cc + seq_of(xx)

    mine, far_tile = eighth(x, co), eighth(pair, 1 - co)
    part_of_mine = pl.ds(pl.multiple_of(seq_of(x) * CROWS, CROWS), CROWS)

    def send_tokens(ch):
        for h in (0, 1):
            dst = buf.at[ch, h, z, y, xh]
            for part, dev in ((xh, right), (1 - xh, left)):
                src = tok.at[ch, pl.ds(pl.multiple_of(part * CROWS + h * sub, sub), sub)]
                send(src, dst, at_x(dev), "rows", ("tok", ch, h))

    loads[0].wait()
    send_tokens(0)
    loads[1].wait()
    for cp in loads[3:]:
        cp.wait()

    def w_rows(xx):
        return pl.ds(pl.multiple_of(((xx % 2) * 2 + co) * 1024, 1024), 1024)

    def send_w(j):
        send(w_own.at[j, w_rows(x)], w_far.at[j, w_rows(x)], at_x(pair), "w", ("far_w", j))

    def relay_w(j):
        send.wait("far_w", j)
        ref = w_far.at[j, w_rows(pair)]
        send(ref, ref, at_x(same), "w", ("same_w", j))
        send(ref, ref, other, "w", ("relayed", j == 2))

    def relay_w2(j):
        send.wait("same_w", j)
        ref = w_far.at[j, w_rows(pair + 1)]
        send(ref, ref, other, "w", ("relayed", j == 2))

    send_w(0)
    send_w(1)
    send_tokens(1)
    send_w(2)
    send(gains, gains_far, at_x(pair), "small", ("gains",))

    def dots(target, w, ch, h, blocks, zero=False, kinds=(0, 1, 2), at=0):
        lhs, rhs = [], []
        for zz, yy in blocks:
            lhs += [buf[ch, h, zz, yy, 0], buf[ch, h, zz, yy, 1]]
            rows = pl.ds(pl.multiple_of((zz * 4 + yy) * 256, 256), 256)
            some = [w[j, rows, :] for j in kinds]
            rhs.append(some[0] if len(some) == 1 else jnp.concatenate(some, axis=-1))
        lhs = jnp.concatenate(lhs, axis=-1)
        rhs = rhs[0] if len(rhs) == 1 else jnp.concatenate(rhs, axis=0)
        out = jnp.dot(lhs, rhs, preferred_element_type=jnp.float32)
        place = (pl.ds(ch * CROWS + h * sub, sub), slice(at, at + HEAD * len(kinds)))
        target[place] = out if zero else target[place] + out

    def gather_of(ch):
        return Gather(
            ("tokens", ch), buf.at[ch], send, z, y, lambda h, zz, yy: dots(acc, w_own, ch, h, [(zz, yy)])
        )

    def own_dot(ch, h):
        dots(acc, w_own, ch, h, [(z, y)], True)

    def far_dots(ch, kinds, at, lines=(0, 1, 3, 2)):
        for i in lines:
            for h in (0, 1):
                blocks = [g[ch].at(h, f, i) for f in range(4)]
                dots(acc_far, w_far, ch, h, blocks, i == 0, kinds, at)

    def tables():
        def some(i, carry):
            rows = pl.ds(pl.multiple_of(i * 256, 256), 256)
            p = lax.broadcasted_iota(jnp.int32, (256, HEAD), 0) + (mine * CROWS + i * 256)
            lane = lax.broadcasted_iota(jnp.int32, (256, HEAD), 1)
            angle = p.astype(jnp.float32) * freq[...]
            cosf[rows, :] = jnp.cos(angle)
            sine = jnp.sin(angle)
            sinf[rows, :] = jnp.where(lane < HEAD // 2, -sine, sine)
            return carry

        lax.fori_loop(0, CROWS // 256, some, 0)

    def squares(ch):
        for j, c in ((0, CQ), (1, CK)):
            cols = pl.ds(c, HEAD)
            for i in range(2):
                rows = pl.ds(ch * CROWS + i * sub, sub)
                a, b = acc[rows, cols], acc_far[rows, cols]
                zb[ch, z, j : j + 1, i * sub : (i + 1) * sub] = jnp.sum(
                    (a * a + b * b).T, axis=0, keepdims=True
                )
        ref = zb.at[ch, z]
        for i in (1, 2, 3):
            send(ref, ref, {"z": (z + i) % 4}, "small", ("zsum", ch))

    def totals(ch):
        send.wait("zsum", ch)
        yb[ch, y] = (zb[ch, 0] + zb[ch, 1]) + (zb[ch, 2] + zb[ch, 3])
        ref = yb.at[ch, y]
        for i in (1, 2, 3):
            send(ref, ref, {"y": (y + i) % 4}, "small", ("ysum", ch))

    def turned(a, j, g, ch, i):
        rows = pl.ds(ch * CROWS + i * sub, sub)
        table = slice(i * sub, (i + 1) * sub)
        col = jnp.broadcast_to(inv[ch, j : j + 1, table], (HEAD, sub)).T
        t = a[rows, j * HEAD : (j + 1) * HEAD] * col * g[j : j + 1, :]
        return (t * cosf[table, :] + pltpu.roll(t, HEAD // 2, 1) * sinf[table, :]).astype(
            jnp.bfloat16
        )

    def give(name, ch, far, all_):
        slot = all_.at[ch, mine]
        send(far.at[ch], slot, at_x(pair), name, ("pair", name, ch))
        send(slot, slot, at_x(same), name, ("same", name, ch))
        send(slot, slot, other, name, ("near", ch))

    def take_pair(name, ch):
        ref = (k_all if name == "k" else v_all).at[ch, eighth(pair, co)]
        send.wait("pair", name, ch)
        send(ref, ref, at_x(same), name, ("fwd", name, ch))
        send(ref, ref, other, name, ("near", ch))

    def take_same(name, ch):
        ref = (k_all if name == "k" else v_all).at[ch, eighth(same, co)]
        send.wait("same", name, ch)
        send(ref, ref, other, name, ("near", ch))

    def take_fwd(name, ch):
        ref = (k_all if name == "k" else v_all).at[ch, eighth((x + 2) % 4, co)]
        send.wait("fwd", name, ch)
        send(ref, ref, other, name, ("near", ch))

    def values(ch):
        for i in range(2):
            here_rows = slice(i * sub, (i + 1) * sub)
            rows = pl.ds(ch * CROWS + i * sub, sub)
            v_far[ch, :, here_rows] = acc_far[rows, CV : CV + HEAD].T.astype(jnp.bfloat16)
            v_all[ch, mine, :, here_rows] = acc[rows, CV : CV + HEAD].T.astype(jnp.bfloat16)
        give("v", ch, v_far, v_all)

    def keys(ch):
        for i in range(2):
            here_rows = slice(i * sub, (i + 1) * sub)
            k_far[ch, here_rows, :] = turned(acc_far, 1, gains_far, ch, i)
            k_all[ch, mine, here_rows, :] = turned(acc, 1, gains, ch, i)
        give("k", ch, k_far, k_all)

    def queries(ch):
        for i in range(2):
            q_far[ch, i * sub : (i + 1) * sub, :] = turned(acc_far, 0, gains_far, ch, i)
        send(q_far.at[ch], q_all.at[ch, 1], at_x(pair, 1 - co), "rows", ("q", ch))
        for i in range(2):
            q_all[ch, 0, i * sub : (i + 1) * sub, :] = turned(acc, 0, gains, ch, i)

    def norms(ch):
        send.wait("ysum", ch)
        inv[ch] = lax.rsqrt(((yb[ch, 0] + yb[ch, 1]) + (yb[ch, 2] + yb[ch, 3])) / WIDTH + EPS)
        for dev in (right, left):
            send(inv.at[ch], inv_in.at[ch, seq_of(x)], at_x(dev), "small", ("stats",))

    part = pl.ds(pl.multiple_of(co * 64, 64), 64)
    strip = pl.ds(pl.multiple_of((co * 2 + x % 2) * 32, 32), 32)

    def z_cols(zz):
        return pl.ds(pl.multiple_of((zz % 4) * 1024, 1024), 1024)

    def y_cols(yy):
        return pl.ds(pl.multiple_of((yy % 4) * 256, 256), 256)

    def cols_z():
        wz[z] = w_out[strip, z_cols(z)]
        for i in (1, 2, 3):
            send(
                w_out.at[strip, z_cols(z + i)], wz.at[z], {"z": (z + i) % 4}, "cols", ("wz",)
            )

    def cols_y():
        send.wait("wz")
        w_cols[:, y, xh, strip, :] = wz[:, :, y_cols(y)]
        for i in (1, 2, 3):
            send(
                wz.at[:, :, y_cols(y + i)],
                w_cols.at[:, y, xh, strip],
                {"y": (y + i) % 4},
                "cols",
                ("wy",),
            )

    def cols_same():
        send.wait("wy")
        ref = w_cols.at[:, :, xh, strip]
        send(ref, ref, at_x(same), "cols", ("ws",))

    def cols_x(i):
        ref = w_cols.at[2 * i : 2 * i + 2, :, xh, part]
        send(ref, ref, at_x(pair), "cols", ("wx", i))

    def cols_core(i):
        send.wait("wx", i)
        ref = w_cols.at[2 * i : 2 * i + 2, :, :, part]
        send(ref, ref, other, "core", ("wc",))

    best = []

    def attend(ch):
        count = far_tile + 1
        total = count + mine + 1

        top_r[...] = jnp.full((2, 1, CROWS), NEG, jnp.float32)
        den_r[...] = jnp.zeros((2, 1, CROWS), jnp.float32)
        acc_r[...] = jnp.zeros((2, HEAD, CROWS), jnp.float32)

        def where(t):
            own = (t + 16 - count) // 16
            return 1 - own, (1 - own) * (count - 1 - t) + own * (t - count)

        def score(t, into):
            which, j = where(t)
            raw = lax.dot_general(
                k_all[ch, j], q_all[ch, which], (((1,), (1,)), ((), ())),
                preferred_element_type=jnp.float32,
            )
            into[...] = raw

        def weigh(t, cur, masked):
            which, j = where(t)
            s = cur[...]
            if masked:
                r = lax.broadcasted_iota(jnp.int32, (BK, CROWS), 0)
                c = lax.broadcasted_iota(jnp.int32, (BK, CROWS), 1)
                s = jnp.where(r <= c, s, NEG)
            top, p = top_r[which], SCALE * LOG2E
            new = jnp.maximum(top, jnp.max(s, axis=0, keepdims=True))
            e = jnp.exp2((s - new) * p)
            keep = jnp.exp2((top - new) * p)
            den_r[which] = den_r[which] * keep + jnp.sum(e, axis=0, keepdims=True)
            acc_r[which] = acc_r[which] * keep + jnp.dot(
                v_all[ch, j], e.astype(jnp.bfloat16), preferred_element_type=jnp.float32
            )
            top_r[which] = new

        score(0, sc0)
        score(1, sc1)
        weigh(0, sc0, True)

        def two(i, carry):
            t = 2 * i + 1
            score(t + 1, sc0)
            weigh(t, sc1, False)
            score(t + 2, sc1)
            weigh(t + 1, sc0, False)
            return carry

        lax.fori_loop(0, 3 + seq_of(x), two, 0)
        weigh(total - 1, sc1, True)
        for h in (0, 1):
            o_far[ch, h] = (
                (acc_r[1, :, h * sub : (h + 1) * sub] / den_r[1, :, h * sub : (h + 1) * sub])
                .T.astype(jnp.bfloat16)
            )
            dst = buf2.at[ch, h, z, y, xh]
            send(o_far.at[ch, h], dst, at_x(pair, 1 - co), "rows", ("back", ch, h))
        for h in (0, 1):
            buf2[ch, h, z, y, xh] = (
                (acc_r[0, :, h * sub : (h + 1) * sub] / den_r[0, :, h * sub : (h + 1) * sub])
                .T.astype(jnp.bfloat16)
            )
            g2[ch].start(h, xh)
        peaks_here = [jnp.max(top_r[i], axis=1, keepdims=True) for i in (0, 1)]
        best.append(jnp.maximum(*peaks_here) * SCALE)

    def start_far(ch):
        for h in (0, 1):
            send.wait("back", ch, h)
            g2[ch].start(h, 1 - xh)

    def use2(ch, h, zz, yy, zero=False):
        lhs = jnp.concatenate([buf2[ch, h, zz, yy, 0], buf2[ch, h, zz, yy, 1]], axis=-1)
        rhs = jnp.concatenate([w_cols[zz, yy, 0], w_cols[zz, yy, 1]], axis=0)
        out = jnp.dot(lhs, rhs, preferred_element_type=jnp.float32)
        rows = pl.ds(ch * CROWS + h * sub, sub)
        acc2[rows, :] = out if zero else acc2[rows, :] + out

    g = [gather_of(0), gather_of(1)]
    g2 = [
        Gather(
            ("attended", ch),
            buf2.at[ch],
            send,
            z,
            y,
            lambda h, zz, yy, ch=ch: use2(ch, h, zz, yy),
        )
        for ch in (0, 1)
    ]

    def finish(ch, h):
        rows = pl.ds(ch * CROWS + h * sub, sub)
        to = pl.ds(pl.multiple_of(seq_of(x) * CROWS + h * sub, sub), sub)
        for i in (0, 1):
            ob[i, rows, :] = acc2[rows, i * HEAD : (i + 1) * HEAD].astype(jnp.bfloat16)
        for dev in (right, left):
            send(ob.at[dev // 2, rows], mixed.at[ch, to], at_x(dev), "rows", ("fin",))

    def begin(ch):
        for h in (0, 1):
            send.wait("tok", ch, h)
            g[ch].start(h)

    def both(method, *args):
        for h in (0, 1):
            method(h, *args)

    def nears(ga):
        both(ga.near)
        both(ga.spread)

    def use_nears(ga):
        for d in DIRS:
            both(ga.use_near, d)

    def own_take(ch):
        send.wait("near", ch)
        send.wait("q", ch)

    with scope("begin0"):
        loads[2].wait()
        cols_z()
        begin(0)
    with scope("tables"):
        tables()
    with scope("middle0"):
        for h in (0, 1):
            own_dot(0, h)
        nears(g[0])
        use_nears(g[0])
        both(g[0].pass_on, 0)
        both(g[0].opposite)
        relay_w(0)
        both(g[0].use_passed, 0)
        both(g[0].use_opposite)
        both(g[0].pass_on, -1)
        both(g[0].use_passed, -1)
        both(g[0].pass_on, 1)
        relay_w(1)
    with scope("begin1"):
        begin(1)
    with scope("pass0"):
        both(g[0].pass_on, 2)
        both(g[0].use_passed, 1)
        relay_w2(0)
        relay_w(2)
        both(g[0].use_passed, 2)
    with scope("drain0a"):
        both(g[0].last, 0)
    with scope("near1"):
        nears(g[1])
    with scope("relay_w2"):
        relay_w2(1)
    with scope("drain0b"):
        both(g[0].last, -1)
        both(g[0].last, 1)
    with scope("pass1_0"):
        both(g[1].pass_on, 0)
    with scope("drain0c"):
        both(g[0].last, 2)
    with scope("have_w"):
        send.wait("relayed", False)
    with scope("far_qk0"):
        far_dots(0, (0, 1), CQ)
        squares(0)
    with scope("opp1"):
        both(g[1].opposite)
        relay_w2(2)
    with scope("uses1"):
        for h in (0, 1):
            own_dot(1, h)
        use_nears(g[1])
        send.wait("gains")
    with scope("tot0"):
        totals(0)
    with scope("have_wv"):
        send.wait("relayed", True)
    with scope("far_v0"):
        far_dots(0, (2,), CV)
        values(0)
    with scope("norms0"):
        norms(0)
        keys(0)
        queries(0)
    with scope("pass1_m"):
        both(g[1].pass_on, -1)
        both(g[1].use_passed, 0)
        both(g[1].use_opposite)
        both(g[1].use_passed, -1)
    with scope("take_v"):
        take_pair("v", 0)
        take_same("v", 0)
    with scope("pass1_1"):
        both(g[1].pass_on, 1)
    with scope("take_k"):
        take_pair("k", 0)
        take_same("k", 0)
    with scope("pass1_2"):
        both(g[1].pass_on, 2)
        cols_y()
    with scope("uses1c"):
        both(g[1].use_passed, 1)
        both(g[1].use_passed, 2)
        far_dots(1, (0, 1), CQ, (0, 1, 3))
    with scope("take_f"):
        take_fwd("v", 0)
        take_fwd("k", 0)
    with scope("drain1"):
        for j in (0, -1, 1, 2):
            both(g[1].last, j)
    with scope("far1"):
        far_dots(1, (0, 1), CQ, (2,))
        squares(1)
        cols_same()
    with scope("take0"):
        own_take(0)
    with scope("attend0"):
        attend(0)
    with scope("far_v1"):
        far_dots(1, (2,), CV)
        values(1)
    with scope("tot1"):
        totals(1)
    with scope("start_far0"):
        start_far(0)
    with scope("norms1"):
        norms(1)
        keys(1)
        queries(1)
    with scope("take_v1"):
        take_pair("v", 1)
        take_same("v", 1)
    with scope("near2"):
        nears(g2[0])
    with scope("take_k1"):
        take_pair("k", 1)
        take_same("k", 1)
        take_fwd("v", 1)
        send.wait("ws")
        cols_x(0)
    with scope("pass2_0"):
        both(g2[0].pass_on, 0)
        both(g2[0].opposite)
    with scope("pass2_m"):
        both(g2[0].pass_on, -1)
    with scope("take_fk1"):
        take_fwd("k", 1)
    with scope("pass2_1"):
        both(g2[0].pass_on, 1)
    with scope("take1"):
        own_take(1)
    with scope("attend1"):
        attend(1)
    with scope("pass2_2"):
        cols_x(1)
        both(g2[0].pass_on, 2)
    with scope("start_far1"):
        start_far(1)
        place = xl * 2 + co
        tops[place] = jnp.broadcast_to(jnp.maximum(*best), (8, HEAD))
        for dev in (other, at_x(same), at_x(same, 1 - co)):
            send(tops.at[place], tops.at[place], dev, "small", ("peak",))
    with scope("near3"):
        cols_core(0)
        nears(g2[1])
    with scope("pass3_0"):
        both(g2[1].pass_on, 0)
        both(g2[1].opposite)
    with scope("pass3_m"):
        cols_core(1)
        both(g2[1].pass_on, -1)
    with scope("cols_core"):
        send.wait("wc")
    with scope("use2"):
        for ch in (0, 1):
            for h in (0, 1):
                use2(ch, h, z, y, True)
        use_nears(g2[0])
        both(g2[0].use_passed, 0)
        both(g2[0].use_opposite)
        for j in (-1, 1, 2):
            both(g2[0].use_passed, j)
    with scope("pass3_1"):
        both(g2[1].pass_on, 1)
    with scope("drain2_0"):
        for j in (0, -1, 1):
            both(g2[0].last, j)
        for h in (0, 1):
            g2[0].last(h, 2)
            finish(0, h)
    with scope("pass3"):
        use_nears(g2[1])
        both(g2[1].use_passed, 0)
        both(g2[1].use_opposite)
        both(g2[1].use_passed, -1)
        both(g2[1].use_passed, 1)
        both(g2[1].pass_on, 2)
        both(g2[1].use_passed, 2)
    with scope("drain2_1"):
        for j in (0, -1, 1):
            both(g2[1].last, j)
        for h in (0, 1):
            g2[1].last(h, 2)
            finish(1, h)
    with scope("final"):
        send.wait("peak")
        peak[...] = jnp.maximum(jnp.maximum(tops[0], tops[1]), jnp.maximum(tops[2], tops[3]))
        send.wait("stats")
        for s in (0, 1):
            for i in (0, 1):
                stat_out[:, s, i * CROWS : (i + 1) * CROWS] = inv_in[s, i]
        send.wait("fin")
    with scope("wait_send"):
        send.flush()


def finish_kernel(mixed, peak, stat, mixed_out, peak_out, stat_out):
    mixed_out[...] = mixed[...]
    peak_out[0] = peak[0, 0]
    stat_out[...] = stat[...]


def vmem(count):
    return [pl.BlockSpec(memory_space=pltpu.VMEM)] * count


def shards(tokens, w_qkv, q_gain, k_gain, w_out):
    bf, f32 = jnp.bfloat16, jnp.float32
    dma = pltpu.SemaphoreType.DMA
    sub = CROWS // 2
    freq = ROPE_BASE ** (-(np.arange(HEAD) % (HEAD // 2) * 2.0) / HEAD)
    mixed, peak, stat = pl.pallas_call(
        layer_kernel,
        out_shape=(
            jax.ShapeDtypeStruct((2, TOK, HEAD), bf),
            jax.ShapeDtypeStruct((8, HEAD), f32),
            jax.ShapeDtypeStruct((2, 2, TOK), f32),
        ),
        in_specs=[pl.BlockSpec(memory_space=pltpu.HBM)] * 6,
        out_specs=tuple(vmem(3)),
        scratch_shapes=[
            pltpu.VMEM((2, TOK, HEAD), bf),
            pltpu.VMEM((3, WIDTH, HEAD), bf),
            pltpu.VMEM((HEAD, WIDTH), bf),
            pltpu.VMEM((1, HEAD), f32),
            pltpu.VMEM((CHUNKS, 2, 4, 4, 2, sub, HEAD), bf),
            pltpu.VMEM((3, WIDTH, HEAD), bf),
            pltpu.VMEM((8, HEAD), f32),
            pltpu.VMEM((8, HEAD), f32),
            pltpu.VMEM((CROWS, HEAD), f32),
            pltpu.VMEM((CROWS, HEAD), f32),
            pltpu.VMEM((TOK, 3 * HEAD), f32),
            pltpu.VMEM((TOK, 3 * HEAD), f32),
            pltpu.VMEM((CHUNKS, 4, 2, CROWS), f32),
            pltpu.VMEM((CHUNKS, 4, 2, CROWS), f32),
            pltpu.VMEM((CHUNKS, 2, CROWS), f32),
            pltpu.VMEM((CHUNKS, 2, 2, CROWS), f32),
            pltpu.VMEM((CHUNKS, 2, CROWS, HEAD), bf),
            pltpu.VMEM((CHUNKS, 8, CROWS, HEAD), bf),
            pltpu.VMEM((CHUNKS, 8, HEAD, CROWS), bf),
            pltpu.VMEM((CHUNKS, CROWS, HEAD), bf),
            pltpu.VMEM((CHUNKS, CROWS, HEAD), bf),
            pltpu.VMEM((CHUNKS, HEAD, CROWS), bf),
            pltpu.VMEM((4, 32, 1024), bf),
            pltpu.VMEM((4, 4, 2, HEAD, 256), bf),
            pltpu.VMEM((CHUNKS, 2, 4, 4, 2, sub, HEAD), bf),
            pltpu.VMEM((CHUNKS, 2, sub, HEAD), bf),
            pltpu.VMEM((TOK, 256), f32),
            pltpu.VMEM((2, TOK, HEAD), bf),
            pltpu.VMEM((4, 8, HEAD), f32),
            pltpu.VMEM((BK, CROWS), f32),
            pltpu.VMEM((BK, CROWS), f32),
            pltpu.VMEM((2, 1, CROWS), f32),
            pltpu.VMEM((2, 1, CROWS), f32),
            pltpu.VMEM((2, HEAD, CROWS), f32),
            dma((11,)),
            dma((129,)),
            dma((6,)),
        ],
        compiler_params=pltpu.CompilerParams(
            collective_id=0, has_side_effects=True, vmem_limit_bytes=VMEM_CAP
        ),
        name="layer",
    )(
        tokens,
        w_qkv.transpose(1, 0, 2),
        q_gain[None],
        k_gain[None],
        w_out,
        jnp.asarray(freq[None], f32),
    )
    return pl.pallas_call(
        finish_kernel,
        out_shape=(
            jax.ShapeDtypeStruct((2, TOK, HEAD), bf),
            jax.ShapeDtypeStruct((1,), f32),
            jax.ShapeDtypeStruct((2, 2, TOK), f32),
        ),
        in_specs=vmem(3),
        out_specs=(
            pl.BlockSpec(memory_space=pltpu.VMEM),
            pl.BlockSpec(memory_space=pltpu.SMEM),
            pl.BlockSpec(memory_space=pltpu.VMEM),
        ),
        name="finish",
    )(mixed, peak, stat)


def solution(mesh):
    finer = Mesh(mesh.devices.reshape(2, 2, 4, 4, 2), ("xl", "co", "z", "y", "xh"))
    tensor = ("z", "y", "xh")
    seq = ("xl", "co")
    placed = (P(None, seq, tensor), P(None, None, tensor), P(tensor), P(tensor), P(tensor, None))
    return jax.shard_map(
        shards,
        mesh=finer,
        in_specs=placed,
        out_specs=(P(None, seq, tensor), P(tensor), P(None, None, seq)),
        check_vma=False,
    )
```

```python
import contextlib
import math

import jax
import jax.numpy as jnp
import numpy as np
from jax import lax
from jax.experimental import pallas as pl
from jax.experimental.pallas import tpu as pltpu
from jax.sharding import Mesh
from jax.sharding import PartitionSpec as P

EPS = 1e-06
ROPE_BASE = 500000.0
NEG = -1e30
MESH = pl.DeviceIdType.MESH
HEAD = 128
TOK = 1024
CHUNKS = 2
CROWS = TOK // CHUNKS
WIDTH = 4096
BK = 512
VMEM_CAP = 60 * 1024 * 1024
SCALE = HEAD ** (-0.5)
LOG2E = math.log2(math.e)
DIRS = (1, -1)
PART = {1: 0, -1: 1}
CQ, CK, CV = 0, HEAD, 2 * HEAD


def scope(name):
    return contextlib.nullcontext()


def here():
    xh, xl = lax.axis_index("xh"), lax.axis_index("xl")
    return xh * 2 + xl, xh, xl, lax.axis_index("co"), lax.axis_index("z"), lax.axis_index("y")


def seq_of(x):
    return 1 - ((x + 1) // 2) % 2


def half_of(x):
    return 1 - x % 2


def at_x(x, core=None):
    dev = {"xl": x % 2, "xh": x // 2}
    if core is not None:
        dev["co"] = core
    return dev


class Sender:
    def __init__(self, ssem, rsem, region):
        self.ssem, self.rsem, self.region = ssem, rsem, region
        self.groups, self.keys = {}, {}
        self.leaving, self.arriving = {}, {}

    def __call__(self, src, dst, dev, group, key):
        g = self.groups.setdefault(group, len(self.groups))
        k = self.keys.setdefault(key, len(self.keys))
        size = math.prod(src.shape) * jnp.dtype(src.dtype).itemsize
        self.leaving[group] = self.leaving.get(group, 0) + size
        self.arriving[key] = self.arriving.get(key, 0) + size
        pltpu.make_async_remote_copy(
            src_ref=src,
            dst_ref=dst,
            send_sem=self.ssem.at[g],
            recv_sem=self.rsem.at[k],
            device_id=dev,
            device_id_type=MESH,
        ).start()

    def wait(self, *key):
        ref = self.region(self.arriving.pop(key))
        pltpu.make_async_copy(ref, ref, self.rsem.at[self.keys[key]]).wait()

    def flush(self):
        assert not self.arriving, self.arriving
        for group, size in self.leaving.items():
            ref = self.region(size)
            pltpu.make_async_copy(ref, ref, self.ssem.at[self.groups[group]]).wait()


class Gather:
    def __init__(self, name, buf, send, z, y, use):
        self.name, self.buf, self.send, self.use = name, buf, send, use
        self.first, self.second = (z, y), (y, z)

    def place(self, h, f, s):
        return (f % 4, s % 4) if h == 0 else (s % 4, f % 4)

    def at(self, h, df, ds):
        return self.place(h, self.first[h] + df, self.second[h] + ds)

    def move(self, h, df, ds, part, along, d, *key):
        zz, yy = self.at(h, df, ds)
        ref = self.buf.at[h, zz, yy] if part is None else self.buf.at[h, zz, yy, part]
        name = (("z", "y"), ("y", "z"))[h][along]
        me = (self.first[h], self.second[h])[along]
        self.send(ref, ref, {name: (me + d + 4) % 4}, self.name, (self.name, *key))

    def wait(self, h, *key):
        if h == 0:
            self.send.wait(self.name, *key)

    def start(self, h, part=None):
        for d in DIRS:
            self.move(h, 0, 0, part, 0, d, "p1")
            self.move(h, 0, 0, part, 1, d, "p2", 0)

    def near(self, h):
        self.wait(h, "p1")
        for d in DIRS:
            self.move(h, 4 - d, 0, PART[d], 0, d, "p1f")

    def spread(self, h):
        for d in DIRS:
            for e in DIRS:
                self.move(h, 4 - d, 0, None, 1, e, "p2", -d)

    def use_near(self, h, d):
        self.use(h, *self.at(h, 4 - d, 0))

    def pass_on(self, h, j):
        self.wait(h, "p2", j)
        for d in DIRS:
            self.move(h, j + 4, 4 - d, PART[d], 1, d, "p2f", j)

    def use_passed(self, h, j):
        for d in DIRS:
            self.use(h, *self.at(h, j + 4, 4 - d))

    def opposite(self, h):
        self.wait(h, "p1f")
        for d in DIRS:
            self.move(h, 2, 0, None, 1, d, "p2", 2)

    def use_opposite(self, h):
        self.use(h, *self.at(h, 2, 0))

    def last(self, h, j):
        self.wait(h, "p2f", j)
        self.use(h, *self.at(h, j + 4, 2))


def layer_kernel(
    tok_hbm, w_hbm, q_gain, k_gain, w_out_hbm, freq_hbm,
    mixed, peak, stat_out,
    tok, w_own, w_out, freq, buf, w_far, gains, gains_far, cosf, sinf, acc, acc_far, zb, yb, inv, inv_in,
    q_all, k_all, v_all, q_far, k_far, v_far,
    wz, w_cols, buf2, o_far, acc2, ob, tops,
    sc0, sc1, top_r, den_r, acc_r,
    ssem, rsem, ins,
):
    loads = [
        pltpu.make_async_copy(src, dst, ins.at[i])
        for i, (src, dst) in enumerate(
            (
                (tok_hbm, tok), (w_hbm, w_own), (w_out_hbm, w_out), (freq_hbm, freq),
                (q_gain, gains.at[0:1]), (k_gain, gains.at[1:2]),
            )
        )
    ]
    for cp in loads:
        cp.start()
    x, xh, xl, co, z, y = here()
    right, left, pair, same = (x + 1) % 4, (x + 3) % 4, 3 - x, xh * 2 + (1 - xl)
    other = {"co": 1 - co}
    peers = (
        [other] + [at_x((x + i) % 4, cc) for i in (1, 2, 3) for cc in (co, 1 - co)]
        + [{"z": (z + i) % 4} for i in (1, 2, 3)]
        + [{"y": (y + i) % 4} for i in (1, 2, 3)]
    )
    with scope("greet"):
        barrier = pltpu.get_barrier_semaphore()
        for dev in peers:
            pl.semaphore_signal(barrier, inc=1, device_id=dev, device_id_type=MESH)
        pl.semaphore_wait(barrier, len(peers))

    def region(size):
        for n in (1, 2, 3):
            if size % (n * 4096) == 0 and size <= n * WIDTH * HEAD * 2:
                return w_far.at[0:n, 0 : size // (n * HEAD * 2)]
        rows, rest = divmod(size, 64 * HEAD * 2)
        assert rest == 0 and rows % 16 == 0 and rows <= CROWS // 2, size
        return buf.at[0, :, :, :, :, 0:rows]

    send = Sender(ssem, rsem, region)
    sub = CROWS // 2

    def eighth(xx, cc):
        return 4 * half_of(xx) + 2 * cc + seq_of(xx)

    mine, far_tile = eighth(x, co), eighth(pair, 1 - co)
    part_of_mine = pl.ds(pl.multiple_of(seq_of(x) * CROWS, CROWS), CROWS)

    def send_tokens(ch):
        for h in (0, 1):
            dst = buf.at[ch, h, z, y, xh]
            for part, dev in ((xh, right), (1 - xh, left)):
                src = tok.at[ch, pl.ds(pl.multiple_of(part * CROWS + h * sub, sub), sub)]
                send(src, dst, at_x(dev), "rows", ("tok", ch, h))

    loads[0].wait()
    send_tokens(0)
    loads[1].wait()
    for cp in loads[3:]:
        cp.wait()

    def w_rows(xx):
        return pl.ds(pl.multiple_of(((xx % 2) * 2 + co) * 1024, 1024), 1024)

    def send_w(j):
        send(w_own.at[j, w_rows(x)], w_far.at[j, w_rows(x)], at_x(pair), "w", ("far_w", j))

    def relay_w(j):
        send.wait("far_w", j)
        ref = w_far.at[j, w_rows(pair)]
        send(ref, ref, at_x(same), "w", ("same_w", j))
        send(ref, ref, other, "w", ("relayed", j == 2))

    def relay_w2(j):
        send.wait("same_w", j)
        ref = w_far.at[j, w_rows(pair + 1)]
        send(ref, ref, other, "w", ("relayed", j == 2))

    send_w(0)
    send_w(1)
    send_tokens(1)
    send_w(2)
    send(gains, gains_far, at_x(pair), "small", ("gains",))

    def dots(target, w, ch, h, blocks, zero=False, kinds=(0, 1, 2), at=0):
        lhs, rhs = [], []
        for zz, yy in blocks:
            lhs += [buf[ch, h, zz, yy, 0], buf[ch, h, zz, yy, 1]]
            rows = pl.ds(pl.multiple_of((zz * 4 + yy) * 256, 256), 256)
            some = [w[j, rows, :] for j in kinds]
            rhs.append(some[0] if len(some) == 1 else jnp.concatenate(some, axis=-1))
        lhs = jnp.concatenate(lhs, axis=-1)
        rhs = rhs[0] if len(rhs) == 1 else jnp.concatenate(rhs, axis=0)
        out = jnp.dot(lhs, rhs, preferred_element_type=jnp.float32)
        place = (pl.ds(ch * CROWS + h * sub, sub), slice(at, at + HEAD * len(kinds)))
        target[place] = out if zero else target[place] + out

    def gather_of(ch):
        return Gather(
            ("tokens", ch), buf.at[ch], send, z, y, lambda h, zz, yy: dots(acc, w_own, ch, h, [(zz, yy)])
        )

    def own_dot(ch, h):
        dots(acc, w_own, ch, h, [(z, y)], True)

    def far_dots(ch, kinds, at, lines=(0, 1, 3, 2)):
        for i in lines:
            for h in (0, 1):
                blocks = [g[ch].at(h, f, i) for f in range(4)]
                dots(acc_far, w_far, ch, h, blocks, i == 0, kinds, at)

    def tables():
        def some(i, carry):
            rows = pl.ds(pl.multiple_of(i * 256, 256), 256)
            p = lax.broadcasted_iota(jnp.int32, (256, HEAD), 0) + (mine * CROWS + i * 256)
            lane = lax.broadcasted_iota(jnp.int32, (256, HEAD), 1)
            angle = p.astype(jnp.float32) * freq[...]
            cosf[rows, :] = jnp.cos(angle)
            sine = jnp.sin(angle)
            sinf[rows, :] = jnp.where(lane < HEAD // 2, -sine, sine)
            return carry

        lax.fori_loop(0, CROWS // 256, some, 0)

    def squares(ch):
        for j, c in ((0, CQ), (1, CK)):
            cols = pl.ds(c, HEAD)
            for i in range(2):
                rows = pl.ds(ch * CROWS + i * sub, sub)
                a, b = acc[rows, cols], acc_far[rows, cols]
                zb[ch, z, j : j + 1, i * sub : (i + 1) * sub] = jnp.sum(
                    (a * a + b * b).T, axis=0, keepdims=True
                )
        ref = zb.at[ch, z]
        for i in (1, 2, 3):
            send(ref, ref, {"z": (z + i) % 4}, "small", ("zsum", ch))

    def totals(ch):
        send.wait("zsum", ch)
        yb[ch, y] = (zb[ch, 0] + zb[ch, 1]) + (zb[ch, 2] + zb[ch, 3])
        ref = yb.at[ch, y]
        for i in (1, 2, 3):
            send(ref, ref, {"y": (y + i) % 4}, "small", ("ysum", ch))

    def turned(a, j, g, ch, i):
        rows = pl.ds(ch * CROWS + i * sub, sub)
        table = slice(i * sub, (i + 1) * sub)
        col = jnp.broadcast_to(inv[ch, j : j + 1, table], (HEAD, sub)).T
        t = a[rows, j * HEAD : (j + 1) * HEAD] * col * g[j : j + 1, :]
        return (t * cosf[table, :] + pltpu.roll(t, HEAD // 2, 1) * sinf[table, :]).astype(
            jnp.bfloat16
        )

    def give(name, ch, far, all_):
        slot = all_.at[ch, mine]
        send(far.at[ch], slot, at_x(pair), name, ("pair", name, ch))
        send(slot, slot, at_x(same), name, ("same", name, ch))
        send(slot, slot, other, name, ("near", ch))

    def take_pair(name, ch):
        ref = (k_all if name == "k" else v_all).at[ch, eighth(pair, co)]
        send.wait("pair", name, ch)
        send(ref, ref, at_x(same), name, ("fwd", name, ch))
        send(ref, ref, other, name, ("near", ch))

    def take_same(name, ch):
        ref = (k_all if name == "k" else v_all).at[ch, eighth(same, co)]
        send.wait("same", name, ch)
        send(ref, ref, other, name, ("near", ch))

    def take_fwd(name, ch):
        ref = (k_all if name == "k" else v_all).at[ch, eighth((x + 2) % 4, co)]
        send.wait("fwd", name, ch)
        send(ref, ref, other, name, ("near", ch))

    def values(ch):
        for i in range(2):
            here_rows = slice(i * sub, (i + 1) * sub)
            rows = pl.ds(ch * CROWS + i * sub, sub)
            v_far[ch, :, here_rows] = acc_far[rows, CV : CV + HEAD].T.astype(jnp.bfloat16)
            v_all[ch, mine, :, here_rows] = acc[rows, CV : CV + HEAD].T.astype(jnp.bfloat16)
        give("v", ch, v_far, v_all)

    def keys(ch):
        for i in range(2):
            here_rows = slice(i * sub, (i + 1) * sub)
            k_far[ch, here_rows, :] = turned(acc_far, 1, gains_far, ch, i)
            k_all[ch, mine, here_rows, :] = turned(acc, 1, gains, ch, i)
        give("k", ch, k_far, k_all)

    def queries(ch):
        for i in range(2):
            q_far[ch, i * sub : (i + 1) * sub, :] = turned(acc_far, 0, gains_far, ch, i)
        send(q_far.at[ch], q_all.at[ch, 1], at_x(pair, 1 - co), "rows", ("q", ch))
        for i in range(2):
            q_all[ch, 0, i * sub : (i + 1) * sub, :] = turned(acc, 0, gains, ch, i)

    def norms(ch):
        send.wait("ysum", ch)
        inv[ch] = lax.rsqrt(((yb[ch, 0] + yb[ch, 1]) + (yb[ch, 2] + yb[ch, 3])) / WIDTH + EPS)
        for dev in (right, left):
            send(inv.at[ch], inv_in.at[ch, seq_of(x)], at_x(dev), "small", ("stats",))

    part = pl.ds(pl.multiple_of(co * 64, 64), 64)
    strip = pl.ds(pl.multiple_of((co * 2 + x % 2) * 32, 32), 32)

    def z_cols(zz):
        return pl.ds(pl.multiple_of((zz % 4) * 1024, 1024), 1024)

    def y_cols(yy):
        return pl.ds(pl.multiple_of((yy % 4) * 256, 256), 256)

    def cols_z():
        wz[z] = w_out[strip, z_cols(z)]
        for i in (1, 2, 3):
            send(
                w_out.at[strip, z_cols(z + i)], wz.at[z], {"z": (z + i) % 4}, "cols", ("wz",)
            )

    def cols_y():
        send.wait("wz")
        w_cols[:, y, xh, strip, :] = wz[:, :, y_cols(y)]
        for i in (1, 2, 3):
            send(
                wz.at[:, :, y_cols(y + i)],
                w_cols.at[:, y, xh, strip],
                {"y": (y + i) % 4},
                "cols",
                ("wy",),
            )

    def cols_same():
        send.wait("wy")
        ref = w_cols.at[:, :, xh, strip]
        send(ref, ref, at_x(same), "cols", ("ws",))

    def cols_x(i):
        ref = w_cols.at[2 * i : 2 * i + 2, :, xh, part]
        send(ref, ref, at_x(pair), "cols", ("wx", i))

    def cols_core(i):
        send.wait("wx", i)
        ref = w_cols.at[2 * i : 2 * i + 2, :, :, part]
        send(ref, ref, other, "core", ("wc",))

    best = []

    def attend(ch):
        count = far_tile + 1
        total = count + mine + 1

        top_r[...] = jnp.full((2, 1, CROWS), NEG, jnp.float32)
        den_r[...] = jnp.zeros((2, 1, CROWS), jnp.float32)
        acc_r[...] = jnp.zeros((2, HEAD, CROWS), jnp.float32)

        def where(t):
            own = (t + 16 - count) // 16
            return 1 - own, (1 - own) * (count - 1 - t) + own * (t - count)

        def score(t, into):
            which, j = where(t)
            raw = lax.dot_general(
                k_all[ch, j], q_all[ch, which], (((1,), (1,)), ((), ())),
                preferred_element_type=jnp.float32,
            )
            into[...] = raw

        def weigh(t, cur, masked):
            which, j = where(t)
            s = cur[...]
            if masked:
                r = lax.broadcasted_iota(jnp.int32, (BK, CROWS), 0)
                c = lax.broadcasted_iota(jnp.int32, (BK, CROWS), 1)
                s = jnp.where(r <= c, s, NEG)
            top, p = top_r[which], SCALE * LOG2E
            new = jnp.maximum(top, jnp.max(s, axis=0, keepdims=True))
            e = jnp.exp2((s - new) * p)
            keep = jnp.exp2((top - new) * p)
            den_r[which] = den_r[which] * keep + jnp.sum(e, axis=0, keepdims=True)
            acc_r[which] = acc_r[which] * keep + jnp.dot(
                v_all[ch, j], e.astype(jnp.bfloat16), preferred_element_type=jnp.float32
            )
            top_r[which] = new

        score(0, sc0)
        score(1, sc1)
        weigh(0, sc0, True)

        def two(i, carry):
            t = 2 * i + 1
            score(t + 1, sc0)
            weigh(t, sc1, False)
            score(t + 2, sc1)
            weigh(t + 1, sc0, False)
            return carry

        lax.fori_loop(0, 3 + seq_of(x), two, 0)
        weigh(total - 1, sc1, True)
        for h in (0, 1):
            o_far[ch, h] = (
                (acc_r[1, :, h * sub : (h + 1) * sub] / den_r[1, :, h * sub : (h + 1) * sub])
                .T.astype(jnp.bfloat16)
            )
            dst = buf2.at[ch, h, z, y, xh]
            send(o_far.at[ch, h], dst, at_x(pair, 1 - co), "rows", ("back", ch, h))
        for h in (0, 1):
            buf2[ch, h, z, y, xh] = (
                (acc_r[0, :, h * sub : (h + 1) * sub] / den_r[0, :, h * sub : (h + 1) * sub])
                .T.astype(jnp.bfloat16)
            )
            g2[ch].start(h, xh)
        peaks_here = [jnp.max(top_r[i], axis=1, keepdims=True) for i in (0, 1)]
        best.append(jnp.maximum(*peaks_here) * SCALE)

    def start_far(ch):
        for h in (0, 1):
            send.wait("back", ch, h)
            g2[ch].start(h, 1 - xh)

    def use2(ch, h, zz, yy, zero=False):
        lhs = jnp.concatenate([buf2[ch, h, zz, yy, 0], buf2[ch, h, zz, yy, 1]], axis=-1)
        rhs = jnp.concatenate([w_cols[zz, yy, 0], w_cols[zz, yy, 1]], axis=0)
        out = jnp.dot(lhs, rhs, preferred_element_type=jnp.float32)
        rows = pl.ds(ch * CROWS + h * sub, sub)
        acc2[rows, :] = out if zero else acc2[rows, :] + out

    g = [gather_of(0), gather_of(1)]
    g2 = [
        Gather(
            ("attended", ch),
            buf2.at[ch],
            send,
            z,
            y,
            lambda h, zz, yy, ch=ch: use2(ch, h, zz, yy),
        )
        for ch in (0, 1)
    ]

    def finish(ch, h):
        rows = pl.ds(ch * CROWS + h * sub, sub)
        to = pl.ds(pl.multiple_of(seq_of(x) * CROWS + h * sub, sub), sub)
        for i in (0, 1):
            ob[i, rows, :] = acc2[rows, i * HEAD : (i + 1) * HEAD].astype(jnp.bfloat16)
        for dev in (right, left):
            send(ob.at[dev // 2, rows], mixed.at[ch, to], at_x(dev), "rows", ("fin",))

    def begin(ch):
        for h in (0, 1):
            send.wait("tok", ch, h)
            g[ch].start(h)

    def both(method, *args):
        for h in (0, 1):
            method(h, *args)

    def nears(ga):
        both(ga.near)
        both(ga.spread)

    def use_nears(ga):
        for d in DIRS:
            both(ga.use_near, d)

    def own_take(ch):
        send.wait("near", ch)
        send.wait("q", ch)

    with scope("begin0"):
        loads[2].wait()
        cols_z()
        begin(0)
    with scope("tables"):
        tables()
    with scope("middle0"):
        for h in (0, 1):
            own_dot(0, h)
        nears(g[0])
        use_nears(g[0])
        both(g[0].pass_on, 0)
        both(g[0].opposite)
        relay_w(0)
        both(g[0].use_passed, 0)
        both(g[0].use_opposite)
        both(g[0].pass_on, -1)
        both(g[0].use_passed, -1)
        both(g[0].pass_on, 1)
        relay_w(1)
    with scope("begin1"):
        begin(1)
    with scope("pass0"):
        both(g[0].pass_on, 2)
        both(g[0].use_passed, 1)
        relay_w2(0)
        relay_w(2)
        both(g[0].use_passed, 2)
    with scope("drain0a"):
        both(g[0].last, 0)
    with scope("near1"):
        nears(g[1])
    with scope("relay_w2"):
        relay_w2(1)
    with scope("drain0b"):
        both(g[0].last, -1)
        both(g[0].last, 1)
    with scope("pass1_0"):
        both(g[1].pass_on, 0)
    with scope("drain0c"):
        both(g[0].last, 2)
    with scope("have_w"):
        send.wait("relayed", False)
    with scope("far_qk0"):
        far_dots(0, (0, 1), CQ)
        squares(0)
    with scope("opp1"):
        both(g[1].opposite)
        relay_w2(2)
    with scope("uses1"):
        for h in (0, 1):
            own_dot(1, h)
        use_nears(g[1])
        send.wait("gains")
    with scope("tot0"):
        totals(0)
    with scope("have_wv"):
        send.wait("relayed", True)
    with scope("far_v0"):
        far_dots(0, (2,), CV)
        values(0)
    with scope("norms0"):
        norms(0)
        keys(0)
        queries(0)
    with scope("pass1_m"):
        both(g[1].pass_on, -1)
        both(g[1].use_passed, 0)
        both(g[1].use_opposite)
        both(g[1].use_passed, -1)
    with scope("take_v"):
        take_pair("v", 0)
        take_same("v", 0)
    with scope("pass1_1"):
        both(g[1].pass_on, 1)
    with scope("take_k"):
        take_pair("k", 0)
        take_same("k", 0)
    with scope("pass1_2"):
        both(g[1].pass_on, 2)
        cols_y()
    with scope("uses1c"):
        both(g[1].use_passed, 1)
        both(g[1].use_passed, 2)
        far_dots(1, (0, 1), CQ, (0, 1, 3))
    with scope("take_f"):
        take_fwd("v", 0)
        take_fwd("k", 0)
    with scope("drain1"):
        for j in (0, -1, 1, 2):
            both(g[1].last, j)
    with scope("far1"):
        far_dots(1, (0, 1), CQ, (2,))
        squares(1)
        cols_same()
    with scope("take0"):
        own_take(0)
    with scope("attend0"):
        attend(0)
    with scope("far_v1"):
        far_dots(1, (2,), CV)
        values(1)
    with scope("tot1"):
        totals(1)
    with scope("start_far0"):
        start_far(0)
    with scope("norms1"):
        norms(1)
        keys(1)
        queries(1)
    with scope("take_v1"):
        take_pair("v", 1)
        take_same("v", 1)
    with scope("near2"):
        nears(g2[0])
    with scope("take_k1"):
        take_pair("k", 1)
        take_same("k", 1)
        take_fwd("v", 1)
        send.wait("ws")
        cols_x(0)
    with scope("pass2_0"):
        both(g2[0].pass_on, 0)
        both(g2[0].opposite)
    with scope("pass2_m"):
        both(g2[0].pass_on, -1)
    with scope("take_fk1"):
        take_fwd("k", 1)
    with scope("pass2_1"):
        both(g2[0].pass_on, 1)
    with scope("take1"):
        own_take(1)
    with scope("attend1"):
        attend(1)
    with scope("pass2_2"):
        cols_x(1)
        both(g2[0].pass_on, 2)
    with scope("start_far1"):
        start_far(1)
        place = xl * 2 + co
        tops[place] = jnp.broadcast_to(jnp.maximum(*best), (8, HEAD))
        for dev in (other, at_x(same), at_x(same, 1 - co)):
            send(tops.at[place], tops.at[place], dev, "small", ("peak",))
    with scope("near3"):
        cols_core(0)
        nears(g2[1])
    with scope("pass3_0"):
        both(g2[1].pass_on, 0)
        both(g2[1].opposite)
    with scope("pass3_m"):
        cols_core(1)
        both(g2[1].pass_on, -1)
    with scope("cols_core"):
        send.wait("wc")
    with scope("use2"):
        for ch in (0, 1):
            for h in (0, 1):
                use2(ch, h, z, y, True)
        use_nears(g2[0])
        both(g2[0].use_passed, 0)
        both(g2[0].use_opposite)
        for j in (-1, 1, 2):
            both(g2[0].use_passed, j)
    with scope("pass3_1"):
        both(g2[1].pass_on, 1)
    with scope("drain2_0"):
        for j in (0, -1, 1):
            both(g2[0].last, j)
        for h in (0, 1):
            g2[0].last(h, 2)
            finish(0, h)
    with scope("pass3"):
        use_nears(g2[1])
        both(g2[1].use_passed, 0)
        both(g2[1].use_opposite)
        both(g2[1].use_passed, -1)
        both(g2[1].use_passed, 1)
        both(g2[1].pass_on, 2)
        both(g2[1].use_passed, 2)
    with scope("drain2_1"):
        for j in (0, -1, 1):
            both(g2[1].last, j)
        for h in (0, 1):
            g2[1].last(h, 2)
            finish(1, h)
    with scope("final"):
        send.wait("peak")
        peak[...] = jnp.maximum(jnp.maximum(tops[0], tops[1]), jnp.maximum(tops[2], tops[3]))
        send.wait("stats")
        for s in (0, 1):
            for i in (0, 1):
                stat_out[:, s, i * CROWS : (i + 1) * CROWS] = inv_in[s, i]
        send.wait("fin")
    with scope("wait_send"):
        send.flush()


def finish_kernel(mixed, peak, stat, mixed_out, peak_out, stat_out):
    mixed_out[...] = mixed[...]
    peak_out[0] = peak[0, 0]
    stat_out[...] = stat[...]


def vmem(count):
    return [pl.BlockSpec(memory_space=pltpu.VMEM)] * count


def shards(tokens, w_qkv, q_gain, k_gain, w_out):
    bf, f32 = jnp.bfloat16, jnp.float32
    dma = pltpu.SemaphoreType.DMA
    sub = CROWS // 2
    freq = ROPE_BASE ** (-(np.arange(HEAD) % (HEAD // 2) * 2.0) / HEAD)
    mixed, peak, stat = pl.pallas_call(
        layer_kernel,
        out_shape=(
            jax.ShapeDtypeStruct((2, TOK, HEAD), bf),
            jax.ShapeDtypeStruct((8, HEAD), f32),
            jax.ShapeDtypeStruct((2, 2, TOK), f32),
        ),
        in_specs=[pl.BlockSpec(memory_space=pltpu.HBM)] * 6,
        out_specs=tuple(vmem(3)),
        scratch_shapes=[
            pltpu.VMEM((2, TOK, HEAD), bf),
            pltpu.VMEM((3, WIDTH, HEAD), bf),
            pltpu.VMEM((HEAD, WIDTH), bf),
            pltpu.VMEM((1, HEAD), f32),
            pltpu.VMEM((CHUNKS, 2, 4, 4, 2, sub, HEAD), bf),
            pltpu.VMEM((3, WIDTH, HEAD), bf),
            pltpu.VMEM((8, HEAD), f32),
            pltpu.VMEM((8, HEAD), f32),
            pltpu.VMEM((CROWS, HEAD), f32),
            pltpu.VMEM((CROWS, HEAD), f32),
            pltpu.VMEM((TOK, 3 * HEAD), f32),
            pltpu.VMEM((TOK, 3 * HEAD), f32),
            pltpu.VMEM((CHUNKS, 4, 2, CROWS), f32),
            pltpu.VMEM((CHUNKS, 4, 2, CROWS), f32),
            pltpu.VMEM((CHUNKS, 2, CROWS), f32),
            pltpu.VMEM((CHUNKS, 2, 2, CROWS), f32),
            pltpu.VMEM((CHUNKS, 2, CROWS, HEAD), bf),
            pltpu.VMEM((CHUNKS, 8, CROWS, HEAD), bf),
            pltpu.VMEM((CHUNKS, 8, HEAD, CROWS), bf),
            pltpu.VMEM((CHUNKS, CROWS, HEAD), bf),
            pltpu.VMEM((CHUNKS, CROWS, HEAD), bf),
            pltpu.VMEM((CHUNKS, HEAD, CROWS), bf),
            pltpu.VMEM((4, 32, 1024), bf),
            pltpu.VMEM((4, 4, 2, HEAD, 256), bf),
            pltpu.VMEM((CHUNKS, 2, 4, 4, 2, sub, HEAD), bf),
            pltpu.VMEM((CHUNKS, 2, sub, HEAD), bf),
            pltpu.VMEM((TOK, 256), f32),
            pltpu.VMEM((2, TOK, HEAD), bf),
            pltpu.VMEM((4, 8, HEAD), f32),
            pltpu.VMEM((BK, CROWS), f32),
            pltpu.VMEM((BK, CROWS), f32),
            pltpu.VMEM((2, 1, CROWS), f32),
            pltpu.VMEM((2, 1, CROWS), f32),
            pltpu.VMEM((2, HEAD, CROWS), f32),
            dma((11,)),
            dma((89,)),
            dma((6,)),
        ],
        compiler_params=pltpu.CompilerParams(
            collective_id=0, has_side_effects=True, vmem_limit_bytes=VMEM_CAP
        ),
        name="layer",
    )(
        tokens,
        w_qkv.transpose(1, 0, 2),
        q_gain[None],
        k_gain[None],
        w_out,
        jnp.asarray(freq[None], f32),
    )
    return pl.pallas_call(
        finish_kernel,
        out_shape=(
            jax.ShapeDtypeStruct((2, TOK, HEAD), bf),
            jax.ShapeDtypeStruct((1,), f32),
            jax.ShapeDtypeStruct((2, 2, TOK), f32),
        ),
        in_specs=vmem(3),
        out_specs=(
            pl.BlockSpec(memory_space=pltpu.VMEM),
            pl.BlockSpec(memory_space=pltpu.SMEM),
            pl.BlockSpec(memory_space=pltpu.VMEM),
        ),
        name="finish",
    )(mixed, peak, stat)


def solution(mesh):
    finer = Mesh(mesh.devices.reshape(2, 2, 4, 4, 2), ("xl", "co", "z", "y", "xh"))
    tensor = ("z", "y", "xh")
    seq = ("xl", "co")
    placed = (P(None, seq, tensor), P(None, None, tensor), P(tensor), P(tensor), P(tensor, None))
    return jax.shard_map(
        shards,
        mesh=finer,
        in_specs=placed,
        out_specs=(P(None, seq, tensor), P(tensor), P(None, None, seq)),
        check_vma=False,
    )
```
